32 devices in a mesh: gx: 4 (over z), gy: 2 (over x), gz: 4 (over y, core).
Axes of the slice: x: 2, y: 2, z: 4, core: 2. Of those that a mesh axis runs over, the one named last changes fastest.
Arguments:
- old_slots: bfloat16 [4, 2, 32, 4096], P('gx', 'gy', 'gz'), may hold values from -6 to 6
- old_ids: int32 [4, 2, 32], P('gx', 'gy', 'gz'), may hold values from -1 to 31, as said below
- old_owner: int32 [4, 2, 32], P('gx', 'gy'), may hold values from 0 to 3, as said below
- coefficient: float32 [64, 32, 512], P('gx', 'gy', 'gz'), may hold values from 0.2 to 5
Outputs:
- solution: float32 [64, 32, 512], P('gx', 'gy', 'gz')
The draws below stay inside these ranges and needn't reach their ends.
Inputs may be any that keep to these rules, and one draw needn't show every extreme that they name: old_owner[a, c, b] is the index along gz of the device that held box b of box column (a, c) before the move; no device holds more than 8 boxes of a column and some device holds exactly 8; no device holds more than 2 of the 8 boxes with one value of b // 8, and that bound is reached. old_ids[a, c, g * 8 + q] is the box held in slot q of device g of box column (a, c), or -1 for an empty slot; it agrees with old_owner and each box stands in exactly one slot.
All inputs are finite; a program needn't handle non-finite values.
Results may differ from the reference program's by a relative error of at most 0.0003.
Values may be sent and summed in bfloat16 or wider, within the bound.
A program may use at most 64 MiB of HBM per device.

```python
import math
import jax
import jax.numpy as jnp
from jax import lax

BOX = 16
NB = 8
SWEEPS = 2
CAP = 8
NX = 64
NY = 32
NZ = 512
N_GX = 4
N_GY = 2
N_GZ = 4


def column_maps(column_key):
    groups = N_GZ
    halves = NB // 2
    pair_count = groups * halves
    subkeys = jax.random.split(column_key, 5)
    labels = jnp.arange(groups, dtype=jnp.int32)
    if NB <= groups:
        counts = jnp.where(labels < groups // 4, 2 * halves, jnp.where(labels < groups // 2, halves, halves // 2)).astype(jnp.int32)
    else:
        counts = jnp.full((groups,), halves, jnp.int32)
    ending = jnp.cumsum(counts).astype(jnp.int32)
    items = jnp.arange(pair_count, dtype=jnp.int32)
    sorted_owner = jnp.sum((items[:, None] >= ending[None, :]).astype(jnp.int32), axis=1)
    relabel = jax.random.permutation(subkeys[0], groups).astype(jnp.int32)
    item_owner = relabel[sorted_owner]
    columns = jax.random.permutation(subkeys[1], groups).astype(jnp.int32)
    target = columns[items % groups]
    levels = items // groups
    placing = jax.vmap(lambda single: jax.random.permutation(single, NB).astype(jnp.int32))(jax.random.split(subkeys[2], groups))
    first_box = target * NB + placing[target, 2 * levels]
    second_box = target * NB + placing[target, 2 * levels + 1]
    box_count = groups * NB
    owners = jnp.zeros((box_count,), jnp.int32).at[first_box].set(item_owner).at[second_box].set(item_owner)
    priority = jax.random.permutation(subkeys[3], box_count).astype(jnp.int32)
    sharing = owners[:, None] == owners[None, :]
    ranking = jnp.sum((sharing & (priority[None, :] < priority[:, None])).astype(jnp.int32), axis=1)
    offsets = jax.random.randint(subkeys[4], (groups,), 0, CAP, dtype=jnp.int32)
    slot_index = (ranking + offsets[owners]) % CAP
    slot_ids = jnp.full((groups * CAP,), -1, jnp.int32).at[owners * CAP + slot_index].set(jnp.arange(box_count, dtype=jnp.int32))
    return (owners, slot_ids)


def all_columns(key):
    column_keys = jax.random.split(jax.random.fold_in(key, 31), N_GX * N_GY)
    return jax.vmap(column_maps)(column_keys)


def draw_old_owner(key, part):
    owners, slot_ids = all_columns(key)
    return owners.reshape(N_GX, N_GY, N_GZ * NB)


def draw_old_ids(key, part):
    owners, slot_ids = all_columns(key)
    return slot_ids.reshape(N_GX, N_GY, N_GZ * CAP)


def draw_old_slots(key, part):
    shape = (N_GX, N_GY, N_GZ * CAP, BOX ** 3)
    noise_key = jax.random.fold_in(jax.random.fold_in(key, 47), 0)
    return jnp.clip(jax.random.normal(noise_key, shape, jnp.float32), -6.0, 6.0).astype(jnp.bfloat16)


def level_of(own_key, extent, cuts, low, largest):
    gain, own = 1.0, jax.random.fold_in(own_key, 6)
    for axis_at, shards_of in cuts:
        draws = jnp.exp(jax.random.uniform(jax.random.fold_in(own, axis_at), (shards_of,), jnp.float32, low / len(cuts), largest / len(cuts)))
        gain = gain * jnp.repeat(draws, extent[axis_at] // shards_of).reshape([-1 if axis == axis_at else 1 for axis in range(len(extent))])
    return gain


def setup_inputs(seed: int = 0) -> dict:
    key_list = jax.random.split(jax.random.key(seed), 5)
    return {
        "old_slots": draw_old_slots(jax.random.fold_in(key_list[4], 71), 0),
        "old_ids": draw_old_ids(jax.random.fold_in(key_list[4], 71), 0),
        "old_owner": draw_old_owner(jax.random.fold_in(key_list[4], 71), 0),
        "coefficient": jnp.clip(jnp.exp(math.log(5.0) - 3.218876 * jax.random.uniform(key_list[3], (NX, NY, NZ), jnp.float32) ** level_of(key_list[3], (NX, NY, NZ), ((0, 4), (1, 2), (2, 4)), -0.2, 0.2)), 0.2, 5.0),
    }


def inner(padded):
    return padded[1:-1, 1:-1, 1:-1]


def operator_parts(padded):
    face_first = 0.5 * (padded[:-1, 1:-1, 1:-1] + padded[1:, 1:-1, 1:-1])
    face_second = 0.5 * (padded[1:-1, :-1, 1:-1] + padded[1:-1, 1:, 1:-1])
    face_third = 0.5 * (padded[1:-1, 1:-1, :-1] + padded[1:-1, 1:-1, 1:])
    diagonal = face_first[:-1] + face_first[1:] + face_second[:, :-1] + face_second[:, 1:] + face_third[:, :, :-1] + face_third[:, :, 1:]
    return face_first, face_second, face_third, diagonal


def neighbours(padded, stencil):
    face_first, face_second, face_third, diagonal = stencil
    summed = face_first[:-1] * padded[:-2, 1:-1, 1:-1] + face_first[1:] * padded[2:, 1:-1, 1:-1]
    summed = summed + face_second[:, :-1] * padded[1:-1, :-2, 1:-1] + face_second[:, 1:] * padded[1:-1, 2:, 1:-1]
    summed = summed + face_third[:, :, :-1] * padded[1:-1, 1:-1, :-2] + face_third[:, :, 1:] * padded[1:-1, 1:-1, 2:]
    return summed


def red_cells(shape, margin):
    index_first = lax.broadcasted_iota(jnp.int32, shape, 0)
    index_second = lax.broadcasted_iota(jnp.int32, shape, 1)
    index_third = lax.broadcasted_iota(jnp.int32, shape, 2)
    return (index_first + index_second + index_third + margin) % 2 == 0


def relax(padded, source, stencil, factor, chosen):
    fresh = (factor * source + neighbours(padded, stencil)) / stencil[3]
    return jnp.where(chosen, fresh, inner(padded))


def apply_operator(values, stencil, factor):
    return (stencil[3] * values - neighbours(jnp.pad(values, 1), stencil)) / factor


def smooth(values, source, stencil, factor):
    red_mask = red_cells(source.shape, 0)
    black_mask = jnp.logical_not(red_mask)
    for counter in range(SWEEPS):
        values = relax(jnp.pad(values, 1), source, stencil, factor, red_mask)
        values = relax(jnp.pad(values, 1), source, stencil, factor, black_mask)
    return values


def coarsen(values):
    extent_first, extent_second, extent_third = values.shape
    grouped = values.reshape(extent_first // 2, 2, extent_second // 2, 2, extent_third // 2, 2)
    return grouped.mean(axis=(1, 3, 5))


def refine(values):
    return jnp.repeat(jnp.repeat(jnp.repeat(values, 2, axis=0), 2, axis=1), 2, axis=2)


def bicgstab(rhs_low, stencil, factor):
    image_low = apply_operator(rhs_low, stencil, factor)
    alpha_step = jnp.sum(rhs_low * rhs_low) / jnp.sum(rhs_low * image_low)
    rest_low = rhs_low - alpha_step * image_low
    turned = apply_operator(rest_low, stencil, factor)
    omega_step = jnp.sum(turned * rest_low) / jnp.sum(turned * turned)
    return alpha_step * rhs_low + omega_step * rest_low


def move_boxes(old_slots, old_ids, old_owner):
    column_boxes = NB * N_GZ
    held = old_ids.reshape(N_GX, N_GY, N_GZ, CAP)
    owner_index = jnp.broadcast_to(old_owner[:, :, :, None], (N_GX, N_GY, column_boxes, CAP))
    owner_slots = jnp.take_along_axis(held, owner_index, axis=2)
    wanted = jnp.arange(column_boxes, dtype=jnp.int32)
    position = jnp.argmax(owner_slots == wanted[None, None, :, None], axis=3).astype(jnp.int32)
    global_slot = old_owner * CAP + position
    picked = jax.vmap(jax.vmap(lambda stacked, chosen_rows: stacked[chosen_rows]))(old_slots, global_slot)
    boxes = picked.reshape(N_GX, N_GY, column_boxes, BOX, BOX, BOX).transpose(0, 3, 1, 4, 2, 5)
    return boxes.reshape(N_GX * BOX, N_GY * BOX, column_boxes * BOX)


def reference(old_slots, old_ids, old_owner, coefficient):
    source_fine = move_boxes(old_slots, old_ids, old_owner).astype(jnp.float32)
    stencil_fine = operator_parts(jnp.pad(coefficient, 1))
    fine_values = smooth(jnp.zeros_like(source_fine), source_fine, stencil_fine, 1.0)
    residual_fine = source_fine - apply_operator(fine_values, stencil_fine, 1.0)
    coefficient_mid = coarsen(coefficient)
    stencil_mid = operator_parts(jnp.pad(coefficient_mid, 1))
    source_mid = coarsen(residual_fine)
    middle_values = smooth(jnp.zeros_like(source_mid), source_mid, stencil_mid, 4.0)
    residual_mid = source_mid - apply_operator(middle_values, stencil_mid, 4.0)
    coefficient_low = coarsen(coefficient_mid)
    stencil_low = operator_parts(jnp.pad(coefficient_low, 1))
    bottom_values = bicgstab(coarsen(residual_mid), stencil_low, 16.0)
    middle_values = smooth(middle_values + refine(bottom_values), source_mid, stencil_mid, 4.0)
    return smooth(fine_values + refine(middle_values), source_fine, stencil_fine, 1.0)
```

```python
import functools
import itertools

import jax
import jax.numpy as jnp
from jax import lax
from jax.experimental import pallas as pl
from jax.experimental.pallas import tpu as pltpu
from jax.sharding import PartitionSpec as P

BOX = 16
SEND = 2
F32 = jnp.float32
BF16 = jnp.bfloat16
MESH = pl.DeviceIdType.MESH
HIGH = lax.Precision.HIGHEST


def iota(shape, dim):
    return lax.broadcasted_iota(jnp.int32, shape, dim)


def up(v, axis):
    return pltpu.roll(v, 1, axis)


def down(v, axis):
    return pltpu.roll(v, v.shape[axis] - 1, axis)


class Level:
    def __init__(self, x, y, z, w, deep=False):
        self.x, self.y, self.z, self.w, self.deep = x, y, z, w, deep
        self.wx, self.wy = w + deep, -(-w // 4) * 4
        self.xe, self.ye = x + 2 * self.wx, y + 2 * self.wy
        self.ze = 128 if z + 2 * w <= 128 else z + 128
        self.shape = (self.xe, self.ye, self.ze)
        self.blocks = y // self.wy

    def units(self, a, b, c):
        extra = self.x // 4 if self.deep and not a and (not b or not c) else 0
        if c:
            return (self.wy if b else self.y) // 4 + extra
        return (self.wx if a else self.x) * (self.wy if b else self.y) // 4 + extra


NEAR = [(a, b, c) for c in (-1, 0, 1) for b in (-1, 0, 1) for a in (-1, 0, 1) if (a, b, c) != (0, 0, 0)]


def near(offset, counts):
    target, exists = {}, None
    for axis, step in zip(("gx", "gy", "gz"), offset):
        me, n = lax.axis_index(axis), counts[axis]
        if step:
            target[axis] = lax.rem(me + step + n, n)
            inside = me > 0 if step < 0 else me < n - 1
            exists = inside if exists is None else jnp.logical_and(exists, inside)
    return target, exists


def wait_units(units, count, sem):
    part = units.at[pl.ds(0, count)]
    pltpu.make_async_copy(part, part, sem).wait()


def wait_near(lv, counts, units, sems):
    choices = []
    for axis in ("gx", "gy", "gz"):
        me, n = lax.axis_index(axis), counts[axis]
        if n == 1:
            choices.append([(0, None)])
        elif n == 2:
            choices.append([(1, None)])
        else:
            edge = jnp.logical_or(me == 0, me == n - 1)
            choices.append([(1, edge), (2, jnp.logical_not(edge))])
    for chosen in itertools.product(*choices):
        total = 0
        for kind in itertools.product((0, 1), repeat=3):
            if any(kind):
                copies = 1
                for used, (number, _) in zip(kind, chosen):
                    copies *= number if used else 1
                total += copies * lv.units(*kind)
        conditions = [condition for _, condition in chosen if condition is not None]

        def wait():
            for sem in sems:
                wait_units(units, total, sem)

        if conditions:
            pl.when(functools.reduce(jnp.logical_and, conditions))(wait)
        else:
            wait()


def pack_sides(lv, v, bufs, deep=None):
    py, ly, pz, lz, lzb = bufs
    own, w = slice(lv.wx, lv.wx + lv.x), lv.w
    if lv.blocks > 1:
        py[0] = v[own, 0 : lv.wy, 0:128]
        py[1] = v[own, lv.y - lv.wy : lv.y, 0:128]
    lane = iota((lv.y, 128), 1)
    packed = layer = jnp.zeros((lv.y, 128), F32)
    for k in range(lv.x):
        plane = v[lv.wx + k, 0 : lv.y, 0:128]
        if lv.z == 64:
            plane = jnp.where(lane >= 64, pltpu.roll(plane, 64, 1), plane)
        turned = pltpu.roll(plane, (2 * w * k + w) % 128, 1)
        packed = jnp.where(lane // (2 * w) == k, turned, packed)
        if deep:
            layer = jnp.where((lane == (2 * w * k - 1) % 128) | (lane == (2 * w * k + 2 * w) % 128), turned, layer)
            deep[0][0, k : k + 1, :] = plane[w : w + 1, :]
            deep[0][1, k : k + 1, :] = plane[lv.y - w - 1 : lv.y - w, :]
    if deep:
        deep[2][...] = layer
    for block in range(lv.blocks):
        pz[block] = packed[block * lv.wy : block * lv.wy + lv.wy]


def send_sides(lv, v, bufs, sems, counts, deep=None):
    py, ly, pz, lz, lzb = bufs
    wx, block = lv.wx, (pl.ds(0, lv.y), pl.ds(0, 128))
    taken = {-1: (0, wx), 0: (0, lv.x), 1: (lv.x - wx, wx)}
    landed = {-1: lv.x + wx, 0: wx, 1: 0}
    for a, b, c in reversed(sorted(NEAR, key=lambda n: (n[0] != 0) + (n[1] != 0) + (n[2] != 0))):
        target, exists = near((a, b, c), counts)
        first, count = taken[a]
        if c and b:
            src, dst = pz.at[0 if b < 0 else lv.blocks - 1], lzb.at[(1 - c) // 2, 1 - a, (1 - b) // 2]
        elif c:
            src, dst = pz, lz.at[(1 - c) // 2, 1 - a]
        elif b:
            side = (b + 1) // 2
            src = py.at[side, pl.ds(first, count)] if lv.blocks > 1 else v.at[(pl.ds(wx + first, count),) + block]
            dst = ly.at[side, pl.ds(landed[a], count)]
        else:
            src, dst = v.at[(pl.ds(wx + first, count),) + block], v.at[(pl.ds(landed[a], count),) + block]
        copy = pltpu.make_async_remote_copy(
            src, dst, sems.at[0], sems.at[1], device_id=target, device_id_type=MESH)
        pl.when(exists)(copy.start)
        if deep and not a and (not b or not c):
            src, dst = (deep[2], deep[3].at[(1 - c) // 2]) if c else (deep[0].at[side], deep[1].at[side])
            copy = pltpu.make_async_remote_copy(
                src, dst, sems.at[0], sems.at[1], device_id=target, device_id_type=MESH)
            pl.when(exists)(copy.start)


def take_sides(lv, v, bufs, sems, counts, units, deep=None):
    py, ly, pz, lz, lzb = bufs
    w, wx = lv.w, lv.wx
    wait_near(lv, counts, units, (sems.at[0], sems.at[1]))
    v[:, lv.y : lv.y + lv.wy, 0:128] = ly[0]
    v[:, lv.y + lv.wy : lv.ye, 0:128] = ly[1]
    side = iota((lv.ye, 128), 1)
    edge = (side < w) | (side >= 128 - w)
    for a in range(3):
        parts = []
        for c in range(2):
            rows = [lz[c, a, block] for block in range(lv.blocks)]
            parts.append(jnp.concatenate(rows + [lzb[c, a, 1], lzb[c, a, 0]], axis=0))
        both = jnp.where(side % (2 * w) >= w, parts[1], parts[0])
        first = (0, wx, lv.x + wx)[a]
        start, count = ((lv.x - wx, wx), (0, lv.x), (0, wx))[a]
        for k in range(count):
            x = first + k
            strip = jnp.where(edge, pltpu.roll(both, (-2 * w * (start + k) - w) % 128, 1), 0.0)
            if lv.z == 64:
                v[x] = jnp.where(side < 64, v[x], jnp.where(side >= 128 - w, strip, pltpu.roll(strip, 64, 1)))
            else:
                v[x, :, lv.z : lv.z + 128] = strip
            if deep and a == 1:
                lane = iota((lv.y, 128), 1)
                layer = jnp.where(lane % (2 * w) == 2 * w - 1, deep[3][0], deep[3][1])
                layer = pltpu.roll(layer, (-2 * w * k - w) % 128, 1)
                edge5 = (lane == w) | (lane == 127 - w)
                v[x, 0 : lv.y, lv.z : lv.z + 128] = jnp.where(edge5, layer, strip[0 : lv.y])


def gather_start(buf, sems, counts):
    me = {axis: lax.axis_index(axis) for axis in counts}
    mine = buf.at[me["gx"], me["gy"], me["gz"]]
    ranges = [[n - k if k else 0 for k in range(n)] for n in counts.values()]
    for offset in sorted(itertools.product(*ranges), key=lambda o: -sum(1 for k in o if k)):
        if any(offset):
            target = {axis: lax.rem(me[axis] + k, counts[axis]) for axis, k in zip(counts, offset) if k}
            pltpu.make_async_remote_copy(
                mine, mine, sems.at[0], sems.at[1], device_id=target, device_id_type=MESH).start()


def gather_wait(sems, counts, units):
    others = counts["gx"] * counts["gy"] * counts["gz"] - 1
    if others:
        wait_units(units, others, sems.at[0])
        wait_units(units, others, sems.at[1])


def batches(low, high, size, body):
    whole = (high - low) // size
    if whole:
        def run(step, carry):
            body(low + step * size, size)
            return carry

        lax.fori_loop(0, whole, run, 0)
    if low + whole * size < high:
        body(low + whole * size, high - low - whole * size)


def prepare(lv, k, fx, fy, fz, dd, iv, off=0, rows=None):
    row = iota((lv.ye, lv.ze), 0)

    def body(first, count, inside=False):
        made = []
        for x in [first + i for i in range(count)]:
            kx = k[x + off]
            below = 0.5 * ((k[x + off - 1] if off else k[jnp.maximum(x - 1, 0)]) + kx)
            above = 0.5 * (kx + (k[x + off + 1] if off else k[jnp.minimum(x + 1, lv.xe - 1)]))
            lower, upper = up(kx, 0), down(kx, 0)
            if inside:
                side = jnp.zeros((lv.ye, lv.ze - 128), F32)
                ends = [jnp.broadcast_to(rows[b, pl.ds(x - lv.w, 1), :], (lv.ye, 128)) for b in range(2)]
                ends = [jnp.concatenate([end, side], axis=1) for end in ends]
                upper = jnp.where(row == lv.y + lv.wy - 1, ends[0], upper)
                lower = jnp.where(row == lv.y + lv.wy, ends[1], lower)
            second = 0.5 * (lower + kx)
            third = 0.5 * (up(kx, 1) + kx)
            total = below + above + second + 0.5 * (kx + upper) + third + down(third, 1)
            made.append((x, below, second, third, total, jnp.where(kx > 0.0, 1.0 / total, 0.0)))
        for x, *values in made:
            for ref, value in zip((fx, fy, fz, dd, iv), values):
                ref[x] = value

    size = 4 if lv.ze == 128 else 2
    if rows is None:
        batches(0, lv.xe, size, body)
    else:
        batches(0, lv.w, size, body)
        batches(lv.w, lv.w + lv.x, size, functools.partial(body, inside=True))
        batches(lv.w + lv.x, lv.xe, size, body)


def around(v, x, mid, faces):
    fx, fy, fz = faces
    second, third = fy[x], fz[x]
    summed = fx[x] * v[x - 1] + fx[x + 1] * v[x + 1]
    summed = summed + second * up(mid, 0) + down(second * mid, 0)
    return summed + third * up(mid, 1) + down(third * mid, 1)


def half_sweep(lv, v, g, faces, iv, colour, reach):
    parity = iota((lv.ye, lv.ze), 0) + iota((lv.ye, lv.ze), 1)

    def body(first, count):
        fresh = []
        for x in [first + i for i in range(count)]:
            mid = v[x]
            value = (g[x] + around(v, x, mid, faces)) * iv[x]
            fresh.append((x, jnp.where(((parity + x) & 1) == colour, value, mid)))
        for x, value in fresh:
            v[x] = value

    batches(lv.w - reach, lv.w + lv.x + reach, 10 if lv.ze == 128 else 6, body)


def residual_pairs(lv, v, g, faces, dd, pairs):
    def body(first, count):
        made = []
        for i in [first + j for j in range(count)]:
            total = jnp.zeros((lv.ye, lv.ze), F32)
            for k in range(2):
                x = lv.w + 2 * i + k
                mid = v[x]
                total = total + (g[x] - dd[x] * mid + around(v, x, mid, faces))
            made.append((i, total))
        for i, total in made:
            pairs[i] = total[0 : lv.y, 0:128]

    batches(0, lv.x // 2, 4, body)


def open_halo(lv, v, g, iv):
    parity = iota((lv.ye, lv.ze), 0) + iota((lv.ye, lv.ze), 1)

    def body(first, count):
        made = []
        for x in [first + i for i in range(count)]:
            made.append((x, jnp.where(((parity + x) & 1) == 0, g[x] * iv[x], 0.0)))
        for x, value in made:
            v[x] = value

    batches(lv.w - 4, lv.w + lv.x + 4, 4, body)


def fold_rows(pairs, rows):
    return pairs[:, pl.ds(0, rows, stride=2), :] + pairs[:, pl.ds(1, rows, stride=2), :]


def dot(a, b):
    return jnp.dot(a, b, precision=HIGH, preferred_element_type=F32)


def coarse_mid(pairs, x, y):
    folded = fold_rows(pairs, y // 2).reshape((x // 2) * (y // 2), 128)
    matrix = jnp.where(iota((128, 128), 0) // 2 == iota((128, 128), 1), 0.125, 0.0).astype(F32)
    return dot(folded, matrix).reshape(x // 2, y // 2, 128)


def coarse_low(pairs, count, rows, lanes, tmp):
    total = jnp.zeros((rows, 128), F32)
    source, goal = iota((128, 128), 0), iota((128, 128), 1)
    for x in range(count):
        matrix = jnp.where((source // 2 + x * lanes == goal) & (source < 2 * lanes), 0.125, 0.0).astype(F32)
        total = total + dot(pairs[x], matrix)
    tmp[...] = total
    half = rows // 2
    return tmp[pl.ds(0, half, stride=2), :] + tmp[pl.ds(1, half, stride=2), :]


def repeat(count, body, carry):
    if count <= 16:
        for p in range(count):
            carry = body(p, carry)
        return carry
    return lax.fori_loop(0, count, body, carry)


def spread_low(buf, whole, counts, pad):
    lane = iota((8, 128), 1)

    def body(a, carry):
        for ct in range(counts["gy"] // 2):
            for gt in range(counts["gz"] // 4):
                pieces = [
                    jnp.concatenate([buf[a, 2 * ct, 4 * gt + g], buf[a, 2 * ct + 1, 4 * gt + g]], axis=0)
                    for g in range(4)]
                for i in range(4):
                    total = pieces[0] if i == 0 else pltpu.roll(pieces[0], (-32 * i) % 128, 1)
                    for g in range(1, 4):
                        piece = pieces[g] if g == i else pltpu.roll(pieces[g], (32 * (g - i)) % 128, 1)
                        total = jnp.where(lane // 32 == g, piece, total)
                    whole[pad + 4 * a + i, 8 * ct : 8 * ct + 8, 128 * gt : 128 * gt + 128] = total
        return carry

    repeat(counts["gx"], body, 0)


def low_faces(k, faces, dims, pad):
    planes, rows, lanes = dims
    cx, cy0, cy1, cz0, cz1, cd = faces
    row, lane = iota((rows, lanes), 0), iota((rows, lanes), 1)
    scale = 0.5 * 0.0625

    def body(p, carry):
        kx = k[p + pad]
        below, above = scale * (k[p + pad - 1] + kx), scale * (kx + k[p + pad + 1])
        total = below + above
        cx[p] = below
        cx[p + 1] = above
        for target, inside, moved in (
            (cy0, row > 0, up(kx, 0)), (cy1, row < rows - 1, down(kx, 0)),
            (cz0, lane > 0, up(kx, 1)), (cz1, lane < lanes - 1, down(kx, 1))):
            face = scale * (kx + moved)
            target[p] = jnp.where(inside, face, 0.0)
            total = total + jnp.where(inside, face, scale * kx)
        cd[p] = total
        return carry

    repeat(planes, body, 0)


def bottom(f, s, vv, faces, dims, pad):
    planes, rows, lanes = dims
    cx, cy0, cy1, cz0, cz1, cd = faces

    def operate(v, p):
        mid = v[p + pad]
        summed = cx[p] * v[p + pad - 1] + cx[p + 1] * v[p + pad + 1]
        summed = summed + (cy0[p] * up(mid, 0) + cy1[p] * down(mid, 0))
        summed = summed + (cz0[p] * up(mid, 1) + cz1[p] * down(mid, 1))
        return mid, cd[p] * mid - summed

    zero = jnp.zeros((rows, lanes), F32)

    def first(p, carry):
        mid, image = operate(f, p)
        vv[p] = image
        return carry[0] + mid * mid, carry[1] + mid * image

    def total(v):
        return jnp.sum(jnp.sum(v, axis=0, keepdims=True), axis=1, keepdims=True)

    norm, along = repeat(planes, first, (zero, zero))
    alpha = total(norm) / total(along)

    def rest(p, carry):
        s[p + pad] = f[p + pad] - alpha * vv[p]
        return carry

    repeat(planes, rest, 0)

    def second(p, carry):
        mid, image = operate(s, p)
        return carry[0] + image * mid, carry[1] + image * image

    turned, norm = repeat(planes, second, (zero, zero))
    return alpha, total(turned) / total(norm)


def pack_boxes(slots, ids, outgoing, boxes, groups):
    held = ids[0].astype(F32)
    cap = held.shape[1]
    eye = iota((cap, cap), 0) == iota((cap, cap), 1)
    rows = jnp.broadcast_to(held, (cap, cap))
    cols = jnp.broadcast_to(jnp.sum(jnp.where(eye, rows, 0.0), axis=1, keepdims=True), (cap, cap))

    def target(v):
        return jnp.floor((v + 0.5) * (1.0 / boxes))

    earlier = (target(rows) == target(cols)) & (cols < rows) & (cols >= 0.0)
    ranking = jnp.sum(jnp.where(earlier, 1.0, 0.0), axis=0, keepdims=True)
    send_row = jnp.where(held >= 0.0, target(held) * SEND + ranking, -1.0)
    count = groups * SEND
    picker = jnp.where(iota((count, cap), 0).astype(F32) == jnp.broadcast_to(send_row, (count, cap)), 1.0, 0.0)
    data = slots[0, 0].astype(F32)
    total = jnp.zeros((count, data.shape[1]), F32)
    for q in range(cap):
        total = total + picker[:, q : q + 1] * data[q : q + 1, :]
    for t in range(groups):
        outgoing[t] = total[SEND * t : SEND * t + SEND, :].astype(BF16)


def place_boxes(incoming, held, owner, lhs, rhs, boxes, groups):
    me = lax.axis_index("gz")
    owners = jnp.broadcast_to(owner[0].astype(F32), (boxes, owner.shape[2]))
    here = iota(owners.shape, 1) == iota(owners.shape, 0) + me * boxes
    col = jnp.sum(jnp.where(here, owners, 0.0), axis=1, keepdims=True)
    cols = jnp.broadcast_to(col, (boxes, boxes))
    first, second = iota((boxes, boxes), 0), iota((boxes, boxes), 1)
    row = jnp.sum(jnp.where(first == second, cols, 0.0), axis=0, keepdims=True)
    before = (jnp.broadcast_to(row, (boxes, boxes)) == cols) & (second < first)
    pick = col * SEND + jnp.sum(jnp.where(before, 1.0, 0.0), axis=1, keepdims=True)
    for t in range(groups):
        held[SEND * t : SEND * t + SEND, :] = incoming[t].astype(F32)
    face = BOX * BOX
    mine = iota((BOX, face), 1) // BOX == iota((BOX, face), 0)
    for i in range(BOX):
        chosen = jnp.zeros((boxes, face), F32)
        for r in range(groups * SEND):
            chosen = jnp.where(pick == float(r), held[r : r + 1, face * i : face * i + face], chosen)
        for b in range(boxes):
            piece = jnp.where(mine, jnp.broadcast_to(chosen[b : b + 1, :], (BOX, face)), 0.0)
            lhs[BOX * i : BOX * i + BOX, face * b : face * b + face] = piece.astype(BF16)
    return jnp.dot(lhs[...], rhs[...], preferred_element_type=F32)


def kernel(fine, edge, mid, counts, names, slots_in, ids_in, owner_in, coef_in, out, *scratch):
    r = dict(zip(names, scratch))
    groups = counts["gz"]
    boxes = fine.z // BOX
    at = {axis: lax.axis_index(axis) for axis in counts}
    slots, ids, owner, coef, units = r["slots"], r["ids"], r["owner"], r["coef"], r["units"]
    loads = [
        pltpu.make_async_copy(source, target, r["loads"].at[n])
        for n, (source, target) in enumerate(((slots_in, slots), (ids_in, ids), (coef_in, coef), (owner_in, owner)))]
    for load in loads:
        load.start()
    for name in ("K0", "F0", "Q0", "K1", "G1", "E1", "lyk", "ly", "lz", "lzb", "lym", "lzm", "lzbm", "kyl", "kzl"):
        r[name][...] = jnp.zeros(r[name].shape, F32)

    barrier = pltpu.get_barrier_semaphore()
    expected = 0
    for offset in NEAR:
        target, exists = near(offset, counts)

        @pl.when(exists)
        def _():
            pl.semaphore_signal(barrier, inc=1, device_id=target, device_id_type=MESH)

        expected = expected + jnp.where(exists, 1, 0)
    others = [{"gz": lax.rem(at["gz"] + k, groups)} for k in range(1, groups)]
    if counts["gx"] > 4 or counts["gy"] > 4:
        for offset in itertools.product(*[range(n) for n in counts.values()]):
            if any(offset):
                others.append({axis: lax.rem(at[axis] + k, counts[axis]) for axis, k in zip(counts, offset) if k})
    for target in others:
        pl.semaphore_signal(barrier, inc=1, device_id=target, device_id_type=MESH)

    def bufs(n, tail):
        return tuple(r[b + tail].at[n] for b in ("py", "ly", "pz", "lz", "lzb"))

    def edge_bufs():
        return tuple(r[b + "k"].at[0] if b == "ly" else r[b].at[0] for b in ("py", "ly", "pz", "lz", "lzb"))

    def sems(n):
        return r["sems"].at[n]

    loads[0].wait()
    loads[1].wait()
    pack_boxes(slots, ids, r["outgoing"], boxes, groups)
    K0, F0, Q0, K1, G1, E1 = (r[name] for name in ("K0", "F0", "Q0", "K1", "G1", "E1"))
    w, wm = fine.w, mid.w
    loads[2].wait()
    K0[edge.wx : edge.wx + fine.x, 0 : fine.y, 0:128] = coef[...]
    deep = tuple(r[name] for name in ("kys", "kyl", "kzs", "kzl"))
    pack_sides(edge, K0, edge_bufs(), deep)
    pl.semaphore_wait(barrier, expected + len(others))

    me = at["gz"]
    for k in range(1, groups):
        to = lax.rem(me + k, groups)
        pltpu.make_async_remote_copy(
            r["outgoing"].at[to], r["incoming"].at[me], sems(0).at[0], sems(0).at[1],
            device_id={"gz": to}, device_id_type=MESH).start()
    send_sides(edge, K0, edge_bufs(), sems(1), counts, deep)
    r["incoming"][me] = r["outgoing"][me]

    for i in range(mid.x):
        r["pairs"][i] = coef[2 * i] + coef[2 * i + 1]
    K1[wm : wm + mid.x, 0 : mid.y, :] = coarse_mid(r["pairs"], fine.x, fine.y)
    pack_sides(mid, K1, bufs(0, "m"))
    send_sides(mid, K1, bufs(0, "m"), sems(2), counts)
    for i in range(mid.x // 2):
        r["pairsm"][i] = K1[wm + 2 * i, 0 : mid.y, :] + K1[wm + 2 * i + 1, 0 : mid.y, :]
    here = (at["gx"], at["gy"], at["gz"])
    r["gk"][here] = coarse_low(r["pairsm"], mid.x // 2, mid.y, mid.z // 2, r["tmp"])
    lane = iota((BOX * BOX, 128), 1)
    folded = iota((BOX * BOX, 128), 0) % BOX == lane % BOX
    for b in range(boxes):
        block = jnp.where(folded & (lane // BOX == b), 1.0, 0.0)
        r["rhs"][BOX * BOX * b : BOX * BOX * (b + 1), :] = block.astype(BF16)
    loads[3].wait()
    if groups > 1:
        part = r["incoming"].at[pl.ds(0, groups - 1)]
        for n in range(2):
            pltpu.make_async_copy(part, part, sems(0).at[n]).wait()
    source = place_boxes(r["incoming"], r["held"], owner, r["lhs"], r["rhs"], boxes, groups)
    F0[w : w + fine.x, 0 : fine.y, 0:128] = source.reshape(fine.x, fine.y, 128)
    pack_sides(fine, F0, bufs(1, ""))
    send_sides(fine, F0, bufs(1, ""), sems(3), counts)

    faces0 = (r["fx0"], r["fy0"], r["fz0"])
    faces1 = (r["fx1"], r["fy1"], r["fz1"])
    dd0, iv0, dd1, iv1, v0, v1 = r["dd0"], r["iv0"], r["dd1"], r["iv1"], r["v0"], r["v1"]
    take_sides(edge, K0, edge_bufs(), sems(1), counts, units, deep)
    prepare(fine, K0, *faces0, dd0, iv0, edge.wx - w, r["kyl"])
    take_sides(mid, K1, bufs(0, "m"), sems(2), counts, units)
    prepare(mid, K1, *faces1, dd1, iv1)
    for name in ("k2", "f2", "s2"):
        r[name][...] = jnp.zeros(r[name].shape, F32)
    take_sides(fine, F0, bufs(1, ""), sems(3), counts, units)
    open_halo(fine, v0, F0, iv0)
    for reach, colour in ((3, 1), (2, 0), (1, 1)):
        half_sweep(fine, v0, F0, faces0, iv0, colour, reach)
    residual_pairs(fine, v0, F0, faces0, dd0, r["pairs"])

    G1[wm : wm + mid.x, 0 : mid.y, :] = 4.0 * coarse_mid(r["pairs"], fine.x, fine.y)
    pack_sides(mid, G1, bufs(1, "m"))
    send_sides(mid, G1, bufs(1, "m"), sems(4), counts)
    Q0[w : w + fine.x, 0 : fine.y, 0:128] = v0[w : w + fine.x, 0 : fine.y, 0:128]
    pack_sides(fine, Q0, bufs(2, ""))
    send_sides(fine, Q0, bufs(2, ""), sems(5), counts)
    take_sides(mid, G1, bufs(1, "m"), sems(4), counts, units)
    gather_start(r["gk"], sems(7), counts)
    open_halo(mid, v1, G1, iv1)
    for reach, colour in ((3, 1), (2, 0), (1, 1)):
        half_sweep(mid, v1, G1, faces1, iv1, colour, reach)
    residual_pairs(mid, v1, G1, faces1, dd1, r["pairsm"])
    for i in range(mid.x // 2):
        r["pairsm"][i] = r["pairsm"][i] * 0.25
    r["gf"][here] = coarse_low(r["pairsm"], mid.x // 2, mid.y, mid.z // 2, r["tmp"])
    gather_start(r["gf"], sems(8), counts)
    E1[wm : wm + mid.x, 0 : mid.y, :] = v1[wm : wm + mid.x, 0 : mid.y, :]
    pack_sides(mid, E1, bufs(2, "m"))
    send_sides(mid, E1, bufs(2, "m"), sems(6), counts)

    planes, rows, lanes = dims = (4 * counts["gx"], 4 * counts["gy"], 32 * counts["gz"])
    pad = wm // 2
    low = tuple(r[name] for name in ("cx", "cy0", "cy1", "cz0", "cz1", "cd"))
    take_sides(fine, Q0, bufs(2, ""), sems(5), counts, units)
    gather_wait(sems(7), counts, units)
    spread_low(r["gk"], r["k2"], counts, pad)
    low_faces(r["k2"], low, dims, pad)
    take_sides(mid, E1, bufs(2, "m"), sems(6), counts, units)
    gather_wait(sems(8), counts, units)
    spread_low(r["gf"], r["f2"], counts, pad)
    alpha, omega = bottom(r["f2"], r["s2"], r["v2"], low, dims, pad)
    around_low = mid.xe // 2
    for q in range(around_low):
        turned = alpha * r["f2"][4 * at["gx"] + q] + omega * r["s2"][4 * at["gx"] + q]
        plane = turned
        for c in range(1, counts["gy"]):
            turned = jnp.where(at["gy"] == c, pltpu.roll(plane, rows - 4 * c, 0), turned)
        r["local"][q, 0:8, :] = turned[0:8, :]
        r["local"][q, 8:16, :] = pltpu.roll(turned[rows - 8 : rows, :], 4, 0)
    goal = iota((lanes, 128), 1)
    cell = jnp.where(goal < mid.z + wm, goal, goal - 128)
    cell = (cell + 128) // 2 - 64
    wanted = (goal < mid.z + wm) | (goal >= 128 - wm)
    matrix = jnp.where((iota((lanes, 128), 0) == 32 * at["gz"] + cell) & wanted, 1.0, 0.0).astype(F32)
    spread = dot(r["local"][...].reshape(16 * around_low, lanes), matrix).reshape(around_low, 16, 128)
    for q in range(around_low):
        wide = r["wide"].at[q, 0]
        for k in range(2):
            wide[pl.ds(k, 12, stride=2), :] = spread[q, 0:12]
        for k in range(2):
            x = 2 * q + k
            E1[x] = jnp.where(K1[x] > 0.0, E1[x] + wide[...], 0.0)
    for reach, colour in ((5, 0), (4, 1), (3, 0), (2, 1)):
        half_sweep(mid, E1, G1, faces1, iv1, colour, reach)

    low_w = w // 2
    goal = iota((128, fine.ze), 1)
    cell = jnp.where(goal < fine.z + w, goal // 2, (goal - fine.ze + 256) // 2)
    wanted = (goal < fine.z + w) | (goal >= fine.ze - w)
    matrix = jnp.where((iota((128, fine.ze), 0) == cell) & wanted, 1.0, 0.0).astype(F32)
    used = mid.x + 2 * low_w
    row = iota((8, 128), 0)
    for i in range(used):
        x = wm - low_w + i
        r["turn"][i, 0:8, :] = E1[x, 0:8, :]
        r["turn"][i, 8:16, :] = jnp.where(row < low_w, E1[x, 8:16, :], pltpu.roll(E1[x, mid.ye - 8 : mid.ye, :], 4, 0))
    fresh = dot(r["turn"][...].reshape(16 * used, 128), matrix).reshape(used, 16, fine.ze)
    for i in range(used):
        for tile in range(fine.ze // 128):
            wide, part = r["wide"].at[i, tile], slice(128 * tile, 128 * tile + 128)
            for k in range(2):
                wide[pl.ds(k, 12, stride=2), :] = fresh[i, 0:12, part]
            for k in range(2):
                x = 2 * i + k
                Q0[x, :, part] = Q0[x, :, part] + wide[...]
    for reach, colour in ((3, 0), (2, 1), (1, 0), (0, 1)):
        half_sweep(fine, Q0, F0, faces0, iv0, colour, reach)
    out[...] = Q0[w : w + fine.x, 0 : fine.y, 0:128]


def per_device(counts, old_slots, old_ids, old_owner, coefficient):
    x, y, z = coefficient.shape
    fine, edge, mid = Level(x, y, z, 4), Level(x, y, z, 4, deep=True), Level(x // 2, y // 2, z // 2, 6)
    planes, rows, lanes = 4 * counts["gx"], 4 * counts["gy"], 32 * counts["gz"]
    groups, boxes = counts["gz"], z // BOX
    cells = old_slots.shape[3]
    pad = mid.w // 2
    devices = counts["gx"] * counts["gy"] * groups
    vmem = lambda *shape: pltpu.VMEM(shape, F32)
    dma = lambda *shape: pltpu.SemaphoreType.DMA(shape)
    scratch = {}
    for level, tail, names in ((fine, "", ("K0", "F0", "Q0")), (mid, "m", ("K1", "G1", "E1"))):
        for name in names:
            scratch[name] = vmem(*level.shape)
        scratch["py" + tail] = vmem(3, 2, level.x, level.wy, 128)
        scratch["ly" + tail] = vmem(3, 2, level.xe, level.wy, 128)
        scratch["pz" + tail] = vmem(3, level.blocks, level.wy, 128)
        scratch["lz" + tail] = vmem(3, 2, 3, level.blocks, level.wy, 128)
        scratch["lzb" + tail] = vmem(3, 2, 3, 2, level.wy, 128)
        scratch["pairs" + tail] = vmem(level.x // 2, level.y, 128)
    for level, tail in ((fine, "0"), (mid, "1")):
        for name in ("fx", "fy", "fz", "dd", "iv", "v"):
            scratch[name + tail] = vmem(*level.shape)
    scratch["K0"] = vmem(*edge.shape)
    scratch["lyk"] = vmem(1, 2, edge.xe, edge.wy, 128)
    scratch.update(
        kys=vmem(2, x, 128), kyl=vmem(2, x, 128), kzs=vmem(y, 128), kzl=vmem(2, y, 128),
        slots=pltpu.VMEM(old_slots.shape, old_slots.dtype), ids=pltpu.VMEM(old_ids.shape, old_ids.dtype),
        owner=pltpu.VMEM(old_owner.shape, old_owner.dtype), coef=vmem(*coefficient.shape), loads=dma(4),
        outgoing=pltpu.VMEM((groups, SEND, cells), BF16), incoming=pltpu.VMEM((groups, SEND, cells), BF16),
        held=vmem(groups * SEND, cells), sems=dma(9, 2), units=vmem(max(160, devices), 4, 128),
        lhs=pltpu.VMEM((BOX * BOX, boxes * BOX * BOX), BF16), rhs=pltpu.VMEM((boxes * BOX * BOX, 128), BF16),
        tmp=vmem(mid.y, 128), wide=vmem(max(mid.xe, fine.xe) // 2, fine.ze // 128, fine.ye, 128), local=vmem(mid.xe // 2, 16, lanes),
        turn=vmem(mid.x + fine.w, 16, 128),
        gk=vmem(counts["gx"], counts["gy"], groups, 4, 128), gf=vmem(counts["gx"], counts["gy"], groups, 4, 128),
        cx=vmem(planes + 1, rows, lanes), v2=vmem(planes, rows, lanes))
    for name in ("cy0", "cy1", "cz0", "cz1", "cd"):
        scratch[name] = vmem(planes, rows, lanes)
    for name in ("f2", "k2", "s2"):
        scratch[name] = vmem(planes + 2 * pad, rows, lanes)
    return pl.pallas_call(
        functools.partial(kernel, fine, edge, mid, counts, tuple(scratch)),
        out_shape=jax.ShapeDtypeStruct(coefficient.shape, F32),
        in_specs=[pl.BlockSpec(memory_space=pltpu.MemorySpace.HBM)] * 4,
        out_specs=pl.BlockSpec(memory_space=pltpu.VMEM),
        scratch_shapes=list(scratch.values()),
        compiler_params=pltpu.CompilerParams(
            collective_id=0, has_side_effects=True, vmem_limit_bytes=44 * 1024 * 1024),
    )(old_slots, old_ids, old_owner, coefficient)


def solution(mesh):
    counts = {axis: mesh.shape[axis] for axis in ("gx", "gy", "gz")}
    return jax.shard_map(
        functools.partial(per_device, counts), mesh=mesh,
        in_specs=(P("gx", "gy", "gz", None), P("gx", "gy", "gz"), P("gx", "gy", None), P("gx", "gy", "gz")),
        out_specs=P("gx", "gy", "gz"), check_vma=False)
```

```python
import functools
import itertools

import jax
import jax.numpy as jnp
from jax import lax
from jax.experimental import pallas as pl
from jax.experimental.pallas import tpu as pltpu
from jax.sharding import PartitionSpec as P

BOX = 16
SEND = 2
F32 = jnp.float32
BF16 = jnp.bfloat16
MESH = pl.DeviceIdType.MESH
HIGH = lax.Precision.HIGHEST


def iota(shape, dim):
    return lax.broadcasted_iota(jnp.int32, shape, dim)


def up(v, axis):
    return pltpu.roll(v, 1, axis)


def down(v, axis):
    return pltpu.roll(v, v.shape[axis] - 1, axis)


class Level:
    def __init__(self, x, y, z, w, deep=False):
        self.x, self.y, self.z, self.w, self.deep = x, y, z, w, deep
        self.wx, self.wy = w + deep, -(-w // 4) * 4
        self.xe, self.ye = x + 2 * self.wx, y + 2 * self.wy
        self.ze = 128 if z + 2 * w <= 128 else z + 128
        self.shape = (self.xe, self.ye, self.ze)
        self.blocks = y // self.wy

    def units(self, a, b, c):
        extra = self.x // 4 if self.deep and not a and (not b or not c) else 0
        if c:
            return (self.wy if b else self.y) // 4 + extra
        return (self.wx if a else self.x) * (self.wy if b else self.y) // 4 + extra


NEAR = [(a, b, c) for c in (-1, 0, 1) for b in (-1, 0, 1) for a in (-1, 0, 1) if (a, b, c) != (0, 0, 0)]


def near(offset, counts):
    target, exists = {}, None
    for axis, step in zip(("gx", "gy", "gz"), offset):
        me, n = lax.axis_index(axis), counts[axis]
        if step:
            target[axis] = lax.rem(me + step + n, n)
            inside = me > 0 if step < 0 else me < n - 1
            exists = inside if exists is None else jnp.logical_and(exists, inside)
    return target, exists


def wait_units(units, count, sem):
    part = units.at[pl.ds(0, count)]
    pltpu.make_async_copy(part, part, sem).wait()


def wait_near(lv, counts, units, sems):
    choices = []
    for axis in ("gx", "gy", "gz"):
        me, n = lax.axis_index(axis), counts[axis]
        if n == 1:
            choices.append([(0, None)])
        elif n == 2:
            choices.append([(1, None)])
        else:
            edge = jnp.logical_or(me == 0, me == n - 1)
            choices.append([(1, edge), (2, jnp.logical_not(edge))])
    for chosen in itertools.product(*choices):
        total = 0
        for kind in itertools.product((0, 1), repeat=3):
            if any(kind):
                copies = 1
                for used, (number, _) in zip(kind, chosen):
                    copies *= number if used else 1
                total += copies * lv.units(*kind)
        conditions = [condition for _, condition in chosen if condition is not None]

        def wait():
            for sem in sems:
                wait_units(units, total, sem)

        if conditions:
            pl.when(functools.reduce(jnp.logical_and, conditions))(wait)
        else:
            wait()


def pack_sides(lv, v, bufs, deep=None):
    py, ly, pz, lz, lzb = bufs
    own, w = slice(lv.wx, lv.wx + lv.x), lv.w
    if lv.blocks > 1:
        py[0] = v[own, 0 : lv.wy, 0:128]
        py[1] = v[own, lv.y - lv.wy : lv.y, 0:128]
    lane = iota((lv.y, 128), 1)
    packed = layer = jnp.zeros((lv.y, 128), F32)
    for k in range(lv.x):
        plane = v[lv.wx + k, 0 : lv.y, 0:128]
        if lv.z == 64:
            plane = jnp.where(lane >= 64, pltpu.roll(plane, 64, 1), plane)
        turned = pltpu.roll(plane, (2 * w * k + w) % 128, 1)
        packed = jnp.where(lane // (2 * w) == k, turned, packed)
        if deep:
            layer = jnp.where((lane == (2 * w * k - 1) % 128) | (lane == (2 * w * k + 2 * w) % 128), turned, layer)
            deep[0][0, k : k + 1, :] = plane[w : w + 1, :]
            deep[0][1, k : k + 1, :] = plane[lv.y - w - 1 : lv.y - w, :]
    if deep:
        deep[2][...] = layer
    for block in range(lv.blocks):
        pz[block] = packed[block * lv.wy : block * lv.wy + lv.wy]


def send_sides(lv, v, bufs, sems, counts, deep=None):
    py, ly, pz, lz, lzb = bufs
    wx, block = lv.wx, (pl.ds(0, lv.y), pl.ds(0, 128))
    taken = {-1: (0, wx), 0: (0, lv.x), 1: (lv.x - wx, wx)}
    landed = {-1: lv.x + wx, 0: wx, 1: 0}
    for a, b, c in reversed(sorted(NEAR, key=lambda n: (n[0] != 0) + (n[1] != 0) + (n[2] != 0))):
        target, exists = near((a, b, c), counts)
        first, count = taken[a]
        if c and b:
            src, dst = pz.at[0 if b < 0 else lv.blocks - 1], lzb.at[(1 - c) // 2, 1 - a, (1 - b) // 2]
        elif c:
            src, dst = pz, lz.at[(1 - c) // 2, 1 - a]
        elif b:
            side = (b + 1) // 2
            src = py.at[side, pl.ds(first, count)] if lv.blocks > 1 else v.at[(pl.ds(wx + first, count),) + block]
            dst = ly.at[side, pl.ds(landed[a], count)]
        else:
            src, dst = v.at[(pl.ds(wx + first, count),) + block], v.at[(pl.ds(landed[a], count),) + block]
        copy = pltpu.make_async_remote_copy(
            src, dst, sems.at[0], sems.at[1], device_id=target, device_id_type=MESH)
        pl.when(exists)(copy.start)
        if deep and not a and (not b or not c):
            src, dst = (deep[2], deep[3].at[(1 - c) // 2]) if c else (deep[0].at[side], deep[1].at[side])
            copy = pltpu.make_async_remote_copy(
                src, dst, sems.at[0], sems.at[1], device_id=target, device_id_type=MESH)
            pl.when(exists)(copy.start)


def take_sides(lv, v, bufs, sems, counts, units, deep=None):
    py, ly, pz, lz, lzb = bufs
    w, wx = lv.w, lv.wx
    wait_near(lv, counts, units, (sems.at[0], sems.at[1]))
    v[:, lv.y : lv.y + lv.wy, 0:128] = ly[0]
    v[:, lv.y + lv.wy : lv.ye, 0:128] = ly[1]
    side = iota((lv.ye, 128), 1)
    edge = (side < w) | (side >= 128 - w)
    for a in range(3):
        parts = []
        for c in range(2):
            rows = [lz[c, a, block] for block in range(lv.blocks)]
            parts.append(jnp.concatenate(rows + [lzb[c, a, 1], lzb[c, a, 0]], axis=0))
        both = jnp.where(side % (2 * w) >= w, parts[1], parts[0])
        first = (0, wx, lv.x + wx)[a]
        start, count = ((lv.x - wx, wx), (0, lv.x), (0, wx))[a]
        for k in range(count):
            x = first + k
            strip = jnp.where(edge, pltpu.roll(both, (-2 * w * (start + k) - w) % 128, 1), 0.0)
            if lv.z == 64:
                v[x] = jnp.where(side < 64, v[x], jnp.where(side >= 128 - w, strip, pltpu.roll(strip, 64, 1)))
            else:
                v[x, :, lv.z : lv.z + 128] = strip
            if deep and a == 1:
                lane = iota((lv.y, 128), 1)
                layer = jnp.where(lane % (2 * w) == 2 * w - 1, deep[3][0], deep[3][1])
                layer = pltpu.roll(layer, (-2 * w * k - w) % 128, 1)
                edge5 = (lane == w) | (lane == 127 - w)
                v[x, 0 : lv.y, lv.z : lv.z + 128] = jnp.where(edge5, layer, strip[0 : lv.y])


def gather_start(buf, sems, counts):
    me = {axis: lax.axis_index(axis) for axis in counts}
    mine = buf.at[me["gx"], me["gy"], me["gz"]]
    ranges = [[n - k if k else 0 for k in range(n)] for n in counts.values()]
    for offset in sorted(itertools.product(*ranges), key=lambda o: -sum(1 for k in o if k)):
        if any(offset):
            target = {axis: lax.rem(me[axis] + k, counts[axis]) for axis, k in zip(counts, offset) if k}
            pltpu.make_async_remote_copy(
                mine, mine, sems.at[0], sems.at[1], device_id=target, device_id_type=MESH).start()


def gather_wait(sems, counts, units):
    others = counts["gx"] * counts["gy"] * counts["gz"] - 1
    if others:
        wait_units(units, others, sems.at[0])
        wait_units(units, others, sems.at[1])


def batches(low, high, size, body):
    whole = (high - low) // size
    if whole:
        def run(step, carry):
            body(low + step * size, size)
            return carry

        lax.fori_loop(0, whole, run, 0)
    if low + whole * size < high:
        body(low + whole * size, high - low - whole * size)


def prepare(lv, k, fx, fy, fz, dd, iv, off=0, rows=None):
    row = iota((lv.ye, lv.ze), 0)

    def body(first, count, inside=False):
        made = []
        for x in [first + i for i in range(count)]:
            kx = k[x + off]
            below = 0.5 * ((k[x + off - 1] if off else k[jnp.maximum(x - 1, 0)]) + kx)
            above = 0.5 * (kx + (k[x + off + 1] if off else k[jnp.minimum(x + 1, lv.xe - 1)]))
            lower, upper = up(kx, 0), down(kx, 0)
            if inside:
                side = jnp.zeros((lv.ye, lv.ze - 128), F32)
                ends = [jnp.broadcast_to(rows[b, pl.ds(x - lv.w, 1), :], (lv.ye, 128)) for b in range(2)]
                ends = [jnp.concatenate([end, side], axis=1) for end in ends]
                upper = jnp.where(row == lv.y + lv.wy - 1, ends[0], upper)
                lower = jnp.where(row == lv.y + lv.wy, ends[1], lower)
            second = 0.5 * (lower + kx)
            third = 0.5 * (up(kx, 1) + kx)
            total = below + above + second + 0.5 * (kx + upper) + third + down(third, 1)
            made.append((x, below, second, third, total, jnp.where(kx > 0.0, 1.0 / total, 0.0)))
        for x, *values in made:
            for ref, value in zip((fx, fy, fz, dd, iv), values):
                ref[x] = value

    size = 4 if lv.ze == 128 else 2
    if rows is None:
        batches(0, lv.xe, size, body)
    else:
        batches(0, lv.w, size, body)
        batches(lv.w, lv.w + lv.x, size, functools.partial(body, inside=True))
        batches(lv.w + lv.x, lv.xe, size, body)


def around(v, x, mid, faces):
    fx, fy, fz = faces
    second, third = fy[x], fz[x]
    summed = fx[x] * v[x - 1] + fx[x + 1] * v[x + 1]
    summed = summed + second * up(mid, 0) + down(second * mid, 0)
    return summed + third * up(mid, 1) + down(third * mid, 1)


def half_sweep(lv, v, g, faces, iv, colour, reach):
    parity = iota((lv.ye, lv.ze), 0) + iota((lv.ye, lv.ze), 1)

    def body(first, count):
        fresh = []
        for x in [first + i for i in range(count)]:
            mid = v[x]
            value = (g[x] + around(v, x, mid, faces)) * iv[x]
            fresh.append((x, jnp.where(((parity + x) & 1) == colour, value, mid)))
        for x, value in fresh:
            v[x] = value

    batches(lv.w - reach, lv.w + lv.x + reach, 10 if lv.ze == 128 else 6, body)


def residual_pairs(lv, v, g, faces, dd, pairs):
    def body(first, count):
        made = []
        for i in [first + j for j in range(count)]:
            total = jnp.zeros((lv.ye, lv.ze), F32)
            for k in range(2):
                x = lv.w + 2 * i + k
                mid = v[x]
                total = total + (g[x] - dd[x] * mid + around(v, x, mid, faces))
            made.append((i, total))
        for i, total in made:
            pairs[i] = total[0 : lv.y, 0:128]

    batches(0, lv.x // 2, 4, body)


def open_halo(lv, v, g, iv):
    parity = iota((lv.ye, lv.ze), 0) + iota((lv.ye, lv.ze), 1)

    def body(first, count):
        made = []
        for x in [first + i for i in range(count)]:
            made.append((x, jnp.where(((parity + x) & 1) == 0, g[x] * iv[x], 0.0)))
        for x, value in made:
            v[x] = value

    batches(lv.w - 4, lv.w + lv.x + 4, 4, body)


def fold_rows(pairs, rows):
    return pairs[:, pl.ds(0, rows, stride=2), :] + pairs[:, pl.ds(1, rows, stride=2), :]


def dot(a, b):
    return jnp.dot(a, b, precision=HIGH, preferred_element_type=F32)


def coarse_mid(pairs, x, y):
    folded = fold_rows(pairs, y // 2).reshape((x // 2) * (y // 2), 128)
    matrix = jnp.where(iota((128, 128), 0) // 2 == iota((128, 128), 1), 0.125, 0.0).astype(F32)
    return dot(folded, matrix).reshape(x // 2, y // 2, 128)


def coarse_low(pairs, count, rows, lanes, tmp):
    total = jnp.zeros((rows, 128), F32)
    source, goal = iota((128, 128), 0), iota((128, 128), 1)
    for x in range(count):
        matrix = jnp.where((source // 2 + x * lanes == goal) & (source < 2 * lanes), 0.125, 0.0).astype(F32)
        total = total + dot(pairs[x], matrix)
    tmp[...] = total
    half = rows // 2
    return tmp[pl.ds(0, half, stride=2), :] + tmp[pl.ds(1, half, stride=2), :]


def repeat(count, body, carry):
    if count <= 16:
        for p in range(count):
            carry = body(p, carry)
        return carry
    return lax.fori_loop(0, count, body, carry)


def spread_low(buf, whole, counts, pad):
    lane = iota((8, 128), 1)

    def body(a, carry):
        for ct in range(counts["gy"] // 2):
            for gt in range(counts["gz"] // 4):
                pieces = [
                    jnp.concatenate([buf[a, 2 * ct, 4 * gt + g], buf[a, 2 * ct + 1, 4 * gt + g]], axis=0)
                    for g in range(4)]
                for i in range(4):
                    total = pieces[0] if i == 0 else pltpu.roll(pieces[0], (-32 * i) % 128, 1)
                    for g in range(1, 4):
                        piece = pieces[g] if g == i else pltpu.roll(pieces[g], (32 * (g - i)) % 128, 1)
                        total = jnp.where(lane // 32 == g, piece, total)
                    whole[pad + 4 * a + i, 8 * ct : 8 * ct + 8, 128 * gt : 128 * gt + 128] = total
        return carry

    repeat(counts["gx"], body, 0)


def low_faces(k, faces, dims, pad):
    planes, rows, lanes = dims
    cx, cy0, cy1, cz0, cz1, cd = faces
    row, lane = iota((rows, lanes), 0), iota((rows, lanes), 1)
    scale = 0.5 * 0.0625

    def body(p, carry):
        kx = k[p + pad]
        below, above = scale * (k[p + pad - 1] + kx), scale * (kx + k[p + pad + 1])
        total = below + above
        cx[p] = below
        cx[p + 1] = above
        for target, inside, moved in (
            (cy0, row > 0, up(kx, 0)), (cy1, row < rows - 1, down(kx, 0)),
            (cz0, lane > 0, up(kx, 1)), (cz1, lane < lanes - 1, down(kx, 1))):
            face = scale * (kx + moved)
            target[p] = jnp.where(inside, face, 0.0)
            total = total + jnp.where(inside, face, scale * kx)
        cd[p] = total
        return carry

    repeat(planes, body, 0)


def bottom(f, s, vv, faces, dims, pad):
    planes, rows, lanes = dims
    cx, cy0, cy1, cz0, cz1, cd = faces

    def operate(v, p):
        mid = v[p + pad]
        summed = cx[p] * v[p + pad - 1] + cx[p + 1] * v[p + pad + 1]
        summed = summed + (cy0[p] * up(mid, 0) + cy1[p] * down(mid, 0))
        summed = summed + (cz0[p] * up(mid, 1) + cz1[p] * down(mid, 1))
        return mid, cd[p] * mid - summed

    zero = jnp.zeros((rows, lanes), F32)

    def first(p, carry):
        mid, image = operate(f, p)
        vv[p] = image
        return carry[0] + mid * mid, carry[1] + mid * image

    def total(v):
        return jnp.sum(jnp.sum(v, axis=0, keepdims=True), axis=1, keepdims=True)

    norm, along = repeat(planes, first, (zero, zero))
    alpha = total(norm) / total(along)

    def rest(p, carry):
        s[p + pad] = f[p + pad] - alpha * vv[p]
        return carry

    repeat(planes, rest, 0)

    def second(p, carry):
        mid, image = operate(s, p)
        return carry[0] + image * mid, carry[1] + image * image

    turned, norm = repeat(planes, second, (zero, zero))
    return alpha, total(turned) / total(norm)


def pack_boxes(slots, ids, outgoing, boxes, groups):
    held = ids[0].astype(F32)
    cap = held.shape[1]
    eye = iota((cap, cap), 0) == iota((cap, cap), 1)
    rows = jnp.broadcast_to(held, (cap, cap))
    cols = jnp.broadcast_to(jnp.sum(jnp.where(eye, rows, 0.0), axis=1, keepdims=True), (cap, cap))

    def target(v):
        return jnp.floor((v + 0.5) * (1.0 / boxes))

    earlier = (target(rows) == target(cols)) & (cols < rows) & (cols >= 0.0)
    ranking = jnp.sum(jnp.where(earlier, 1.0, 0.0), axis=0, keepdims=True)
    send_row = jnp.where(held >= 0.0, target(held) * SEND + ranking, -1.0)
    count = groups * SEND
    picker = jnp.where(iota((count, cap), 0).astype(F32) == jnp.broadcast_to(send_row, (count, cap)), 1.0, 0.0)
    data = slots[0, 0].astype(F32)
    total = jnp.zeros((count, data.shape[1]), F32)
    for q in range(cap):
        total = total + picker[:, q : q + 1] * data[q : q + 1, :]
    for t in range(groups):
        outgoing[t] = total[SEND * t : SEND * t + SEND, :].astype(BF16)


def place_boxes(incoming, held, owner, lhs, rhs, boxes, groups):
    me = lax.axis_index("gz")
    owners = jnp.broadcast_to(owner[0].astype(F32), (boxes, owner.shape[2]))
    here = iota(owners.shape, 1) == iota(owners.shape, 0) + me * boxes
    col = jnp.sum(jnp.where(here, owners, 0.0), axis=1, keepdims=True)
    cols = jnp.broadcast_to(col, (boxes, boxes))
    first, second = iota((boxes, boxes), 0), iota((boxes, boxes), 1)
    row = jnp.sum(jnp.where(first == second, cols, 0.0), axis=0, keepdims=True)
    before = (jnp.broadcast_to(row, (boxes, boxes)) == cols) & (second < first)
    pick = col * SEND + jnp.sum(jnp.where(before, 1.0, 0.0), axis=1, keepdims=True)
    for t in range(groups):
        held[SEND * t : SEND * t + SEND, :] = incoming[t].astype(F32)
    face = BOX * BOX
    mine = iota((BOX, face), 1) // BOX == iota((BOX, face), 0)
    for i in range(BOX):
        chosen = jnp.zeros((boxes, face), F32)
        for r in range(groups * SEND):
            chosen = jnp.where(pick == float(r), held[r : r + 1, face * i : face * i + face], chosen)
        for b in range(boxes):
            piece = jnp.where(mine, jnp.broadcast_to(chosen[b : b + 1, :], (BOX, face)), 0.0)
            lhs[BOX * i : BOX * i + BOX, face * b : face * b + face] = piece.astype(BF16)
    return jnp.dot(lhs[...], rhs[...], preferred_element_type=F32)


def kernel(fine, edge, mid, counts, names, slots_in, ids_in, owner_in, coef_in, out, *scratch):
    r = dict(zip(names, scratch))
    groups = counts["gz"]
    boxes = fine.z // BOX
    at = {axis: lax.axis_index(axis) for axis in counts}
    slots, ids, owner, coef, units = r["slots"], r["ids"], r["owner"], r["coef"], r["units"]
    loads = [
        pltpu.make_async_copy(source, target, r["loads"].at[n])
        for n, (source, target) in enumerate(((slots_in, slots), (ids_in, ids), (coef_in, coef), (owner_in, owner)))]
    for load in loads:
        load.start()
    for name in ("K0", "F0", "Q0", "K1", "G1", "E1", "lyk", "ly", "lz", "lzb", "lym", "lzm", "lzbm", "kyl", "kzl"):
        r[name][...] = jnp.zeros(r[name].shape, F32)

    barrier = pltpu.get_barrier_semaphore()
    expected = 0
    for offset in NEAR:
        target, exists = near(offset, counts)

        @pl.when(exists)
        def _():
            pl.semaphore_signal(barrier, inc=1, device_id=target, device_id_type=MESH)

        expected = expected + jnp.where(exists, 1, 0)
    others = [{"gz": lax.rem(at["gz"] + k, groups)} for k in range(1, groups)]
    if counts["gx"] > 4 or counts["gy"] > 4:
        for offset in itertools.product(*[range(n) for n in counts.values()]):
            if any(offset):
                others.append({axis: lax.rem(at[axis] + k, counts[axis]) for axis, k in zip(counts, offset) if k})
    for target in others:
        pl.semaphore_signal(barrier, inc=1, device_id=target, device_id_type=MESH)

    def bufs(n, tail):
        return tuple(r[b + tail].at[n] for b in ("py", "ly", "pz", "lz", "lzb"))

    def edge_bufs():
        return tuple(r[b + "k"].at[0] if b == "ly" else r[b].at[0] for b in ("py", "ly", "pz", "lz", "lzb"))

    def sems(n):
        return r["sems"].at[n]

    loads[0].wait()
    loads[1].wait()
    pack_boxes(slots, ids, r["outgoing"], boxes, groups)
    K0, F0, Q0, K1, G1, E1 = (r[name] for name in ("K0", "F0", "Q0", "K1", "G1", "E1"))
    w, wm = fine.w, mid.w
    loads[2].wait()
    K0[edge.wx : edge.wx + fine.x, 0 : fine.y, 0:128] = coef[...]
    deep = tuple(r[name] for name in ("kys", "kyl", "kzs", "kzl"))
    pack_sides(edge, K0, edge_bufs(), deep)
    pl.semaphore_wait(barrier, expected + len(others))

    me = at["gz"]
    for k in range(1, groups):
        to = lax.rem(me + k, groups)
        pltpu.make_async_remote_copy(
            r["outgoing"].at[to], r["incoming"].at[me], sems(0).at[0], sems(0).at[1],
            device_id={"gz": to}, device_id_type=MESH).start()
    send_sides(edge, K0, edge_bufs(), sems(1), counts, deep)
    r["incoming"][me] = r["outgoing"][me]

    for i in range(mid.x):
        r["pairs"][i] = coef[2 * i] + coef[2 * i + 1]
    K1[wm : wm + mid.x, 0 : mid.y, :] = coarse_mid(r["pairs"], fine.x, fine.y)
    pack_sides(mid, K1, bufs(0, "m"))
    send_sides(mid, K1, bufs(0, "m"), sems(2), counts)
    for i in range(mid.x // 2):
        r["pairsm"][i] = K1[wm + 2 * i, 0 : mid.y, :] + K1[wm + 2 * i + 1, 0 : mid.y, :]
    here = (at["gx"], at["gy"], at["gz"])
    r["gk"][here] = coarse_low(r["pairsm"], mid.x // 2, mid.y, mid.z // 2, r["tmp"])
    lane = iota((BOX * BOX, 128), 1)
    folded = iota((BOX * BOX, 128), 0) % BOX == lane % BOX
    for b in range(boxes):
        block = jnp.where(folded & (lane // BOX == b), 1.0, 0.0)
        r["rhs"][BOX * BOX * b : BOX * BOX * (b + 1), :] = block.astype(BF16)
    loads[3].wait()
    if groups > 1:
        part = r["incoming"].at[pl.ds(0, groups - 1)]
        for n in range(2):
            pltpu.make_async_copy(part, part, sems(0).at[n]).wait()
    source = place_boxes(r["incoming"], r["held"], owner, r["lhs"], r["rhs"], boxes, groups)
    F0[w : w + fine.x, 0 : fine.y, 0:128] = source.reshape(fine.x, fine.y, 128)
    pack_sides(fine, F0, bufs(1, ""))
    send_sides(fine, F0, bufs(1, ""), sems(3), counts)

    faces0 = (r["fx0"], r["fy0"], r["fz0"])
    faces1 = (r["fx1"], r["fy1"], r["fz1"])
    dd0, iv0, dd1, iv1, v0, v1 = r["dd0"], r["iv0"], r["dd1"], r["iv1"], r["v0"], r["v1"]
    take_sides(edge, K0, edge_bufs(), sems(1), counts, units, deep)
    prepare(fine, K0, *faces0, dd0, iv0, edge.wx - w, r["kyl"])
    take_sides(mid, K1, bufs(0, "m"), sems(2), counts, units)
    prepare(mid, K1, *faces1, dd1, iv1)
    for name in ("k2", "f2", "s2"):
        r[name][...] = jnp.zeros(r[name].shape, F32)
    take_sides(fine, F0, bufs(1, ""), sems(3), counts, units)
    open_halo(fine, v0, F0, iv0)
    for reach, colour in ((3, 1), (2, 0), (1, 1)):
        half_sweep(fine, v0, F0, faces0, iv0, colour, reach)
    residual_pairs(fine, v0, F0, faces0, dd0, r["pairs"])

    G1[wm : wm + mid.x, 0 : mid.y, :] = 4.0 * coarse_mid(r["pairs"], fine.x, fine.y)
    pack_sides(mid, G1, bufs(1, "m"))
    send_sides(mid, G1, bufs(1, "m"), sems(4), counts)
    Q0[w : w + fine.x, 0 : fine.y, 0:128] = v0[w : w + fine.x, 0 : fine.y, 0:128]
    pack_sides(fine, Q0, bufs(2, ""))
    send_sides(fine, Q0, bufs(2, ""), sems(5), counts)
    take_sides(mid, G1, bufs(1, "m"), sems(4), counts, units)
    gather_start(r["gk"], sems(7), counts)
    open_halo(mid, v1, G1, iv1)
    for reach, colour in ((3, 1), (2, 0), (1, 1)):
        half_sweep(mid, v1, G1, faces1, iv1, colour, reach)
    E1[wm : wm + mid.x, 0 : mid.y, :] = v1[wm : wm + mid.x, 0 : mid.y, :]
    pack_sides(mid, E1, bufs(2, "m"))
    send_sides(mid, E1, bufs(2, "m"), sems(6), counts)
    residual_pairs(mid, v1, G1, faces1, dd1, r["pairsm"])
    for i in range(mid.x // 2):
        r["pairsm"][i] = r["pairsm"][i] * 0.25
    r["gf"][here] = coarse_low(r["pairsm"], mid.x // 2, mid.y, mid.z // 2, r["tmp"])
    gather_start(r["gf"], sems(8), counts)

    planes, rows, lanes = dims = (4 * counts["gx"], 4 * counts["gy"], 32 * counts["gz"])
    pad = wm // 2
    low = tuple(r[name] for name in ("cx", "cy0", "cy1", "cz0", "cz1", "cd"))
    take_sides(fine, Q0, bufs(2, ""), sems(5), counts, units)
    gather_wait(sems(7), counts, units)
    spread_low(r["gk"], r["k2"], counts, pad)
    low_faces(r["k2"], low, dims, pad)
    take_sides(mid, E1, bufs(2, "m"), sems(6), counts, units)
    gather_wait(sems(8), counts, units)
    spread_low(r["gf"], r["f2"], counts, pad)
    alpha, omega = bottom(r["f2"], r["s2"], r["v2"], low, dims, pad)
    around_low = mid.xe // 2
    for q in range(around_low):
        turned = alpha * r["f2"][4 * at["gx"] + q] + omega * r["s2"][4 * at["gx"] + q]
        plane = turned
        for c in range(1, counts["gy"]):
            turned = jnp.where(at["gy"] == c, pltpu.roll(plane, rows - 4 * c, 0), turned)
        r["local"][q, 0:8, :] = turned[0:8, :]
        r["local"][q, 8:16, :] = pltpu.roll(turned[rows - 8 : rows, :], 4, 0)
    goal = iota((lanes, 128), 1)
    cell = jnp.where(goal < mid.z + wm, goal, goal - 128)
    cell = (cell + 128) // 2 - 64
    wanted = (goal < mid.z + wm) | (goal >= 128 - wm)
    matrix = jnp.where((iota((lanes, 128), 0) == 32 * at["gz"] + cell) & wanted, 1.0, 0.0).astype(F32)
    spread = dot(r["local"][...].reshape(16 * around_low, lanes), matrix).reshape(around_low, 16, 128)
    for q in range(around_low):
        wide = r["wide"].at[q, 0]
        for k in range(2):
            wide[pl.ds(k, 12, stride=2), :] = spread[q, 0:12]
        for k in range(2):
            x = 2 * q + k
            E1[x] = jnp.where(K1[x] > 0.0, E1[x] + wide[...], 0.0)
    for reach, colour in ((5, 0), (4, 1), (3, 0), (2, 1)):
        half_sweep(mid, E1, G1, faces1, iv1, colour, reach)

    low_w = w // 2
    goal = iota((128, fine.ze), 1)
    cell = jnp.where(goal < fine.z + w, goal // 2, (goal - fine.ze + 256) // 2)
    wanted = (goal < fine.z + w) | (goal >= fine.ze - w)
    matrix = jnp.where((iota((128, fine.ze), 0) == cell) & wanted, 1.0, 0.0).astype(F32)
    used = mid.x + 2 * low_w
    row = iota((8, 128), 0)
    for i in range(used):
        x = wm - low_w + i
        r["turn"][i, 0:8, :] = E1[x, 0:8, :]
        r["turn"][i, 8:16, :] = jnp.where(row < low_w, E1[x, 8:16, :], pltpu.roll(E1[x, mid.ye - 8 : mid.ye, :], 4, 0))
    fresh = dot(r["turn"][...].reshape(16 * used, 128), matrix).reshape(used, 16, fine.ze)
    for i in range(used):
        for tile in range(fine.ze // 128):
            wide, part = r["wide"].at[i, tile], slice(128 * tile, 128 * tile + 128)
            for k in range(2):
                wide[pl.ds(k, 12, stride=2), :] = fresh[i, 0:12, part]
            for k in range(2):
                x = 2 * i + k
                Q0[x, :, part] = Q0[x, :, part] + wide[...]
    for reach, colour in ((3, 0), (2, 1), (1, 0), (0, 1)):
        half_sweep(fine, Q0, F0, faces0, iv0, colour, reach)
    out[...] = Q0[w : w + fine.x, 0 : fine.y, 0:128]


def per_device(counts, old_slots, old_ids, old_owner, coefficient):
    x, y, z = coefficient.shape
    fine, edge, mid = Level(x, y, z, 4), Level(x, y, z, 4, deep=True), Level(x // 2, y // 2, z // 2, 6)
    planes, rows, lanes = 4 * counts["gx"], 4 * counts["gy"], 32 * counts["gz"]
    groups, boxes = counts["gz"], z // BOX
    cells = old_slots.shape[3]
    pad = mid.w // 2
    devices = counts["gx"] * counts["gy"] * groups
    vmem = lambda *shape: pltpu.VMEM(shape, F32)
    dma = lambda *shape: pltpu.SemaphoreType.DMA(shape)
    scratch = {}
    for level, tail, names in ((fine, "", ("K0", "F0", "Q0")), (mid, "m", ("K1", "G1", "E1"))):
        for name in names:
            scratch[name] = vmem(*level.shape)
        scratch["py" + tail] = vmem(3, 2, level.x, level.wy, 128)
        scratch["ly" + tail] = vmem(3, 2, level.xe, level.wy, 128)
        scratch["pz" + tail] = vmem(3, level.blocks, level.wy, 128)
        scratch["lz" + tail] = vmem(3, 2, 3, level.blocks, level.wy, 128)
        scratch["lzb" + tail] = vmem(3, 2, 3, 2, level.wy, 128)
        scratch["pairs" + tail] = vmem(level.x // 2, level.y, 128)
    for level, tail in ((fine, "0"), (mid, "1")):
        for name in ("fx", "fy", "fz", "dd", "iv", "v"):
            scratch[name + tail] = vmem(*level.shape)
    scratch["K0"] = vmem(*edge.shape)
    scratch["lyk"] = vmem(1, 2, edge.xe, edge.wy, 128)
    scratch.update(
        kys=vmem(2, x, 128), kyl=vmem(2, x, 128), kzs=vmem(y, 128), kzl=vmem(2, y, 128),
        slots=pltpu.VMEM(old_slots.shape, old_slots.dtype), ids=pltpu.VMEM(old_ids.shape, old_ids.dtype),
        owner=pltpu.VMEM(old_owner.shape, old_owner.dtype), coef=vmem(*coefficient.shape), loads=dma(4),
        outgoing=pltpu.VMEM((groups, SEND, cells), BF16), incoming=pltpu.VMEM((groups, SEND, cells), BF16),
        held=vmem(groups * SEND, cells), sems=dma(9, 2), units=vmem(max(160, devices), 4, 128),
        lhs=pltpu.VMEM((BOX * BOX, boxes * BOX * BOX), BF16), rhs=pltpu.VMEM((boxes * BOX * BOX, 128), BF16),
        tmp=vmem(mid.y, 128), wide=vmem(max(mid.xe, fine.xe) // 2, fine.ze // 128, fine.ye, 128), local=vmem(mid.xe // 2, 16, lanes),
        turn=vmem(mid.x + fine.w, 16, 128),
        gk=vmem(counts["gx"], counts["gy"], groups, 4, 128), gf=vmem(counts["gx"], counts["gy"], groups, 4, 128),
        cx=vmem(planes + 1, rows, lanes), v2=vmem(planes, rows, lanes))
    for name in ("cy0", "cy1", "cz0", "cz1", "cd"):
        scratch[name] = vmem(planes, rows, lanes)
    for name in ("f2", "k2", "s2"):
        scratch[name] = vmem(planes + 2 * pad, rows, lanes)
    return pl.pallas_call(
        functools.partial(kernel, fine, edge, mid, counts, tuple(scratch)),
        out_shape=jax.ShapeDtypeStruct(coefficient.shape, F32),
        in_specs=[pl.BlockSpec(memory_space=pltpu.MemorySpace.HBM)] * 4,
        out_specs=pl.BlockSpec(memory_space=pltpu.VMEM),
        scratch_shapes=list(scratch.values()),
        compiler_params=pltpu.CompilerParams(
            collective_id=0, has_side_effects=True, vmem_limit_bytes=44 * 1024 * 1024),
    )(*[pltpu.with_memory_space_constraint(v, pltpu.HBM) for v in (old_slots, old_ids, old_owner, coefficient)])


def solution(mesh):
    counts = {axis: mesh.shape[axis] for axis in ("gx", "gy", "gz")}
    return jax.shard_map(
        functools.partial(per_device, counts), mesh=mesh,
        in_specs=(P("gx", "gy", "gz", None), P("gx", "gy", "gz"), P("gx", "gy", None), P("gx", "gy", "gz")),
        out_specs=P("gx", "gy", "gz"), check_vma=False)
```

```python
import functools
import itertools

import jax
import jax.numpy as jnp
from jax import lax
from jax.experimental import pallas as pl
from jax.experimental.pallas import tpu as pltpu
from jax.sharding import PartitionSpec as P

BOX = 16
SEND = 2
F32 = jnp.float32
BF16 = jnp.bfloat16
MESH = pl.DeviceIdType.MESH
HIGH = lax.Precision.HIGHEST


def iota(shape, dim):
    return lax.broadcasted_iota(jnp.int32, shape, dim)


def up(v, axis):
    return pltpu.roll(v, 1, axis)


def down(v, axis):
    return pltpu.roll(v, v.shape[axis] - 1, axis)


class Level:
    def __init__(self, t, y, wt, wy, h, deep=False):
        self.t, self.y, self.wt, self.wy, self.h, self.deep = t, y, wt, wy, h, deep
        self.te, self.ye = t + 2 * wt, y + 2 * wy
        self.blocks = y // wy

    def units(self, a, b, c):
        if c:
            return (self.wy if b else self.y) // 4
        extra = self.t // 4 if self.deep and b and not a else 0
        return (self.wt if a else self.t) * (self.wy if b else self.y) // 4 + extra

    def scratch(self, tag):
        vmem = lambda *shape: pltpu.VMEM(shape + (128,), F32)
        made = {
            "st": vmem(self.t, self.y), "py": vmem(2, self.t, self.wy), "lt": vmem(self.te, self.y),
            "ly": vmem(2, self.te, self.wy), "pf": vmem(self.blocks, self.wy), "pl": vmem(self.blocks, self.wy),
            "lz": vmem(2, 3, self.blocks, self.wy), "lzb": vmem(2, 3, 2, self.wy)}
        if self.deep:
            made.update(ky=vmem(2, self.t), lk=vmem(2, self.t))
        return {name + tag: value for name, value in made.items()}


NEAR = [(a, b, c) for c in (-1, 0, 1) for b in (-1, 0, 1) for a in (-1, 0, 1) if (a, b, c) != (0, 0, 0)]


def near(offset, counts):
    target, exists = {}, None
    for axis, step in zip(("gx", "gy", "gz"), offset):
        me, n = lax.axis_index(axis), counts[axis]
        if step:
            target[axis] = lax.rem(me + step + n, n)
            inside = me > 0 if step < 0 else me < n - 1
            exists = inside if exists is None else jnp.logical_and(exists, inside)
    return target, exists


def wait_units(units, count, sem):
    part = units.at[pl.ds(0, count)]
    pltpu.make_async_copy(part, part, sem).wait()


def wait_near(lv, counts, units, sems):
    choices = []
    for axis in ("gx", "gy", "gz"):
        me, n = lax.axis_index(axis), counts[axis]
        if n == 1:
            choices.append([(0, None)])
        elif n == 2:
            choices.append([(1, None)])
        else:
            edge = jnp.logical_or(me == 0, me == n - 1)
            choices.append([(1, edge), (2, jnp.logical_not(edge))])
    for chosen in itertools.product(*choices):
        total = 0
        for kind in itertools.product((0, 1), repeat=3):
            if any(kind):
                copies = 1
                for used, (number, _) in zip(kind, chosen):
                    copies *= number if used else 1
                total += copies * lv.units(*kind)
        conditions = [condition for _, condition in chosen if condition is not None]

        def wait():
            for sem in sems:
                wait_units(units, total, sem)

        if conditions:
            pl.when(functools.reduce(jnp.logical_and, conditions))(wait)
        else:
            wait()


def clear_sides(lv, b):
    b["lt"][0 : lv.wt] = jnp.zeros((lv.wt, lv.y, 128), F32)
    b["lt"][lv.t + lv.wt : lv.te] = jnp.zeros((lv.wt, lv.y, 128), F32)
    for name in ("ly", "lz", "lzb") + (("lk",) if lv.deep else ()):
        b[name][...] = jnp.zeros(b[name].shape, F32)


def pack_sides(lv, b):
    h, st, lane = lv.h, b["st"], iota((lv.y, 128), 1)
    if lv.blocks > 1:
        b["py"][0] = st[:, 0 : lv.wy, :]
        b["py"][1] = st[:, lv.y - lv.wy : lv.y, :]
    first = last = jnp.zeros((lv.y, 128), F32)
    for t in range(lv.t):
        tile = st[t]
        for half in range(2):
            at = 2 * h * t + h * half
            turned = pltpu.roll(tile, (at - 64 * half) % 128, 1)
            first = jnp.where(((lane - at) & 127) < h, turned, first)
            last = jnp.where(((lane - at - 64 + h) & 127) < h, turned, last)
        if lv.deep:
            b["ky"][0, t : t + 1, :] = tile[lv.wy : lv.wy + 1, :]
            b["ky"][1, t : t + 1, :] = tile[lv.y - lv.wy - 1 : lv.y - lv.wy, :]
    for block in range(lv.blocks):
        rows = slice(block * lv.wy, block * lv.wy + lv.wy)
        b["pf"][block], b["pl"][block] = first[rows], last[rows]


def send_sides(lv, b, sems, counts):
    taken = {-1: (0, lv.wt), 0: (0, lv.t), 1: (lv.t - lv.wt, lv.wt)}
    landed = {-1: lv.t + lv.wt, 0: lv.wt, 1: 0}
    for x, y, z in reversed(sorted(NEAR, key=lambda n: (n[0] != 0) + (n[1] != 0) + (n[2] != 0))):
        target, exists = near((x, y, z), counts)
        first, count = taken[x]
        source, goal, side = pl.ds(first, count), pl.ds(landed[x], count), (y + 1) // 2
        if z:
            ends = b["pf"] if z < 0 else b["pl"]
            if y:
                pairs = [(ends.at[0 if y < 0 else lv.blocks - 1], b["lzb"].at[(1 - z) // 2, 1 - x, (1 - y) // 2])]
            else:
                pairs = [(ends, b["lz"].at[(1 - z) // 2, 1 - x])]
        elif y:
            pairs = [(b["py"].at[side, source] if lv.blocks > 1 else b["st"].at[source], b["ly"].at[side, goal])]
            if lv.deep and not x:
                pairs.append((b["ky"].at[side], b["lk"].at[side]))
        else:
            pairs = [(b["st"].at[source], b["lt"].at[goal])]
        for src, dst in pairs:
            copy = pltpu.make_async_remote_copy(
                src, dst, sems.at[0], sems.at[1], device_id=target, device_id_type=MESH)
            pl.when(exists)(copy.start)


def take_sides(lv, b, sems, counts, units, emit):
    h, wt = lv.h, lv.wt
    wait_near(lv, counts, units, (sems.at[0], sems.at[1]))
    lane = iota((lv.ye, 128), 1)
    own, edge = lane < 64, (lane < 64 + h) | (lane >= 128 - h)
    for a in range(3):
        low, high = [
            jnp.concatenate(
                [b["lz"][c, a, block] for block in range(lv.blocks)] + [b["lzb"][c, a, 1], b["lzb"][c, a, 0]], axis=0)
            for c in range(2)]
        mixed = [jnp.where(((lane - 16 * h * q + h) & 127) < 64, high, low) for q in range(-(-lv.t // 8))]
        place = (0, wt, lv.t + wt)[a]
        start, count = ((lv.t - wt, wt), (0, lv.t), (0, wt))[a]
        for k in range(count):
            n, t = start + k, place + k
            rows = b["st"][n] if a == 1 else b["lt"][t]
            full = jnp.concatenate([rows, b["ly"][0, t], b["ly"][1, t]], axis=0)
            slices = []
            for half in range(2):
                ends = pltpu.roll(mixed[n // 8], (64 - 2 * h * n - h * half) % 128, 1)
                values = pltpu.roll(full, 64, 1) if half else full
                slices.append(jnp.where(own, values, jnp.where(edge, ends, 0.0)))
            emit(t, *slices)


def gather_start(buf, sems, counts):
    me = {axis: lax.axis_index(axis) for axis in counts}
    mine = buf.at[me["gx"], me["gy"], me["gz"]]
    ranges = [[n - k if k else 0 for k in range(n)] for n in counts.values()]
    for offset in sorted(itertools.product(*ranges), key=lambda o: -sum(1 for k in o if k)):
        if any(offset):
            target = {axis: lax.rem(me[axis] + k, counts[axis]) for axis, k in zip(counts, offset) if k}
            pltpu.make_async_remote_copy(
                mine, mine, sems.at[0], sems.at[1], device_id=target, device_id_type=MESH).start()


def gather_wait(sems, counts, units):
    others = counts["gx"] * counts["gy"] * counts["gz"] - 1
    if others:
        wait_units(units, others, sems.at[0])
        wait_units(units, others, sems.at[1])


def batches(low, high, size, body):
    whole = (high - low) // size
    if whole:
        def run(step, carry):
            body(low + step * size, size)
            return carry

        lax.fori_loop(0, whole, run, 0)
    if low + whole * size < high:
        body(low + whole * size, high - low - whole * size)


def even_rows(x, rows):
    return ((iota((rows, 128), 0) + x) & 1) == 0


def prepare_fine(lv, k, rows, fx, fy, zs, zo, dd, iv):
    row = iota((lv.ye, 128), 0)

    def body(first, count, inside=False):
        made = []
        for x in [first + i for i in range(count)]:
            first_red = even_rows(x, lv.ye)
            mids = [k[c][x + 1] for c in range(2)]
            for c in range(2):
                kx, other = mids[c], mids[1 - c]
                below = 0.5 * (k[1 - c][x] + kx)
                above = 0.5 * (kx + k[1 - c][x + 2])
                lower, upper = up(other, 0), down(other, 0)
                if inside:
                    ends = [jnp.broadcast_to(rows[side, pl.ds(x - lv.wt, 1), :], (lv.ye, 128)) for side in range(2)]
                    if c == 0:
                        ends = [pltpu.roll(end, 64, 1) for end in ends]
                    upper = jnp.where(row == lv.y + lv.wy - 1, ends[0], upper)
                    lower = jnp.where(row == lv.y + lv.wy, ends[1], lower)
                second = 0.5 * (lower + kx)
                same = 0.5 * (kx + other)
                moved = [up(other, 1), down(other, 1)]
                third = 0.5 * (kx + jnp.where(first_red, moved[c], moved[1 - c]))
                total = below + above + second + 0.5 * (kx + upper) + same + third
                made.append((x, c, below, second, third, total, jnp.where(kx > 0.0, 1.0 / total, 0.0), same))
        for x, c, *values, same in made:
            for ref, value in zip((fx, fy, zo, dd, iv), values):
                ref[c][x] = value
            if c == 0:
                zs[x] = same

    batches(0, lv.wt, 2, body)
    batches(lv.wt, lv.wt + lv.t, 2, functools.partial(body, inside=True))
    batches(lv.wt + lv.t, lv.te, 2, body)


def around_fine(lv, v, c, x, faces):
    fx, fy, zs, zo = faces
    o = 1 - c
    mid, first_red = v[o][x], even_rows(x, lv.ye)
    moved = [up(mid, 1), down(mid, 1)]
    summed = fx[c][x] * v[o][x - 1] + fx[o][x + 1] * v[o][x + 1]
    summed = summed + fy[c][x] * up(mid, 0) + down(fy[o][x] * mid, 0)
    return summed + zs[x] * mid + zo[c][x] * jnp.where(first_red, moved[c], moved[o])


def half_sweep_fine(lv, v, g, faces, iv, c, reach):
    low, high = lv.wt - reach, lv.wt + lv.t + reach

    def body(first, count):
        fresh = [(x, (g[c][x] + around_fine(lv, v, c, x, faces)) * iv[c][x]) for x in [first + i for i in range(count)]]
        for x, value in fresh:
            v[c][x] = value

    batches(low, high, (high - low) // 2, body)


def residual_fine(lv, v, g, faces, dd, pairs):
    def body(first, count):
        made = []
        for i in [first + j for j in range(count)]:
            total = jnp.zeros((lv.ye, 128), F32)
            for x in (lv.wt + 2 * i, lv.wt + 2 * i + 1):
                for c in range(2):
                    total = total + (g[c][x] - dd[c][x] * v[c][x] + around_fine(lv, v, c, x, faces))
            made.append((i, total))
        for i, total in made:
            pairs[i] = total[0 : lv.y, :]

    batches(0, lv.t // 2, 4, body)


def prepare(k, fx, fy, fz, dd, iv):
    planes = k.shape[0]

    def body(first, count):
        made = []
        for x in [first + i for i in range(count)]:
            kx = k[x]
            below = 0.5 * (k[jnp.maximum(x - 1, 0)] + kx)
            above = 0.5 * (kx + k[jnp.minimum(x + 1, planes - 1)])
            second = 0.5 * (up(kx, 0) + kx)
            third = 0.5 * (up(kx, 1) + kx)
            total = below + above + second + down(second, 0) + third + down(third, 1)
            made.append((x, below, second, third, total, jnp.where(kx > 0.0, 1.0 / total, 0.0)))
        for x, *values in made:
            for ref, value in zip((fx, fy, fz, dd, iv), values):
                ref[x] = value

    batches(0, planes, 4, body)


def around(v, x, mid, faces):
    fx, fy, fz = faces
    second, third = fy[x], fz[x]
    summed = fx[x] * v[x - 1] + fx[x + 1] * v[x + 1]
    summed = summed + second * up(mid, 0) + down(second * mid, 0)
    return summed + third * up(mid, 1) + down(third * mid, 1)


def half_sweep(v, g, faces, iv, colour, low, high):
    parity = iota(v.shape[1:], 0) + iota(v.shape[1:], 1)

    def body(first, count):
        fresh = []
        for x in [first + i for i in range(count)]:
            mid = v[x]
            value = (g[x] + around(v, x, mid, faces)) * iv[x]
            fresh.append((x, jnp.where(((parity + x) & 1) == colour, value, mid)))
        for x, value in fresh:
            v[x] = value

    batches(low, high, 10, body)


def residual_pairs(v, g, faces, dd, pairs, halo):
    for i in range(pairs.shape[0]):
        total = jnp.zeros(v.shape[1:], F32)
        for x in (halo + 2 * i, halo + 2 * i + 1):
            mid = v[x]
            total = total + (g[x] - dd[x] * mid + around(v, x, mid, faces))
        pairs[i] = 0.25 * total[0 : pairs.shape[1]]


def pair_planes(planes, target):
    lane = iota(planes[0].shape, 1)
    for t in range(len(planes) // 2):
        target[t] = jnp.where(lane < 64, planes[2 * t], pltpu.roll(planes[2 * t + 1], 64, 1))


def fold_rows(pairs, rows):
    return pairs[:, pl.ds(0, rows, stride=2), :] + pairs[:, pl.ds(1, rows, stride=2), :]


def dot(a, b):
    return jnp.dot(a, b, precision=HIGH, preferred_element_type=F32)


def split_lanes(transposed):
    cell, lane = iota((128, 128), int(transposed)), iota((128, 128), 1 - int(transposed))
    return jnp.where(lane == cell // 2 + 64 * (cell % 2), 1.0, 0.0).astype(F32)


def coarse_low(pairs, count, rows, lanes, tmp):
    total = jnp.zeros((rows, 128), F32)
    source, goal = iota((128, 128), 0), iota((128, 128), 1)
    for x in range(count):
        matrix = jnp.where((source // 2 + x * lanes == goal) & (source < 2 * lanes), 0.125, 0.0).astype(F32)
        total = total + dot(pairs[x], matrix)
    tmp[...] = total
    half = rows // 2
    return tmp[pl.ds(0, half, stride=2), :] + tmp[pl.ds(1, half, stride=2), :]


def repeat(count, body, carry):
    if count <= 16:
        for p in range(count):
            carry = body(p, carry)
        return carry
    return lax.fori_loop(0, count, body, carry)


def spread_low(buf, whole, counts, pad):
    lane = iota((8, 128), 1)

    def body(a, carry):
        for ct in range(counts["gy"] // 2):
            for gt in range(counts["gz"] // 4):
                pieces = [
                    jnp.concatenate([buf[a, 2 * ct, 4 * gt + g], buf[a, 2 * ct + 1, 4 * gt + g]], axis=0)
                    for g in range(4)]
                for i in range(4):
                    total = pieces[0] if i == 0 else pltpu.roll(pieces[0], (-32 * i) % 128, 1)
                    for g in range(1, 4):
                        piece = pieces[g] if g == i else pltpu.roll(pieces[g], (32 * (g - i)) % 128, 1)
                        total = jnp.where(lane // 32 == g, piece, total)
                    whole[pad + 4 * a + i, 8 * ct : 8 * ct + 8, 128 * gt : 128 * gt + 128] = total
        return carry

    repeat(counts["gx"], body, 0)


def low_faces(k, faces, dims, pad):
    planes, rows, lanes = dims
    cx, cy0, cy1, cz0, cz1, cd = faces
    row, lane = iota((rows, lanes), 0), iota((rows, lanes), 1)
    scale = 0.5 * 0.0625

    def body(p, carry):
        kx = k[p + pad]
        below, above = scale * (k[p + pad - 1] + kx), scale * (kx + k[p + pad + 1])
        total = below + above
        cx[p] = below
        cx[p + 1] = above
        for target, inside, moved in (
            (cy0, row > 0, up(kx, 0)), (cy1, row < rows - 1, down(kx, 0)),
            (cz0, lane > 0, up(kx, 1)), (cz1, lane < lanes - 1, down(kx, 1))):
            face = scale * (kx + moved)
            target[p] = jnp.where(inside, face, 0.0)
            total = total + jnp.where(inside, face, scale * kx)
        cd[p] = total
        return carry

    repeat(planes, body, 0)


def bottom(f, s, vv, faces, dims, pad):
    planes, rows, lanes = dims
    cx, cy0, cy1, cz0, cz1, cd = faces

    def operate(v, p):
        mid = v[p + pad]
        summed = cx[p] * v[p + pad - 1] + cx[p + 1] * v[p + pad + 1]
        summed = summed + (cy0[p] * up(mid, 0) + cy1[p] * down(mid, 0))
        summed = summed + (cz0[p] * up(mid, 1) + cz1[p] * down(mid, 1))
        return mid, cd[p] * mid - summed

    zero = jnp.zeros((rows, lanes), F32)

    def first(p, carry):
        mid, image = operate(f, p)
        vv[p] = image
        return carry[0] + mid * mid, carry[1] + mid * image

    def total(v):
        return jnp.sum(jnp.sum(v, axis=0, keepdims=True), axis=1, keepdims=True)

    norm, along = repeat(planes, first, (zero, zero))
    alpha = total(norm) / total(along)

    def rest(p, carry):
        s[p + pad] = f[p + pad] - alpha * vv[p]
        return carry

    repeat(planes, rest, 0)

    def second(p, carry):
        mid, image = operate(s, p)
        return carry[0] + image * mid, carry[1] + image * image

    turned, norm = repeat(planes, second, (zero, zero))
    return alpha, total(turned) / total(norm)


def pack_boxes(slots, ids, outgoing, boxes, groups):
    held = ids[0].astype(F32)
    cap = held.shape[1]
    eye = iota((cap, cap), 0) == iota((cap, cap), 1)
    rows = jnp.broadcast_to(held, (cap, cap))
    cols = jnp.broadcast_to(jnp.sum(jnp.where(eye, rows, 0.0), axis=1, keepdims=True), (cap, cap))

    def target(v):
        return jnp.floor((v + 0.5) * (1.0 / boxes))

    earlier = (target(rows) == target(cols)) & (cols < rows) & (cols >= 0.0)
    ranking = jnp.sum(jnp.where(earlier, 1.0, 0.0), axis=0, keepdims=True)
    send_row = jnp.where(held >= 0.0, target(held) * SEND + ranking, -1.0)
    count = groups * SEND
    picker = jnp.where(iota((count, cap), 0).astype(F32) == jnp.broadcast_to(send_row, (count, cap)), 1.0, 0.0)
    data = slots[0, 0].astype(F32)
    total = jnp.zeros((count, data.shape[1]), F32)
    for q in range(cap):
        total = total + picker[:, q : q + 1] * data[q : q + 1, :]
    for t in range(groups):
        outgoing[t] = total[SEND * t : SEND * t + SEND, :].astype(BF16)


def place_boxes(incoming, held, owner, lhs, rhs, boxes, groups):
    me = lax.axis_index("gz")
    owners = jnp.broadcast_to(owner[0].astype(F32), (boxes, owner.shape[2]))
    here = iota(owners.shape, 1) == iota(owners.shape, 0) + me * boxes
    col = jnp.sum(jnp.where(here, owners, 0.0), axis=1, keepdims=True)
    cols = jnp.broadcast_to(col, (boxes, boxes))
    first, second = iota((boxes, boxes), 0), iota((boxes, boxes), 1)
    row = jnp.sum(jnp.where(first == second, cols, 0.0), axis=0, keepdims=True)
    before = (jnp.broadcast_to(row, (boxes, boxes)) == cols) & (second < first)
    pick = col * SEND + jnp.sum(jnp.where(before, 1.0, 0.0), axis=1, keepdims=True)
    for t in range(groups):
        held[SEND * t : SEND * t + SEND, :] = incoming[t].astype(F32)
    face = BOX * BOX
    mine = iota((BOX, face), 1) // BOX == iota((BOX, face), 0)
    for i in range(BOX):
        chosen = jnp.zeros((boxes, face), F32)
        for r in range(groups * SEND):
            chosen = jnp.where(pick == float(r), held[r : r + 1, face * i : face * i + face], chosen)
        for b in range(boxes):
            piece = jnp.where(mine, jnp.broadcast_to(chosen[b : b + 1, :], (BOX, face)), 0.0)
            lhs[BOX * i : BOX * i + BOX, face * b : face * b + face] = piece.astype(BF16)
    return jnp.dot(lhs[...], rhs[...], preferred_element_type=F32)


def kernel(levels, counts, names, slots_in, ids_in, owner_in, coef_in, out, *scratch):
    r = dict(zip(names, scratch))
    groups = counts["gz"]
    at = {axis: lax.axis_index(axis) for axis in counts}
    slots, ids, owner, coef, units = r["slots"], r["ids"], r["owner"], r["coef"], r["units"]
    loads = [
        pltpu.make_async_copy(source, target, r["loads"].at[n])
        for n, (source, target) in enumerate(((slots_in, slots), (ids_in, ids), (coef_in, coef), (owner_in, owner)))]
    for load in loads:
        load.start()
    fine, mid = levels["f"], levels["g"]
    sides = {tag: {name[: -len(tag)]: r[name] for name in lv.scratch(tag)} for tag, lv in levels.items()}
    for tag, lv in levels.items():
        clear_sides(lv, sides[tag])

    barrier = pltpu.get_barrier_semaphore()
    expected = 0
    for offset in NEAR:
        target, exists = near(offset, counts)

        @pl.when(exists)
        def _():
            pl.semaphore_signal(barrier, inc=1, device_id=target, device_id_type=MESH)

        expected = expected + jnp.where(exists, 1, 0)
    others = [{"gz": lax.rem(at["gz"] + k, groups)} for k in range(1, groups)]
    if counts["gx"] > 4 or counts["gy"] > 4:
        for offset in itertools.product(*[range(n) for n in counts.values()]):
            if any(offset):
                others.append({axis: lax.rem(at[axis] + k, counts[axis]) for axis, k in zip(counts, offset) if k})
    for target in others:
        pl.semaphore_signal(barrier, inc=1, device_id=target, device_id_type=MESH)

    sems = {tag: r["sems"].at[n] for n, tag in enumerate(("k", "c", "f", "g", "q", "e", "move", "low_k", "low_f"))}

    def send(tag):
        send_sides(levels[tag], sides[tag], sems[tag], counts)

    def take(tag, emit):
        take_sides(levels[tag], sides[tag], sems[tag], counts, units, emit)

    loads[0].wait()
    loads[1].wait()
    boxes = r["boxes"].shape[0] // BOX
    pack_boxes(slots, ids, r["outgoing"], boxes, groups)
    loads[2].wait()
    swap = lambda tile, t: jnp.where(even_rows(t, fine.y), tile, pltpu.roll(tile, 64, 1))
    split = dot(coef[...].reshape(fine.t * fine.y, 128), split_lanes(False)).reshape(fine.t, fine.y, 128)
    for t in range(fine.t):
        sides["k"]["st"][t] = swap(split[t], t)
    pack_sides(levels["k"], sides["k"])
    pl.semaphore_wait(barrier, expected + len(others))

    me = at["gz"]
    for k in range(1, groups):
        to = lax.rem(me + k, groups)
        pltpu.make_async_remote_copy(
            r["outgoing"].at[to], r["incoming"].at[me], sems["move"].at[0], sems["move"].at[1],
            device_id={"gz": to}, device_id_type=MESH).start()
    send("k")
    r["incoming"][me] = r["outgoing"][me]

    half_t, half_y = fine.t // 2, fine.y // 2
    for i in range(half_t):
        pair = sides["k"]["st"][2 * i] + sides["k"]["st"][2 * i + 1]
        r["pairs"][i] = pair + pltpu.roll(pair, 64, 1)
    coarse = 0.125 * fold_rows(r["pairs"], half_y)
    pair_planes([coarse[i] for i in range(half_t)], sides["c"]["st"])
    pack_sides(mid, sides["c"])
    send("c")
    for i in range(half_t // 2):
        r["pairsm"][i] = coarse[2 * i] + coarse[2 * i + 1]
    here = (at["gx"], at["gy"], at["gz"])
    r["gk"][here] = coarse_low(r["pairsm"], half_t // 2, half_y, 32, r["tmp"])
    lane = iota((BOX * BOX, 128), 1)
    cell = 2 * (lane % 64) + lane // 64
    folded = iota((BOX * BOX, 128), 0) % BOX == cell % BOX
    for b in range(boxes):
        block = jnp.where(folded & (cell // BOX == b), 1.0, 0.0)
        r["rhs"][BOX * BOX * b : BOX * BOX * (b + 1), :] = block.astype(BF16)
    loads[3].wait()
    if groups > 1:
        part = r["incoming"].at[pl.ds(0, groups - 1)]
        for n in range(2):
            pltpu.make_async_copy(part, part, sems["move"].at[n]).wait()
    source = place_boxes(r["incoming"], r["held"], owner, r["lhs"], r["rhs"], boxes, groups)
    source = source.reshape(fine.t, fine.y, 128)
    for t in range(fine.t):
        sides["f"]["st"][t] = swap(source[t], t)
    pack_sides(fine, sides["f"])
    send("f")

    pair_of = lambda name: (r[name + "r"], r[name + "b"])
    v0, g0, k0 = pair_of("v0"), pair_of("g0"), pair_of("k0")
    fx, fy, zo, dd0, iv0 = (pair_of(name) for name in ("fx0", "fy0", "zo0", "dd0", "iv0"))
    faces0 = (fx, fy, r["zs0"], zo)
    faces1 = (r["fx1"], r["fy1"], r["fz1"])
    dd1, iv1, v1, K1, G1, E1 = (r[name] for name in ("dd1", "iv1", "v1", "K1", "G1", "E1"))

    def store_pair(refs):
        def emit(t, first, second):
            refs[0][t] = first
            refs[1][t] = second
        return emit

    def store_planes(ref):
        def emit(t, first, second):
            ref[2 * t] = first
            ref[2 * t + 1] = second
        return emit

    take("k", store_pair(k0))
    prepare_fine(fine, k0, sides["k"]["lk"], fx, fy, r["zs0"], zo, dd0, iv0)
    take("c", store_planes(K1))
    prepare(K1, *faces1, dd1, iv1)
    for name in ("k2", "f2", "s2"):
        r[name][...] = jnp.zeros(r[name].shape, F32)

    def open_fine(t, red, black):
        g0[0][t] = red
        g0[1][t] = black
        v0[0][t] = red * iv0[0][t]

    take("f", open_fine)
    for reach, colour in ((3, 1), (2, 0), (1, 1)):
        half_sweep_fine(fine, v0, g0, faces0, iv0, colour, reach)
    residual_fine(fine, v0, g0, faces0, dd0, r["pairs"])

    coarse = 0.5 * fold_rows(r["pairs"], half_y)
    pair_planes([coarse[i] for i in range(half_t)], sides["g"]["st"])
    pack_sides(mid, sides["g"])
    send("g")
    pair_planes([v0[1][fine.wt + x, 0 : fine.y, :] for x in range(fine.t)], sides["q"]["st"])
    pack_sides(levels["q"], sides["q"])
    send("q")
    wm = 2 * mid.wt
    parity = iota((mid.ye, 128), 0) + iota((mid.ye, 128), 1)

    def open_mid(t, *planes):
        for k, plane in enumerate(planes):
            x = 2 * t + k
            G1[x] = plane
            v1[x] = jnp.where(((parity + x) & 1) == 0, plane * iv1[x], 0.0)

    take("g", open_mid)
    gather_start(r["gk"], sems["low_k"], counts)
    for reach, colour in ((3, 1), (2, 0), (1, 1)):
        half_sweep(v1, G1, faces1, iv1, colour, wm - reach, wm + half_t + reach)
    pair_planes([v1[wm + x, 0 : mid.y, :] for x in range(half_t)], sides["e"]["st"])
    pack_sides(mid, sides["e"])
    send("e")
    residual_pairs(v1, G1, faces1, dd1, r["pairsm"], wm)
    r["gf"][here] = coarse_low(r["pairsm"], half_t // 2, half_y, 32, r["tmp"])
    gather_start(r["gf"], sems["low_f"], counts)

    planes, rows, lanes = dims = (4 * counts["gx"], 4 * counts["gy"], 32 * counts["gz"])
    pad = wm // 2
    low = tuple(r[name] for name in ("cx", "cy0", "cy1", "cz0", "cz1", "cd"))
    take("q", store_planes(r["q0"]))
    gather_wait(sems["low_k"], counts, units)
    spread_low(r["gk"], r["k2"], counts, pad)
    low_faces(r["k2"], low, dims, pad)
    take("e", store_planes(E1))
    gather_wait(sems["low_f"], counts, units)
    spread_low(r["gf"], r["f2"], counts, pad)
    alpha, omega = bottom(r["f2"], r["s2"], r["v2"], low, dims, pad)
    around_low = mid.te
    for q in range(around_low):
        turned = alpha * r["f2"][4 * at["gx"] + q] + omega * r["s2"][4 * at["gx"] + q]
        plane = turned
        for c in range(1, counts["gy"]):
            turned = jnp.where(at["gy"] == c, pltpu.roll(plane, rows - 4 * c, 0), turned)
        r["local"][q, 0:8, :] = turned[0:8, :]
        r["local"][q, 8:16, :] = pltpu.roll(turned[rows - 8 : rows, :], 4, 0)
    goal = iota((lanes, 128), 1)
    cell = jnp.where(goal < 64 + wm, goal, goal - 128)
    cell = (cell + 128) // 2 - 64
    wanted = (goal < 64 + wm) | (goal >= 128 - wm)
    matrix = jnp.where((iota((lanes, 128), 0) == 32 * at["gz"] + cell) & wanted, 1.0, 0.0).astype(F32)
    spread = dot(r["local"][...].reshape(16 * around_low, lanes), matrix).reshape(around_low, 16, 128)
    for q in range(around_low):
        wide = r["wide"].at[q]
        for k in range(2):
            wide[pl.ds(k, 12, stride=2), :] = spread[q, 0:12]
        for k in range(2):
            x = 2 * q + k
            E1[x] = jnp.where(K1[x] > 0.0, E1[x] + wide[...], 0.0)
    for reach, colour in ((5, 0), (4, 1), (3, 0), (2, 1)):
        half_sweep(E1, G1, faces1, iv1, colour, wm - reach, wm + half_t + reach)

    low_w = fine.wt // 2
    row = iota((8, 128), 0)
    for i in range(half_t + 2 * low_w):
        x = wm - low_w + i
        wide = r["wide"].at[i]
        ends = jnp.where(row < low_w, E1[x, 8:16, :], pltpu.roll(E1[x, mid.ye - 8 : mid.ye, :], 4, 0))
        turned = jnp.concatenate([E1[x, 0:8, :], ends[0:4]], axis=0)
        for k in range(2):
            wide[pl.ds(k, 12, stride=2), :] = turned
        for k in range(2):
            v0[1][2 * i + k] = r["q0"][2 * i + k] + wide[...]
    for reach, colour in ((3, 0), (2, 1), (1, 0), (0, 1)):
        half_sweep_fine(fine, v0, g0, faces0, iv0, colour, reach)
    lane = iota((fine.y, 128), 1)
    for t in range(fine.t):
        red, black = (v0[c][fine.wt + t, 0 : fine.y, :] for c in range(2))
        r["joined"][t] = swap(jnp.where(lane < 64, red, pltpu.roll(black, 64, 1)), t)
    joined = dot(r["joined"][...].reshape(fine.t * fine.y, 128), split_lanes(True))
    out[...] = joined.reshape(out.shape)


def per_device(counts, old_slots, old_ids, old_owner, coefficient):
    x, y, z = coefficient.shape
    planes, rows, lanes = 4 * counts["gx"], 4 * counts["gy"], 32 * counts["gz"]
    groups, boxes = counts["gz"], z // BOX
    cells = old_slots.shape[3]
    mid = Level(x // 4, y // 2, 3, 8, 6)
    levels = {
        "k": Level(x, y, 5, 4, 3, deep=True), "f": Level(x, y, 4, 4, 2), "q": Level(x // 2, y, 2, 4, 2),
        "c": mid, "g": mid, "e": mid}
    fine, edge = levels["f"], levels["k"]
    pad = mid.wt
    devices = counts["gx"] * counts["gy"] * groups
    vmem = lambda *shape: pltpu.VMEM(shape, F32)
    dma = lambda *shape: pltpu.SemaphoreType.DMA(shape)
    scratch = {}
    for tag, level in levels.items():
        scratch.update(level.scratch(tag))
    for name in ("v0", "g0", "fx0", "fy0", "zo0", "dd0", "iv0", "k0"):
        for colour in "rb":
            scratch[name + colour] = vmem(edge.te if name == "k0" else fine.te, fine.ye, 128)
    for name in ("zs0", "q0"):
        scratch[name] = vmem(fine.te, fine.ye, 128)
    for name in ("fx1", "fy1", "fz1", "dd1", "iv1", "v1", "K1", "G1", "E1"):
        scratch[name] = vmem(2 * mid.te, mid.ye, 128)
    scratch.update(
        slots=pltpu.VMEM(old_slots.shape, old_slots.dtype), ids=pltpu.VMEM(old_ids.shape, old_ids.dtype),
        owner=pltpu.VMEM(old_owner.shape, old_owner.dtype), coef=vmem(*coefficient.shape), loads=dma(4),
        outgoing=pltpu.VMEM((groups, SEND, cells), BF16), incoming=pltpu.VMEM((groups, SEND, cells), BF16),
        held=vmem(groups * SEND, cells), sems=dma(9, 2), units=vmem(max(160, devices), 4, 128),
        lhs=pltpu.VMEM((BOX * BOX, boxes * BOX * BOX), BF16), rhs=pltpu.VMEM((boxes * BOX * BOX, 128), BF16),
        boxes=vmem(boxes * BOX, 128), pairs=vmem(x // 2, y, 128), pairsm=vmem(x // 4, y // 2, 128),
        joined=vmem(x, y, 128), tmp=vmem(y // 2, 128), local=vmem(mid.te, 16, lanes),
        wide=vmem(max(mid.te, fine.te // 2), 24, 128),
        gk=vmem(counts["gx"], counts["gy"], groups, 4, 128), gf=vmem(counts["gx"], counts["gy"], groups, 4, 128),
        cx=vmem(planes + 1, rows, lanes), v2=vmem(planes, rows, lanes))
    for name in ("cy0", "cy1", "cz0", "cz1", "cd"):
        scratch[name] = vmem(planes, rows, lanes)
    for name in ("f2", "k2", "s2"):
        scratch[name] = vmem(planes + 2 * pad, rows, lanes)
    return pl.pallas_call(
        functools.partial(kernel, levels, counts, tuple(scratch)),
        out_shape=jax.ShapeDtypeStruct(coefficient.shape, F32),
        in_specs=[pl.BlockSpec(memory_space=pltpu.MemorySpace.HBM)] * 4,
        out_specs=pl.BlockSpec(memory_space=pltpu.VMEM),
        scratch_shapes=list(scratch.values()),
        compiler_params=pltpu.CompilerParams(
            collective_id=0, has_side_effects=True, vmem_limit_bytes=44 * 1024 * 1024),
    )(*[pltpu.with_memory_space_constraint(v, pltpu.HBM) for v in (old_slots, old_ids, old_owner, coefficient)])


def solution(mesh):
    counts = {axis: mesh.shape[axis] for axis in ("gx", "gy", "gz")}
    return jax.shard_map(
        functools.partial(per_device, counts), mesh=mesh,
        in_specs=(P("gx", "gy", "gz", None), P("gx", "gy", "gz"), P("gx", "gy", None), P("gx", "gy", "gz")),
        out_specs=P("gx", "gy", "gz"), check_vma=False)
```

```python
import functools
import itertools

import jax
import jax.numpy as jnp
from jax import lax
from jax.experimental import pallas as pl
from jax.experimental.pallas import tpu as pltpu
from jax.sharding import PartitionSpec as P

BOX = 16
SEND = 2
F32 = jnp.float32
BF16 = jnp.bfloat16
MESH = pl.DeviceIdType.MESH
HIGH = lax.Precision.HIGHEST


def iota(shape, dim):
    return lax.broadcasted_iota(jnp.int32, shape, dim)


def up(v, axis):
    return pltpu.roll(v, 1, axis)


def down(v, axis):
    return pltpu.roll(v, v.shape[axis] - 1, axis)


class Level:
    def __init__(self, t, y, wt, wy, h, deep=False):
        self.t, self.y, self.wt, self.wy, self.h, self.deep = t, y, wt, wy, h, deep
        self.te, self.ye = t + 2 * wt, y + 2 * wy
        self.blocks = y // wy

    def units(self, a, b, c):
        if c:
            return (self.wy if b else self.y) // 4
        extra = self.t // 4 if self.deep and b and not a else 0
        return (self.wt if a else self.t) * (self.wy if b else self.y) // 4 + extra

    def scratch(self, tag):
        vmem = lambda *shape: pltpu.VMEM(shape + (128,), F32)
        made = {
            "st": vmem(self.t, self.y), "py": vmem(2, self.t, self.wy), "lt": vmem(self.te, self.y),
            "ly": vmem(2, self.te, self.wy), "pf": vmem(self.blocks, self.wy), "pl": vmem(self.blocks, self.wy),
            "lz": vmem(2, 3, self.blocks, self.wy), "lzb": vmem(2, 3, 2, self.wy)}
        if self.deep:
            made.update(ky=vmem(2, self.t), lk=vmem(2, self.t))
        return {name + tag: value for name, value in made.items()}


NEAR = [(a, b, c) for c in (-1, 0, 1) for b in (-1, 0, 1) for a in (-1, 0, 1) if (a, b, c) != (0, 0, 0)]


def near(offset, counts):
    target, exists = {}, None
    for axis, step in zip(("gx", "gy", "gz"), offset):
        me, n = lax.axis_index(axis), counts[axis]
        if step:
            target[axis] = lax.rem(me + step + n, n)
            inside = me > 0 if step < 0 else me < n - 1
            exists = inside if exists is None else jnp.logical_and(exists, inside)
    return target, exists


def wait_units(units, count, sem):
    part = units.at[pl.ds(0, count)]
    pltpu.make_async_copy(part, part, sem).wait()


def wait_near(lv, counts, units, sems):
    choices = []
    for axis in ("gx", "gy", "gz"):
        me, n = lax.axis_index(axis), counts[axis]
        if n == 1:
            choices.append([(0, None)])
        elif n == 2:
            choices.append([(1, None)])
        else:
            edge = jnp.logical_or(me == 0, me == n - 1)
            choices.append([(1, edge), (2, jnp.logical_not(edge))])
    for chosen in itertools.product(*choices):
        total = 0
        for kind in itertools.product((0, 1), repeat=3):
            if any(kind):
                copies = 1
                for used, (number, _) in zip(kind, chosen):
                    copies *= number if used else 1
                total += copies * lv.units(*kind)
        conditions = [condition for _, condition in chosen if condition is not None]

        def wait():
            for sem in sems:
                wait_units(units, total, sem)

        if conditions:
            pl.when(functools.reduce(jnp.logical_and, conditions))(wait)
        else:
            wait()


def clear_sides(lv, b):
    b["lt"][0 : lv.wt] = jnp.zeros((lv.wt, lv.y, 128), F32)
    b["lt"][lv.t + lv.wt : lv.te] = jnp.zeros((lv.wt, lv.y, 128), F32)
    for name in ("ly", "lz", "lzb") + (("lk",) if lv.deep else ()):
        b[name][...] = jnp.zeros(b[name].shape, F32)


def pack_sides(lv, b):
    h, st, lane = lv.h, b["st"], iota((lv.y, 128), 1)
    if lv.blocks > 1:
        b["py"][0] = st[:, 0 : lv.wy, :]
        b["py"][1] = st[:, lv.y - lv.wy : lv.y, :]
    first = last = jnp.zeros((lv.y, 128), F32)
    for t in range(lv.t):
        tile = st[t]
        for half in range(2):
            at = 2 * h * t + h * half
            turned = pltpu.roll(tile, (at - 64 * half) % 128, 1)
            first = jnp.where(((lane - at) & 127) < h, turned, first)
            last = jnp.where(((lane - at - 64 + h) & 127) < h, turned, last)
        if lv.deep:
            b["ky"][0, t : t + 1, :] = tile[lv.wy : lv.wy + 1, :]
            b["ky"][1, t : t + 1, :] = tile[lv.y - lv.wy - 1 : lv.y - lv.wy, :]
    for block in range(lv.blocks):
        rows = slice(block * lv.wy, block * lv.wy + lv.wy)
        b["pf"][block], b["pl"][block] = first[rows], last[rows]


def send_sides(lv, b, sems, counts):
    taken = {-1: (0, lv.wt), 0: (0, lv.t), 1: (lv.t - lv.wt, lv.wt)}
    landed = {-1: lv.t + lv.wt, 0: lv.wt, 1: 0}
    for x, y, z in reversed(sorted(NEAR, key=lambda n: (n[0] != 0) + (n[1] != 0) + (n[2] != 0))):
        target, exists = near((x, y, z), counts)
        first, count = taken[x]
        source, goal, side = pl.ds(first, count), pl.ds(landed[x], count), (y + 1) // 2
        if z:
            ends = b["pf"] if z < 0 else b["pl"]
            if y:
                pairs = [(ends.at[0 if y < 0 else lv.blocks - 1], b["lzb"].at[(1 - z) // 2, 1 - x, (1 - y) // 2])]
            else:
                pairs = [(ends, b["lz"].at[(1 - z) // 2, 1 - x])]
        elif y:
            pairs = [(b["py"].at[side, source] if lv.blocks > 1 else b["st"].at[source], b["ly"].at[side, goal])]
            if lv.deep and not x:
                pairs.append((b["ky"].at[side], b["lk"].at[side]))
        else:
            pairs = [(b["st"].at[source], b["lt"].at[goal])]
        for src, dst in pairs:
            copy = pltpu.make_async_remote_copy(
                src, dst, sems.at[0], sems.at[1], device_id=target, device_id_type=MESH)
            pl.when(exists)(copy.start)


def take_sides(lv, b, sems, counts, units, emit):
    h, wt = lv.h, lv.wt
    wait_near(lv, counts, units, (sems.at[0], sems.at[1]))
    lane = iota((lv.ye, 128), 1)
    own, edge = lane < 64, (lane < 64 + h) | (lane >= 128 - h)
    for a in range(3):
        low, high = [
            jnp.concatenate(
                [b["lz"][c, a, block] for block in range(lv.blocks)] + [b["lzb"][c, a, 1], b["lzb"][c, a, 0]], axis=0)
            for c in range(2)]
        mixed = [jnp.where(((lane - 16 * h * q + h) & 127) < 64, high, low) for q in range(-(-lv.t // 8))]
        place = (0, wt, lv.t + wt)[a]
        start, count = ((lv.t - wt, wt), (0, lv.t), (0, wt))[a]
        for k in range(count):
            n, t = start + k, place + k
            rows = b["st"][n] if a == 1 else b["lt"][t]
            full = jnp.concatenate([rows, b["ly"][0, t], b["ly"][1, t]], axis=0)
            slices = []
            for half in range(2):
                ends = pltpu.roll(mixed[n // 8], (64 - 2 * h * n - h * half) % 128, 1)
                values = pltpu.roll(full, 64, 1) if half else full
                slices.append(jnp.where(own, values, jnp.where(edge, ends, 0.0)))
            emit(t, *slices)


def gather_start(buf, sems, counts):
    me = {axis: lax.axis_index(axis) for axis in counts}
    mine = buf.at[me["gx"], me["gy"], me["gz"]]
    ranges = [[n - k if k else 0 for k in range(n)] for n in counts.values()]
    for offset in sorted(itertools.product(*ranges), key=lambda o: -sum(1 for k in o if k)):
        if any(offset):
            target = {
                axis: lax.rem(me[axis] + jnp.where(me[axis] < counts[axis] // 2, k, counts[axis] - k), counts[axis])
                for axis, k in zip(counts, offset) if k}
            pltpu.make_async_remote_copy(
                mine, mine, sems.at[0], sems.at[1], device_id=target, device_id_type=MESH).start()


def gather_wait(sems, counts, units):
    others = counts["gx"] * counts["gy"] * counts["gz"] - 1
    if others:
        wait_units(units, others, sems.at[0])
        wait_units(units, others, sems.at[1])


def batches(low, high, size, body):
    whole = (high - low) // size
    if whole == 1:
        body(low, size)
    elif whole:
        def run(step, carry):
            body(low + step * size, size)
            return carry

        lax.fori_loop(0, whole, run, 0)
    if low + whole * size < high:
        body(low + whole * size, high - low - whole * size)


def even_rows(x, rows):
    return ((iota((rows, 128), 0) + x) & 1) == 0


def prepare_fine(lv, k, rows, fx, fy, zs, zo, dd, iv):
    row = iota((lv.ye, 128), 0)

    def body(first, count, inside=False):
        made = []
        for x in [first + i for i in range(count)]:
            first_red = even_rows(x, lv.ye)
            mids = [k[c][x + 1] for c in range(2)]
            for c in range(2):
                kx, other = mids[c], mids[1 - c]
                below = 0.5 * (k[1 - c][x] + kx)
                above = 0.5 * (kx + k[1 - c][x + 2])
                lower, upper = up(other, 0), down(other, 0)
                if inside:
                    ends = [jnp.broadcast_to(rows[side, pl.ds(x - lv.wt, 1), :], (lv.ye, 128)) for side in range(2)]
                    if c == 0:
                        ends = [pltpu.roll(end, 64, 1) for end in ends]
                    upper = jnp.where(row == lv.y + lv.wy - 1, ends[0], upper)
                    lower = jnp.where(row == lv.y + lv.wy, ends[1], lower)
                second = 0.5 * (lower + kx)
                same = 0.5 * (kx + other)
                moved = [up(other, 1), down(other, 1)]
                third = 0.5 * (kx + jnp.where(first_red, moved[c], moved[1 - c]))
                total = below + above + second + 0.5 * (kx + upper) + same + third
                made.append((x, c, below, second, third, total, jnp.where(kx > 0.0, 1.0 / total, 0.0), same))
        for x, c, *values, same in made:
            for ref, value in zip((fx, fy, zo, dd, iv), values):
                ref[c][x] = value
            if c == 0:
                zs[x] = same

    batches(0, lv.wt, 2, body)
    batches(lv.wt, lv.wt + lv.t, 2, functools.partial(body, inside=True))
    batches(lv.wt + lv.t, lv.te, 2, body)


def around_fine(lv, v, c, x, faces):
    fx, fy, zs, zo = faces
    o = 1 - c
    mid, first_red = v[o][x], even_rows(x, lv.ye)
    moved = [up(mid, 1), down(mid, 1)]
    summed = fx[c][x] * v[o][x - 1] + fx[o][x + 1] * v[o][x + 1]
    summed = summed + fy[c][x] * up(mid, 0) + down(fy[o][x] * mid, 0)
    return summed + zs[x] * mid + zo[c][x] * jnp.where(first_red, moved[c], moved[o])


def half_sweep_fine(lv, v, g, faces, iv, c, reach):
    low, high = lv.wt - reach, lv.wt + lv.t + reach

    def body(first, count):
        fresh = [(x, (g[c][x] + around_fine(lv, v, c, x, faces)) * iv[c][x]) for x in [first + i for i in range(count)]]
        for x, value in fresh:
            v[c][x] = value

    batches(low, high, high - low, body)


def residual_fine(lv, v, g, faces, dd, pairs):
    def body(first, count):
        made = []
        for i in [first + j for j in range(count)]:
            total = jnp.zeros((lv.ye, 128), F32)
            for x in (lv.wt + 2 * i, lv.wt + 2 * i + 1):
                for c in range(2):
                    total = total + (g[c][x] - dd[c][x] * v[c][x] + around_fine(lv, v, c, x, faces))
            made.append((i, total))
        for i, total in made:
            pairs[i] = total[0 : lv.y, :]

    batches(0, lv.t // 2, lv.t // 2, body)


def prepare(k, fx, fy, fz, dd, iv):
    planes = k.shape[0]

    def body(first, count):
        made = []
        for x in [first + i for i in range(count)]:
            kx = k[x]
            below = 0.5 * (k[jnp.maximum(x - 1, 0)] + kx)
            above = 0.5 * (kx + k[jnp.minimum(x + 1, planes - 1)])
            second = 0.5 * (up(kx, 0) + kx)
            third = 0.5 * (up(kx, 1) + kx)
            total = below + above + second + down(second, 0) + third + down(third, 1)
            made.append((x, below, second, third, total, jnp.where(kx > 0.0, 1.0 / total, 0.0)))
        for x, *values in made:
            for ref, value in zip((fx, fy, fz, dd, iv), values):
                ref[x] = value

    batches(0, planes, 4, body)


def around(v, x, mid, faces):
    fx, fy, fz = faces
    second, third = fy[x], fz[x]
    summed = fx[x] * v[x - 1] + fx[x + 1] * v[x + 1]
    summed = summed + second * up(mid, 0) + down(second * mid, 0)
    return summed + third * up(mid, 1) + down(third * mid, 1)


def half_sweep(v, g, faces, iv, colour, low, high):
    parity = iota(v.shape[1:], 0) + iota(v.shape[1:], 1)

    def body(first, count):
        fresh = []
        for x in [first + i for i in range(count)]:
            mid = v[x]
            value = (g[x] + around(v, x, mid, faces)) * iv[x]
            fresh.append((x, jnp.where(((parity + x) & 1) == colour, value, mid)))
        for x, value in fresh:
            v[x] = value

    batches(low, high, high - low, body)


def residual_pairs(v, g, faces, dd, pairs, halo):
    for i in range(pairs.shape[0]):
        total = jnp.zeros(v.shape[1:], F32)
        for x in (halo + 2 * i, halo + 2 * i + 1):
            mid = v[x]
            total = total + (g[x] - dd[x] * mid + around(v, x, mid, faces))
        pairs[i] = 0.25 * total[0 : pairs.shape[1]]


def pair_planes(planes, target):
    lane = iota(planes[0].shape, 1)
    for t in range(len(planes) // 2):
        target[t] = jnp.where(lane < 64, planes[2 * t], pltpu.roll(planes[2 * t + 1], 64, 1))


def fold_rows(pairs, rows):
    return pairs[:, pl.ds(0, rows, stride=2), :] + pairs[:, pl.ds(1, rows, stride=2), :]


def dot(a, b):
    return jnp.dot(a, b, precision=HIGH, preferred_element_type=F32)


def pick(values, matrix):
    parts, rest = [], values
    for _ in range(3):
        parts.append(rest.astype(BF16))
        rest = rest - parts[-1].astype(F32)
    return jnp.dot(
        jnp.concatenate(parts, axis=1), jnp.concatenate([matrix.astype(BF16)] * 3, axis=0), preferred_element_type=F32)


def split_lanes(transposed):
    cell, lane = iota((128, 128), int(transposed)), iota((128, 128), 1 - int(transposed))
    return jnp.where(lane == cell // 2 + 64 * (cell % 2), 1.0, 0.0).astype(F32)


def coarse_low(pairs, tmp):
    count, rows, _ = pairs.shape
    half = rows // 2
    for x in range(count):
        tmp[half * x : half * x + half, :] = pairs[x, pl.ds(0, half, stride=2), :] + pairs[x, pl.ds(1, half, stride=2), :]
    source, goal = iota((128, 128), 0), iota((128, 128), 1)
    means = 0.125 * pick(tmp[...], jnp.where((source // 2 == goal) & (source < 64), 1.0, 0.0))
    total = means[0:half]
    for x in range(1, count):
        total = total + pltpu.roll(means[half * x : half * x + half], 32 * x, 1)
    return total


def repeat(count, body, carry):
    if count <= 16:
        for p in range(count):
            carry = body(p, carry)
        return carry
    return lax.fori_loop(0, count, body, carry)


def spread_low(buf, whole, counts, pad):
    lane = iota((8, 128), 1)

    def body(a, carry):
        for ct in range(counts["gy"] // 2):
            for gt in range(counts["gz"] // 4):
                pieces = [
                    jnp.concatenate([buf[a, 2 * ct, 4 * gt + g], buf[a, 2 * ct + 1, 4 * gt + g]], axis=0)
                    for g in range(4)]
                for i in range(4):
                    total = pieces[0] if i == 0 else pltpu.roll(pieces[0], (-32 * i) % 128, 1)
                    for g in range(1, 4):
                        piece = pieces[g] if g == i else pltpu.roll(pieces[g], (32 * (g - i)) % 128, 1)
                        total = jnp.where(lane // 32 == g, piece, total)
                    whole[pad + 4 * a + i, 8 * ct : 8 * ct + 8, 128 * gt : 128 * gt + 128] = total
        return carry

    repeat(counts["gx"], body, 0)


def low_faces(k, faces, dims, pad):
    planes, rows, lanes = dims
    cx, cy0, cy1, cz0, cz1, cd = faces
    row, lane = iota((rows, lanes), 0), iota((rows, lanes), 1)
    scale = 0.5 * 0.0625

    def body(p, carry):
        kx = k[p + pad]
        below, above = scale * (k[p + pad - 1] + kx), scale * (kx + k[p + pad + 1])
        total = below + above
        cx[p] = below
        cx[p + 1] = above
        for target, inside, moved in (
            (cy0, row > 0, up(kx, 0)), (cy1, row < rows - 1, down(kx, 0)),
            (cz0, lane > 0, up(kx, 1)), (cz1, lane < lanes - 1, down(kx, 1))):
            face = scale * (kx + moved)
            target[p] = jnp.where(inside, face, 0.0)
            total = total + jnp.where(inside, face, scale * kx)
        cd[p] = total
        return carry

    repeat(planes, body, 0)


def bottom(f, s, vv, faces, dims, pad):
    planes, rows, lanes = dims
    cx, cy0, cy1, cz0, cz1, cd = faces

    def operate(v, p):
        mid = v[p + pad]
        summed = cx[p] * v[p + pad - 1] + cx[p + 1] * v[p + pad + 1]
        summed = summed + (cy0[p] * up(mid, 0) + cy1[p] * down(mid, 0))
        summed = summed + (cz0[p] * up(mid, 1) + cz1[p] * down(mid, 1))
        return mid, cd[p] * mid - summed

    zero = jnp.zeros((rows, lanes), F32)

    def first(p, carry):
        mid, image = operate(f, p)
        vv[p] = image
        return carry[0] + mid * mid, carry[1] + mid * image

    def total(v):
        return jnp.sum(jnp.sum(v, axis=0, keepdims=True), axis=1, keepdims=True)

    norm, along = repeat(planes, first, (zero, zero))
    alpha = total(norm) / total(along)

    def rest(p, carry):
        s[p + pad] = f[p + pad] - alpha * vv[p]
        return carry

    repeat(planes, rest, 0)

    def second(p, carry):
        mid, image = operate(s, p)
        return carry[0] + image * mid, carry[1] + image * image

    turned, norm = repeat(planes, second, (zero, zero))
    return alpha, total(turned) / total(norm)


def pack_boxes(slots, ids, outgoing, boxes, groups):
    held = ids[0].astype(F32)
    cap = held.shape[1]
    eye = iota((cap, cap), 0) == iota((cap, cap), 1)
    rows = jnp.broadcast_to(held, (cap, cap))
    cols = jnp.broadcast_to(jnp.sum(jnp.where(eye, rows, 0.0), axis=1, keepdims=True), (cap, cap))

    def target(v):
        return jnp.floor((v + 0.5) * (1.0 / boxes))

    earlier = (target(rows) == target(cols)) & (cols < rows) & (cols >= 0.0)
    ranking = jnp.sum(jnp.where(earlier, 1.0, 0.0), axis=0, keepdims=True)
    send_row = jnp.where(held >= 0.0, target(held) * SEND + ranking, -1.0)
    count = groups * SEND
    picker = jnp.where(iota((count, cap), 0).astype(F32) == jnp.broadcast_to(send_row, (count, cap)), 1.0, 0.0)
    data = slots[0, 0].astype(F32)
    total = jnp.zeros((count, data.shape[1]), F32)
    for q in range(cap):
        total = total + picker[:, q : q + 1] * data[q : q + 1, :]
    for t in range(groups):
        outgoing[t] = total[SEND * t : SEND * t + SEND, :].astype(BF16)


def place_boxes(incoming, held, owner, rows, boxes, groups):
    me = lax.axis_index("gz")
    owners = jnp.broadcast_to(owner[0].astype(F32), (boxes, owner.shape[2]))
    here = iota(owners.shape, 1) == iota(owners.shape, 0) + me * boxes
    col = jnp.sum(jnp.where(here, owners, 0.0), axis=1, keepdims=True)
    cols = jnp.broadcast_to(col, (boxes, boxes))
    first, second = iota((boxes, boxes), 0), iota((boxes, boxes), 1)
    row = jnp.sum(jnp.where(first == second, cols, 0.0), axis=0, keepdims=True)
    before = (jnp.broadcast_to(row, (boxes, boxes)) == cols) & (second < first)
    pick = col * SEND + jnp.sum(jnp.where(before, 1.0, 0.0), axis=1, keepdims=True)
    for t in range(groups):
        held[SEND * t : SEND * t + SEND, :] = incoming[t].astype(F32)
    per = 128 // BOX
    lane_box, row = iota((boxes, 128), 1) // BOX, iota((boxes, 128), 0)
    for part in range(BOX * BOX // per):
        lanes = slice(128 * part, 128 * part + 128)
        chosen = jnp.zeros((boxes, 128), F32)
        for r in range(groups * SEND):
            chosen = jnp.where(pick == float(r), held[r : r + 1, lanes], chosen)
        total = chosen
        for d in range(1, boxes):
            moved = pltpu.roll(pltpu.roll(chosen, BOX * d, 1), boxes - d, 0)
            total = jnp.where(((lane_box - row) & (boxes - 1)) == d, moved, total)
        rows[per * part : per * part + per, :] = total
    return jnp.dot(rows[...].astype(BF16), split_lanes(False).astype(BF16), preferred_element_type=F32)


def kernel(levels, counts, names, slots_in, ids_in, owner_in, coef_in, out, *scratch):
    r = dict(zip(names, scratch))
    groups = counts["gz"]
    at = {axis: lax.axis_index(axis) for axis in counts}
    slots, ids, owner, coef, units = r["slots"], r["ids"], r["owner"], r["coef"], r["units"]
    loads = [
        pltpu.make_async_copy(source, target, r["loads"].at[n])
        for n, (source, target) in enumerate(((slots_in, slots), (ids_in, ids), (coef_in, coef), (owner_in, owner)))]
    for load in loads:
        load.start()
    fine, mid = levels["f"], levels["g"]
    sides = {tag: {name[: -len(tag)]: r[name] for name in lv.scratch(tag)} for tag, lv in levels.items()}
    for tag, lv in levels.items():
        clear_sides(lv, sides[tag])

    barrier = pltpu.get_barrier_semaphore()
    expected = 0
    for offset in sorted(NEAR, key=lambda n: -sum(map(abs, n))):
        target, exists = near(offset, counts)

        @pl.when(exists)
        def _():
            pl.semaphore_signal(barrier, inc=1, device_id=target, device_id_type=MESH)

        expected = expected + jnp.where(exists, 1, 0)
    others = [{"gz": lax.rem(at["gz"] + k, groups)} for k in range(1, groups)]
    if counts["gx"] > 4 or counts["gy"] > 4:
        for offset in itertools.product(*[range(n) for n in counts.values()]):
            if any(offset):
                others.append({axis: lax.rem(at[axis] + k, counts[axis]) for axis, k in zip(counts, offset) if k})
    for target in others:
        pl.semaphore_signal(barrier, inc=1, device_id=target, device_id_type=MESH)

    sems = {tag: r["sems"].at[n] for n, tag in enumerate(("k", "c", "f", "g", "q", "e", "move", "low_k", "low_f"))}

    def send(tag):
        send_sides(levels[tag], sides[tag], sems[tag], counts)

    def take(tag, emit):
        take_sides(levels[tag], sides[tag], sems[tag], counts, units, emit)

    loads[0].wait()
    loads[1].wait()
    boxes = out.shape[2] // BOX
    pack_boxes(slots, ids, r["outgoing"], boxes, groups)
    pl.semaphore_wait(barrier, expected + len(others))

    me = at["gz"]
    for k in range(1, groups):
        to = lax.rem(me + k, groups)
        pltpu.make_async_remote_copy(
            r["outgoing"].at[to], r["incoming"].at[me], sems["move"].at[0], sems["move"].at[1],
            device_id={"gz": to}, device_id_type=MESH).start()
    greeted = 0
    for offset in itertools.product((-1, 1), (0,), (-1, 0, 1)):
        target, exists = near(offset, counts)

        @pl.when(exists)
        def _():
            pl.semaphore_signal(r["hello"], inc=1, device_id=target, device_id_type=MESH)

        greeted = greeted + jnp.where(exists, 1, 0)

    loads[2].wait()
    swap = lambda tile, t: jnp.where(even_rows(t, fine.y), tile, pltpu.roll(tile, 64, 1))
    split = pick(coef[...].reshape(fine.t * fine.y, 128), split_lanes(False)).reshape(fine.t, fine.y, 128)
    for t in range(fine.t):
        sides["k"]["st"][t] = swap(split[t], t)
    pack_sides(levels["k"], sides["k"])
    send("k")
    r["incoming"][me] = r["outgoing"][me]

    half_t, half_y = fine.t // 2, fine.y // 2
    for i in range(half_t):
        pair = sides["k"]["st"][2 * i] + sides["k"]["st"][2 * i + 1]
        r["pairs"][i] = pair + pltpu.roll(pair, 64, 1)
    coarse = 0.125 * fold_rows(r["pairs"], half_y)
    pair_planes([coarse[i] for i in range(half_t)], sides["c"]["st"])
    pack_sides(mid, sides["c"])
    send("c")
    for i in range(half_t // 2):
        r["pairsm"][i] = coarse[2 * i] + coarse[2 * i + 1]
    here = (at["gx"], at["gy"], at["gz"])
    r["gk"][here] = coarse_low(r["pairsm"], r["tmp"])
    loads[3].wait()
    if groups > 1:
        part = r["incoming"].at[pl.ds(0, groups - 1)]
        for n in range(2):
            pltpu.make_async_copy(part, part, sems["move"].at[n]).wait()
    source = place_boxes(r["incoming"], r["held"], owner, r["rows"], boxes, groups)
    source = source.reshape(fine.t, fine.y, 128)
    for t in range(fine.t):
        sides["f"]["st"][t] = swap(source[t], t)
    pack_sides(fine, sides["f"])
    pl.semaphore_wait(r["hello"], greeted)
    send("f")

    pair_of = lambda name: (r[name + "r"], r[name + "b"])
    v0, g0, k0 = pair_of("v0"), pair_of("g0"), pair_of("k0")
    fx, fy, zo, dd0, iv0 = (pair_of(name) for name in ("fx0", "fy0", "zo0", "dd0", "iv0"))
    faces0 = (fx, fy, r["zs0"], zo)
    faces1 = (r["fx1"], r["fy1"], r["fz1"])
    dd1, iv1, v1, K1, G1, E1 = (r[name] for name in ("dd1", "iv1", "v1", "K1", "G1", "E1"))

    def store_pair(refs):
        def emit(t, first, second):
            refs[0][t] = first
            refs[1][t] = second
        return emit

    def store_planes(ref):
        def emit(t, first, second):
            ref[2 * t] = first
            ref[2 * t + 1] = second
        return emit

    take("k", store_pair(k0))
    prepare_fine(fine, k0, sides["k"]["lk"], fx, fy, r["zs0"], zo, dd0, iv0)

    def open_fine(t, red, black):
        g0[0][t] = red
        g0[1][t] = black
        v0[0][t] = red * iv0[0][t]

    take("f", open_fine)
    for reach, colour in ((3, 1), (2, 0), (1, 1)):
        half_sweep_fine(fine, v0, g0, faces0, iv0, colour, reach)
    residual_fine(fine, v0, g0, faces0, dd0, r["pairs"])

    coarse = 0.5 * fold_rows(r["pairs"], half_y)
    pair_planes([coarse[i] for i in range(half_t)], sides["g"]["st"])
    pack_sides(mid, sides["g"])
    send("g")
    pair_planes([v0[1][fine.wt + x, 0 : fine.y, :] for x in range(fine.t)], sides["q"]["st"])
    pack_sides(levels["q"], sides["q"])
    send("q")
    gather_start(r["gk"], sems["low_k"], counts)
    take("c", store_planes(K1))
    prepare(K1, *faces1, dd1, iv1)
    for name in ("k2", "f2", "s2"):
        r[name][...] = jnp.zeros(r[name].shape, F32)
    wm = 2 * mid.wt
    parity = iota((mid.ye, 128), 0) + iota((mid.ye, 128), 1)

    def open_mid(t, *planes):
        for k, plane in enumerate(planes):
            x = 2 * t + k
            G1[x] = plane
            v1[x] = jnp.where(((parity + x) & 1) == 0, plane * iv1[x], 0.0)

    take("g", open_mid)
    for reach, colour in ((3, 1), (2, 0), (1, 1)):
        half_sweep(v1, G1, faces1, iv1, colour, wm - reach, wm + half_t + reach)
    residual_pairs(v1, G1, faces1, dd1, r["pairsm"], wm)
    r["gf"][here] = coarse_low(r["pairsm"], r["tmp"])
    gather_start(r["gf"], sems["low_f"], counts)
    pair_planes([v1[wm + x, 0 : mid.y, :] for x in range(half_t)], sides["e"]["st"])
    pack_sides(mid, sides["e"])
    send("e")

    planes, rows, lanes = dims = (4 * counts["gx"], 4 * counts["gy"], 32 * counts["gz"])
    pad = wm // 2
    low = tuple(r[name] for name in ("cx", "cy0", "cy1", "cz0", "cz1", "cd"))
    take("q", store_planes(r["q0"]))
    gather_wait(sems["low_k"], counts, units)
    spread_low(r["gk"], r["k2"], counts, pad)
    low_faces(r["k2"], low, dims, pad)
    take("e", store_planes(E1))
    gather_wait(sems["low_f"], counts, units)
    spread_low(r["gf"], r["f2"], counts, pad)
    alpha, omega = bottom(r["f2"], r["s2"], r["v2"], low, dims, pad)
    around_low = mid.te
    for q in range(around_low):
        turned = alpha * r["f2"][4 * at["gx"] + q] + omega * r["s2"][4 * at["gx"] + q]
        plane = turned
        for c in range(1, counts["gy"]):
            turned = jnp.where(at["gy"] == c, pltpu.roll(plane, rows - 4 * c, 0), turned)
        r["local"][q, 0:8, :] = turned[0:8, :]
        r["local"][q, 8:16, :] = pltpu.roll(turned[rows - 8 : rows, :], 4, 0)
    goal = iota((lanes, 128), 1)
    cell = jnp.where(goal < 64 + wm, goal, goal - 128)
    cell = (cell + 128) // 2 - 64
    wanted = (goal < 64 + wm) | (goal >= 128 - wm)
    matrix = jnp.where((iota((lanes, 128), 0) == 32 * at["gz"] + cell) & wanted, 1.0, 0.0).astype(F32)
    spread = pick(r["local"][...].reshape(16 * around_low, lanes), matrix).reshape(around_low, 16, 128)
    for q in range(around_low):
        wide = r["wide"].at[q]
        for k in range(2):
            wide[pl.ds(k, 12, stride=2), :] = spread[q, 0:12]
        for k in range(2):
            x = 2 * q + k
            E1[x] = jnp.where(K1[x] > 0.0, E1[x] + wide[...], 0.0)
    for reach, colour in ((5, 0), (4, 1), (3, 0), (2, 1)):
        half_sweep(E1, G1, faces1, iv1, colour, wm - reach, wm + half_t + reach)

    low_w = fine.wt // 2
    row = iota((8, 128), 0)
    for i in range(half_t + 2 * low_w):
        x = wm - low_w + i
        wide = r["wide"].at[i]
        ends = jnp.where(row < low_w, E1[x, 8:16, :], pltpu.roll(E1[x, mid.ye - 8 : mid.ye, :], 4, 0))
        turned = jnp.concatenate([E1[x, 0:8, :], ends[0:4]], axis=0)
        for k in range(2):
            wide[pl.ds(k, 12, stride=2), :] = turned
        for k in range(2):
            v0[1][2 * i + k] = r["q0"][2 * i + k] + wide[...]
    for reach, colour in ((3, 0), (2, 1), (1, 0), (0, 1)):
        half_sweep_fine(fine, v0, g0, faces0, iv0, colour, reach)
    lane = iota((fine.y, 128), 1)
    for t in range(fine.t):
        red, black = (v0[c][fine.wt + t, 0 : fine.y, :] for c in range(2))
        r["joined"][t] = swap(jnp.where(lane < 64, red, pltpu.roll(black, 64, 1)), t)
    joined = pick(r["joined"][...].reshape(fine.t * fine.y, 128), split_lanes(True))
    out[...] = joined.reshape(out.shape)


def per_device(counts, old_slots, old_ids, old_owner, coefficient):
    x, y, z = coefficient.shape
    planes, rows, lanes = 4 * counts["gx"], 4 * counts["gy"], 32 * counts["gz"]
    groups, boxes = counts["gz"], z // BOX
    cells = old_slots.shape[3]
    mid = Level(x // 4, y // 2, 3, 8, 6)
    levels = {
        "k": Level(x, y, 5, 4, 3, deep=True), "f": Level(x, y, 4, 4, 2), "q": Level(x // 2, y, 2, 4, 2),
        "c": mid, "g": mid, "e": mid}
    fine, edge = levels["f"], levels["k"]
    pad = mid.wt
    devices = counts["gx"] * counts["gy"] * groups
    vmem = lambda *shape: pltpu.VMEM(shape, F32)
    dma = lambda *shape: pltpu.SemaphoreType.DMA(shape)
    scratch = {}
    for tag, level in levels.items():
        scratch.update(level.scratch(tag))
    for name in ("v0", "g0", "fx0", "fy0", "zo0", "dd0", "iv0", "k0"):
        for colour in "rb":
            scratch[name + colour] = vmem(edge.te if name == "k0" else fine.te, fine.ye, 128)
    for name in ("zs0", "q0"):
        scratch[name] = vmem(fine.te, fine.ye, 128)
    for name in ("fx1", "fy1", "fz1", "dd1", "iv1", "v1", "K1", "G1", "E1"):
        scratch[name] = vmem(2 * mid.te, mid.ye, 128)
    scratch.update(
        slots=pltpu.VMEM(old_slots.shape, old_slots.dtype), ids=pltpu.VMEM(old_ids.shape, old_ids.dtype),
        owner=pltpu.VMEM(old_owner.shape, old_owner.dtype), coef=vmem(*coefficient.shape), loads=dma(4),
        outgoing=pltpu.VMEM((groups, SEND, cells), BF16), incoming=pltpu.VMEM((groups, SEND, cells), BF16),
        held=vmem(groups * SEND, cells), sems=dma(9, 2), hello=pltpu.SemaphoreType.REGULAR, units=vmem(max(160, devices), 4, 128),
        rows=vmem(BOX * BOX, 128), pairs=vmem(x // 2, y, 128), pairsm=vmem(x // 4, y // 2, 128),
        joined=vmem(x, y, 128), tmp=vmem(x * y // 16, 128), local=vmem(mid.te, 16, lanes),
        wide=vmem(max(mid.te, fine.te // 2), 24, 128),
        gk=vmem(counts["gx"], counts["gy"], groups, 4, 128), gf=vmem(counts["gx"], counts["gy"], groups, 4, 128),
        cx=vmem(planes + 1, rows, lanes), v2=vmem(planes, rows, lanes))
    for name in ("cy0", "cy1", "cz0", "cz1", "cd"):
        scratch[name] = vmem(planes, rows, lanes)
    for name in ("f2", "k2", "s2"):
        scratch[name] = vmem(planes + 2 * pad, rows, lanes)
    return pl.pallas_call(
        functools.partial(kernel, levels, counts, tuple(scratch)),
        out_shape=jax.ShapeDtypeStruct(coefficient.shape, F32),
        in_specs=[pl.BlockSpec(memory_space=pltpu.MemorySpace.HBM)] * 4,
        out_specs=pl.BlockSpec(memory_space=pltpu.VMEM),
        scratch_shapes=list(scratch.values()),
        compiler_params=pltpu.CompilerParams(
            collective_id=0, has_side_effects=True, vmem_limit_bytes=44 * 1024 * 1024),
    )(*[pltpu.with_memory_space_constraint(v, pltpu.HBM) for v in (old_slots, old_ids, old_owner, coefficient)])


def solution(mesh):
    counts = {axis: mesh.shape[axis] for axis in ("gx", "gy", "gz")}
    return jax.shard_map(
        functools.partial(per_device, counts), mesh=mesh,
        in_specs=(P("gx", "gy", "gz", None), P("gx", "gy", "gz"), P("gx", "gy", None), P("gx", "gy", "gz")),
        out_specs=P("gx", "gy", "gz"), check_vma=False)
```

```python
import functools
import itertools

import jax
import jax.numpy as jnp
from jax import lax
from jax.experimental import pallas as pl
from jax.experimental.pallas import tpu as pltpu
from jax.sharding import PartitionSpec as P

BOX = 16
SEND = 2
F32 = jnp.float32
BF16 = jnp.bfloat16
MESH = pl.DeviceIdType.MESH
HIGH = lax.Precision.HIGHEST


def iota(shape, dim):
    return lax.broadcasted_iota(jnp.int32, shape, dim)


def up(v, axis):
    return pltpu.roll(v, 1, axis)


def down(v, axis):
    return pltpu.roll(v, v.shape[axis] - 1, axis)


class Level:
    def __init__(self, t, y, wt, wy, h, deep=False, dtype=F32):
        self.dtype = dtype
        self.t, self.y, self.wt, self.wy, self.h, self.deep = t, y, wt, wy, h, deep
        self.te, self.ye = t + 2 * wt, y + 2 * wy
        self.blocks = y // wy

    def units(self, a, b, c):
        if c:
            return (self.wy if b else self.y) // 4
        extra = self.t // 4 if self.deep and b and not a else 0
        return (self.wt if a else self.t) * (self.wy if b else self.y) // 4 + extra

    def scratch(self, tag):
        vmem = lambda *shape: pltpu.VMEM(shape + (128,), self.dtype)
        made = {
            "st": vmem(self.t, self.y), "py": vmem(2, self.t, self.wy), "lt": vmem(self.te, self.y),
            "ly": vmem(2, self.te, self.wy), "pf": vmem(self.blocks, self.wy), "pl": vmem(self.blocks, self.wy),
            "lz": vmem(2, 3, self.blocks, self.wy), "lzb": vmem(2, 3, 2, self.wy)}
        if self.deep:
            made.update(ky=vmem(2, self.t), lk=vmem(2, self.t))
        return {name + tag: value for name, value in made.items()}


NEAR = [(a, b, c) for c in (-1, 0, 1) for b in (-1, 0, 1) for a in (-1, 0, 1) if (a, b, c) != (0, 0, 0)]


def near(offset, counts):
    target, exists = {}, None
    for axis, step in zip(("gx", "gy", "gz"), offset):
        me, n = lax.axis_index(axis), counts[axis]
        if step:
            target[axis] = lax.rem(me + step + n, n)
            inside = me > 0 if step < 0 else me < n - 1
            exists = inside if exists is None else jnp.logical_and(exists, inside)
    return target, exists


def wait_units(units, count, sem):
    part = units.at[pl.ds(0, count)]
    pltpu.make_async_copy(part, part, sem).wait()


def wait_near(lv, counts, units, sems):
    choices = []
    for axis in ("gx", "gy", "gz"):
        me, n = lax.axis_index(axis), counts[axis]
        if n == 1:
            choices.append([(0, None)])
        elif n == 2:
            choices.append([(1, None)])
        else:
            edge = jnp.logical_or(me == 0, me == n - 1)
            choices.append([(1, edge), (2, jnp.logical_not(edge))])
    for chosen in itertools.product(*choices):
        total = 0
        for kind in itertools.product((0, 1), repeat=3):
            if any(kind):
                copies = 1
                for used, (number, _) in zip(kind, chosen):
                    copies *= number if used else 1
                total += copies * lv.units(*kind)
        conditions = [condition for _, condition in chosen if condition is not None]

        def wait():
            for sem in sems:
                wait_units(units, total, sem)

        if conditions:
            pl.when(functools.reduce(jnp.logical_and, conditions))(wait)
        else:
            wait()


def clear_sides(lv, b):
    b["lt"][0 : lv.wt] = jnp.zeros((lv.wt, lv.y, 128), lv.dtype)
    b["lt"][lv.t + lv.wt : lv.te] = jnp.zeros((lv.wt, lv.y, 128), lv.dtype)
    for name in ("ly", "lz", "lzb") + (("lk",) if lv.deep else ()):
        b[name][...] = jnp.zeros(b[name].shape, lv.dtype)


def pack_sides(lv, b):
    h, st, lane = lv.h, b["st"], iota((lv.y, 128), 1)
    first = last = jnp.zeros((lv.y, 128), F32)
    for t in range(lv.t):
        tile = st[t].astype(F32)
        if lv.blocks > 1:
            b["py"][0, t] = tile[0 : lv.wy].astype(lv.dtype)
            b["py"][1, t] = tile[lv.y - lv.wy : lv.y].astype(lv.dtype)
        for half in range(2):
            at = 2 * h * t + h * half
            turned = pltpu.roll(tile, (at - 64 * half) % 128, 1)
            first = jnp.where(((lane - at) & 127) < h, turned, first)
            last = jnp.where(((lane - at - 64 + h) & 127) < h, turned, last)
        if lv.deep:
            b["ky"][0, t : t + 1, :] = tile[lv.wy : lv.wy + 1, :]
            b["ky"][1, t : t + 1, :] = tile[lv.y - lv.wy - 1 : lv.y - lv.wy, :]
    for block in range(lv.blocks):
        rows = slice(block * lv.wy, block * lv.wy + lv.wy)
        b["pf"][block], b["pl"][block] = first[rows].astype(lv.dtype), last[rows].astype(lv.dtype)


def send_sides(lv, b, sems, counts, axes):
    taken = {-1: (0, lv.wt), 0: (0, lv.t), 1: (lv.t - lv.wt, lv.wt)}
    landed = {-1: lv.t + lv.wt, 0: lv.wt, 1: 0}
    pair = counts["gy"] == 2
    me = lax.axis_index("gy")

    def start(x, y, z):
        target = near((x, y, z), counts)[0]
        first, count = taken[x]
        source, goal = pl.ds(first, count), pl.ds(landed[x], count)
        side = 1 - me if pair else (y + 1) // 2
        if z:
            ends = b["pf"] if z < 0 else b["pl"]
            if y:
                pairs = [(ends.at[side * (lv.blocks - 1)], b["lzb"].at[(1 - z) // 2, 1 - x, 1 - side])]
            else:
                pairs = [(ends, b["lz"].at[(1 - z) // 2, 1 - x])]
        elif y:
            pairs = [(b["py"].at[side, source] if lv.blocks > 1 else b["st"].at[source], b["ly"].at[side, goal])]
            if lv.deep and not x:
                pairs.append((b["ky"].at[side], b["lk"].at[side]))
        else:
            pairs = [(b["st"].at[source], b["lt"].at[goal])]
        for src, dst in pairs:
            pltpu.make_async_remote_copy(
                src, dst, sems.at[0], sems.at[1], device_id=target, device_id_type=MESH).start()

    steps = (1, 0) if pair else (1, -1, 0)
    for x, z in sorted(itertools.product((-1, 0, 1), repeat=2), key=lambda n: -abs(n[0]) - abs(n[1])):
        chosen = [y for y in steps if abs(x) + abs(y) + abs(z) in axes]

        def send():
            for y in chosen:
                if pair or not y:
                    start(x, y, z)
                else:
                    pl.when(near((0, y, 0), counts)[1])(functools.partial(start, x, y, z))

        exists = near((x, 0, z), counts)[1]
        if chosen:
            send() if exists is None else pl.when(exists)(send)


def take_sides(lv, b, sems, counts, units, emit):
    h, wt = lv.h, lv.wt
    wait_near(lv, counts, units, (sems.at[0], sems.at[1]))
    lane = iota((lv.ye, 128), 1)
    own, edge = lane < 64, (lane < 64 + h) | (lane >= 128 - h)
    for a in range(3):
        low, high = [
            jnp.concatenate(
                [b["lz"][c, a, block].astype(F32) for block in range(lv.blocks)]
                + [b["lzb"][c, a, side].astype(F32) for side in (1, 0)], axis=0)
            for c in range(2)]
        mixed = [jnp.where(((lane - 16 * h * q + h) & 127) < 64, high, low) for q in range(-(-lv.t // 8))]
        place = (0, wt, lv.t + wt)[a]
        start, count = ((lv.t - wt, wt), (0, lv.t), (0, wt))[a]
        for k in range(count):
            n, t = start + k, place + k
            rows = b["st"][n] if a == 1 else b["lt"][t]
            full = jnp.concatenate([part.astype(F32) for part in (rows, b["ly"][0, t], b["ly"][1, t])], axis=0)
            slices = []
            for half in range(2):
                ends = pltpu.roll(mixed[n // 8], (64 - 2 * h * n - h * half) % 128, 1)
                values = pltpu.roll(full, 64, 1) if half else full
                slices.append(jnp.where(own, values, jnp.where(edge, ends, 0.0)))
            emit(t, *slices)


def gather_start(buf, sems, counts):
    me = {axis: lax.axis_index(axis) for axis in counts}
    mine = buf.at[me["gx"], me["gy"], me["gz"]]
    ranges = [[n - k if k else 0 for k in range(n)] for n in counts.values()]
    for offset in sorted(itertools.product(*ranges), key=lambda o: -sum(1 for k in o if k)):
        if any(offset):
            target = {
                axis: lax.rem(me[axis] + jnp.where(me[axis] < counts[axis] // 2, k, counts[axis] - k), counts[axis])
                for axis, k in zip(counts, offset) if k}
            pltpu.make_async_remote_copy(
                mine, mine, sems.at[0], sems.at[1], device_id=target, device_id_type=MESH).start()


def gather_wait(sems, counts, units):
    others = counts["gx"] * counts["gy"] * counts["gz"] - 1
    if others:
        wait_units(units, others, sems.at[0])
        wait_units(units, others, sems.at[1])


def batches(low, high, size, body):
    whole = (high - low) // size
    if whole == 1:
        body(low, size)
    elif whole:
        def run(step, carry):
            body(low + step * size, size)
            return carry

        lax.fori_loop(0, whole, run, 0)
    if low + whole * size < high:
        body(low + whole * size, high - low - whole * size)


def even_rows(x, rows):
    return ((iota((rows, 128), 0) + x) & 1) == 0


def prepare_fine(lv, k, rows, fx, fy, zs, zo, dd, iv):
    row = iota((lv.ye, 128), 0)

    def body(first, count, inside=False):
        made = []
        for x in [first + i for i in range(count)]:
            first_red = even_rows(x, lv.ye)
            mids = [k[c][x + 1] for c in range(2)]
            for c in range(2):
                kx, other = mids[c], mids[1 - c]
                below = 0.5 * (k[1 - c][x] + kx)
                above = 0.5 * (kx + k[1 - c][x + 2])
                lower, upper = up(other, 0), down(other, 0)
                if inside:
                    ends = [jnp.broadcast_to(rows[side, pl.ds(x - lv.wt, 1), :], (lv.ye, 128)) for side in range(2)]
                    if c == 0:
                        ends = [pltpu.roll(end, 64, 1) for end in ends]
                    upper = jnp.where(row == lv.y + lv.wy - 1, ends[0], upper)
                    lower = jnp.where(row == lv.y + lv.wy, ends[1], lower)
                second = 0.5 * (lower + kx)
                same = 0.5 * (kx + other)
                moved = [up(other, 1), down(other, 1)]
                third = 0.5 * (kx + jnp.where(first_red, moved[c], moved[1 - c]))
                total = below + above + second + 0.5 * (kx + upper) + same + third
                made.append((x, c, below, second, third, total, jnp.where(kx > 0.0, 1.0 / total, 0.0), same))
        for x, c, *values, same in made:
            for ref, value in zip((fx, fy, zo, dd, iv), values):
                ref[c][x] = value
            if c == 0:
                zs[x] = same

    batches(0, lv.wt, 4, body)
    batches(lv.wt, lv.wt + lv.t, 8, functools.partial(body, inside=True))
    batches(lv.wt + lv.t, lv.te, 4, body)


def around_fine(lv, v, c, x, faces):
    fx, fy, zs, zo = faces
    o = 1 - c
    mid, first_red = v[o][x], even_rows(x, lv.ye)
    moved = [up(mid, 1), down(mid, 1)]
    summed = fx[c][x] * v[o][x - 1] + fx[o][x + 1] * v[o][x + 1]
    summed = summed + fy[c][x] * up(mid, 0) + down(fy[o][x] * mid, 0)
    return summed + zs[x] * mid + zo[c][x] * jnp.where(first_red, moved[c], moved[o])


def half_sweep_fine(lv, v, g, faces, iv, c, reach):
    low, high = lv.wt - reach, lv.wt + lv.t + reach

    def body(first, count):
        fresh = [(x, (g[c][x] + around_fine(lv, v, c, x, faces)) * iv[c][x]) for x in [first + i for i in range(count)]]
        for x, value in fresh:
            v[c][x] = value

    batches(low, high, high - low, body)


def residual_fine(lv, v, g, faces, dd, pairs):
    def body(first, count):
        made = []
        for i in [first + j for j in range(count)]:
            total = jnp.zeros((lv.ye, 128), F32)
            for x in (lv.wt + 2 * i, lv.wt + 2 * i + 1):
                for c in range(2):
                    total = total + (g[c][x] - dd[c][x] * v[c][x] + around_fine(lv, v, c, x, faces))
            made.append((i, total))
        for i, total in made:
            pairs[i] = total[0 : lv.y, :]

    batches(0, lv.t // 2, lv.t // 2, body)


def prepare(k, fx, fy, fz, dd, iv):
    planes = k.shape[0]

    def body(first, count):
        made = []
        for x in [first + i for i in range(count)]:
            kx = k[x]
            below = 0.5 * (k[jnp.maximum(x - 1, 0)] + kx)
            above = 0.5 * (kx + k[jnp.minimum(x + 1, planes - 1)])
            second = 0.5 * (up(kx, 0) + kx)
            third = 0.5 * (up(kx, 1) + kx)
            total = below + above + second + down(second, 0) + third + down(third, 1)
            made.append((x, below, second, third, total, jnp.where(kx > 0.0, 1.0 / total, 0.0)))
        for x, *values in made:
            for ref, value in zip((fx, fy, fz, dd, iv), values):
                ref[x] = value

    batches(0, planes, 4, body)


def around(v, x, mid, faces):
    fx, fy, fz = faces
    second, third = fy[x], fz[x]
    summed = fx[x] * v[x - 1] + fx[x + 1] * v[x + 1]
    summed = summed + second * up(mid, 0) + down(second * mid, 0)
    return summed + third * up(mid, 1) + down(third * mid, 1)


def half_sweep(v, g, faces, iv, colour, low, high):
    parity = iota(v.shape[1:], 0) + iota(v.shape[1:], 1)

    def body(first, count):
        fresh = []
        for x in [first + i for i in range(count)]:
            mid = v[x]
            value = (g[x] + around(v, x, mid, faces)) * iv[x]
            fresh.append((x, jnp.where(((parity + x) & 1) == colour, value, mid)))
        for x, value in fresh:
            v[x] = value

    batches(low, high, high - low, body)


def residual_pairs(v, g, faces, dd, pairs, halo):
    for i in range(pairs.shape[0]):
        total = jnp.zeros(v.shape[1:], F32)
        for x in (halo + 2 * i, halo + 2 * i + 1):
            mid = v[x]
            total = total + (g[x] - dd[x] * mid + around(v, x, mid, faces))
        pairs[i] = 0.25 * total[0 : pairs.shape[1]]


def pair_planes(planes, target):
    lane = iota(planes[0].shape, 1)
    for t in range(len(planes) // 2):
        target[t] = jnp.where(lane < 64, planes[2 * t], pltpu.roll(planes[2 * t + 1], 64, 1))


def fold_rows(pairs, rows):
    return pairs[:, pl.ds(0, rows, stride=2), :] + pairs[:, pl.ds(1, rows, stride=2), :]


def dot(a, b):
    return jnp.dot(a, b, precision=HIGH, preferred_element_type=F32)


def pick(values, matrix):
    parts, rest = [], values
    for _ in range(3):
        parts.append(rest.astype(BF16))
        rest = rest - parts[-1].astype(F32)
    return jnp.dot(
        jnp.concatenate(parts, axis=1), jnp.concatenate([matrix.astype(BF16)] * 3, axis=0), preferred_element_type=F32)


def split_lanes(transposed):
    cell, lane = iota((128, 128), int(transposed)), iota((128, 128), 1 - int(transposed))
    return jnp.where(lane == cell // 2 + 64 * (cell % 2), 1.0, 0.0).astype(F32)


def coarse_low(pairs, tmp):
    count, rows, _ = pairs.shape
    half = rows // 2
    for x in range(count):
        tmp[half * x : half * x + half, :] = pairs[x, pl.ds(0, half, stride=2), :] + pairs[x, pl.ds(1, half, stride=2), :]
    source, goal = iota((128, 128), 0), iota((128, 128), 1)
    means = 0.125 * pick(tmp[...], jnp.where((source // 2 == goal) & (source < 64), 1.0, 0.0))
    total = means[0:half]
    for x in range(1, count):
        total = total + pltpu.roll(means[half * x : half * x + half], 32 * x, 1)
    return total


def repeat(count, body, carry):
    if count <= 16:
        for p in range(count):
            carry = body(p, carry)
        return carry
    return lax.fori_loop(0, count, body, carry)


def spread_low(buf, whole, counts, pad):
    lane = iota((8, 128), 1)

    def body(a, carry):
        for ct in range(counts["gy"] // 2):
            for gt in range(counts["gz"] // 4):
                pieces = [
                    jnp.concatenate([buf[a, 2 * ct, 4 * gt + g], buf[a, 2 * ct + 1, 4 * gt + g]], axis=0)
                    for g in range(4)]
                for i in range(4):
                    total = pieces[0] if i == 0 else pltpu.roll(pieces[0], (-32 * i) % 128, 1)
                    for g in range(1, 4):
                        piece = pieces[g] if g == i else pltpu.roll(pieces[g], (32 * (g - i)) % 128, 1)
                        total = jnp.where(lane // 32 == g, piece, total)
                    whole[pad + 4 * a + i, 8 * ct : 8 * ct + 8, 128 * gt : 128 * gt + 128] = total
        return carry

    repeat(counts["gx"], body, 0)


def low_faces(k, faces, dims, pad):
    planes, rows, lanes = dims
    cx, cy0, cy1, cz0, cz1, cd = faces
    row, lane = iota((rows, lanes), 0), iota((rows, lanes), 1)
    scale = 0.5 * 0.0625

    def body(p, carry):
        kx = k[p + pad]
        below, above = scale * (k[p + pad - 1] + kx), scale * (kx + k[p + pad + 1])
        total = below + above
        cx[p] = below
        cx[p + 1] = above
        for target, inside, moved in (
            (cy0, row > 0, up(kx, 0)), (cy1, row < rows - 1, down(kx, 0)),
            (cz0, lane > 0, up(kx, 1)), (cz1, lane < lanes - 1, down(kx, 1))):
            face = scale * (kx + moved)
            target[p] = jnp.where(inside, face, 0.0)
            total = total + jnp.where(inside, face, scale * kx)
        cd[p] = total
        return carry

    repeat(planes, body, 0)


def bottom(f, s, vv, ww, faces, dims, pad):
    planes, rows, lanes = dims
    cx, cy0, cy1, cz0, cz1, cd = faces

    def operate(v, p):
        mid = v[p + pad]
        summed = cx[p] * v[p + pad - 1] + cx[p + 1] * v[p + pad + 1]
        summed = summed + (cy0[p] * up(mid, 0) + cy1[p] * down(mid, 0))
        summed = summed + (cz0[p] * up(mid, 1) + cz1[p] * down(mid, 1))
        return mid, cd[p] * mid - summed

    zero = jnp.zeros((rows, lanes), F32)

    def first(p, carry):
        mid, image = operate(f, p)
        vv[p + pad] = image
        return carry[0] + mid * mid, carry[1] + mid * image

    def total(v):
        return jnp.sum(jnp.sum(v, axis=0, keepdims=True), axis=1, keepdims=True)

    norm, along = repeat(planes, first, (zero, zero))
    alpha = total(norm) / total(along)

    def second(p, carry):
        ww[p] = operate(vv, p)[1]
        return carry

    repeat(planes, second, 0)

    def last(p, carry):
        rest = f[p + pad] - alpha * vv[p + pad]
        image = vv[p + pad] - alpha * ww[p]
        s[p + pad] = rest
        return carry[0] + image * rest, carry[1] + image * image

    turned, norm = repeat(planes, last, (zero, zero))
    return alpha, total(turned) / total(norm)


def pack_boxes(slots, ids, outgoing, boxes, groups):
    held = ids[0].astype(F32)
    cap = held.shape[1]
    eye = iota((cap, cap), 0) == iota((cap, cap), 1)
    rows = jnp.broadcast_to(held, (cap, cap))
    cols = jnp.broadcast_to(jnp.sum(jnp.where(eye, rows, 0.0), axis=1, keepdims=True), (cap, cap))

    def target(v):
        return jnp.floor((v + 0.5) * (1.0 / boxes))

    earlier = (target(rows) == target(cols)) & (cols < rows) & (cols >= 0.0)
    ranking = jnp.sum(jnp.where(earlier, 1.0, 0.0), axis=0, keepdims=True)
    send_row = jnp.where(held >= 0.0, target(held) * SEND + ranking, -1.0)
    count = groups * SEND
    picker = jnp.where(iota((count, cap), 0).astype(F32) == jnp.broadcast_to(send_row, (count, cap)), 1.0, 0.0)
    data = slots[0, 0].astype(F32)
    total = jnp.zeros((count, data.shape[1]), F32)
    for q in range(cap):
        total = total + picker[:, q : q + 1] * data[q : q + 1, :]
    for t in range(groups):
        outgoing[t] = total[SEND * t : SEND * t + SEND, :].astype(BF16)


def place_boxes(incoming, held, owner, rows, boxes, groups):
    me = lax.axis_index("gz")
    owners = jnp.broadcast_to(owner[0].astype(F32), (boxes, owner.shape[2]))
    here = iota(owners.shape, 1) == iota(owners.shape, 0) + me * boxes
    col = jnp.sum(jnp.where(here, owners, 0.0), axis=1, keepdims=True)
    cols = jnp.broadcast_to(col, (boxes, boxes))
    first, second = iota((boxes, boxes), 0), iota((boxes, boxes), 1)
    row = jnp.sum(jnp.where(first == second, cols, 0.0), axis=0, keepdims=True)
    before = (jnp.broadcast_to(row, (boxes, boxes)) == cols) & (second < first)
    pick = col * SEND + jnp.sum(jnp.where(before, 1.0, 0.0), axis=1, keepdims=True)
    for t in range(groups):
        held[SEND * t : SEND * t + SEND, :] = incoming[t].astype(F32)
    per = 128 // BOX
    lane_box, row = iota((boxes, 128), 1) // BOX, iota((boxes, 128), 0)
    for part in range(BOX * BOX // per):
        lanes = slice(128 * part, 128 * part + 128)
        chosen = jnp.zeros((boxes, 128), F32)
        for r in range(groups * SEND):
            chosen = jnp.where(pick == float(r), held[r : r + 1, lanes], chosen)
        total = chosen
        for d in range(1, boxes):
            moved = pltpu.roll(pltpu.roll(chosen, BOX * d, 1), boxes - d, 0)
            total = jnp.where(((lane_box - row) & (boxes - 1)) == d, moved, total)
        rows[per * part : per * part + per, :] = total
    return jnp.dot(rows[...].astype(BF16), split_lanes(False).astype(BF16), preferred_element_type=F32)


def kernel(levels, counts, names, slots_in, ids_in, owner_in, coef_in, out, *scratch):
    r = dict(zip(names, scratch))
    groups = counts["gz"]
    at = {axis: lax.axis_index(axis) for axis in counts}
    slots, ids, owner, coef, units = r["slots"], r["ids"], r["owner"], r["coef"], r["units"]
    loads = [
        pltpu.make_async_copy(source, target, r["loads"].at[n])
        for n, (source, target) in enumerate(((slots_in, slots), (ids_in, ids), (coef_in, coef), (owner_in, owner)))]
    for load in loads:
        load.start()
    fine, mid = levels["f"], levels["g"]
    sides = {tag: {name[: -len(tag)]: r[name] for name in lv.scratch(tag)} for tag, lv in levels.items()}
    for tag, lv in levels.items():
        clear_sides(lv, sides[tag])

    barrier = pltpu.get_barrier_semaphore()
    def signal_near(sem, offsets):
        count = 0
        for offset in offsets:
            target, exists = near(offset, counts)

            @pl.when(exists)
            def _():
                pl.semaphore_signal(sem, inc=1, device_id=target, device_id_type=MESH)

            count = count + jnp.where(exists, 1, 0)
        return count

    expected = signal_near(barrier, sorted([n for n in NEAR if 0 in n], key=lambda n: -sum(map(abs, n))))
    others = [{"gz": lax.rem(at["gz"] + k, groups)} for k in range(1, groups)]
    if counts["gx"] > 4 or counts["gy"] > 4:
        for offset in itertools.product(*[range(n) for n in counts.values()]):
            if any(offset):
                others.append({axis: lax.rem(at[axis] + k, counts[axis]) for axis, k in zip(counts, offset) if k})
    for target in others:
        pl.semaphore_signal(barrier, inc=1, device_id=target, device_id_type=MESH)

    sems = {tag: r["sems"].at[n] for n, tag in enumerate(("k", "c", "f", "g", "q", "e", "move", "low_k", "low_f"))}

    def send(tag, axes=(1, 2, 3)):
        send_sides(levels[tag], sides[tag], sems[tag], counts, axes)

    def take(tag, emit):
        counted = units if levels[tag].dtype == F32 else r["half_units"]
        take_sides(levels[tag], sides[tag], sems[tag], counts, counted, emit)

    loads[0].wait()
    loads[1].wait()
    boxes = out.shape[2] // BOX
    pack_boxes(slots, ids, r["outgoing"], boxes, groups)
    pl.semaphore_wait(barrier, expected + len(others))

    me = at["gz"]
    for k in range(1, groups):
        to = lax.rem(me + k, groups)
        pltpu.make_async_remote_copy(
            r["outgoing"].at[to], r["incoming"].at[me], sems["move"].at[0], sems["move"].at[1],
            device_id={"gz": to}, device_id_type=MESH).start()
    greeted = signal_near(r["hello"], list(itertools.product((-1, 1), (0,), (-1, 0, 1))))
    loads[2].wait()
    swap = lambda tile, t: jnp.where(even_rows(t, fine.y), tile, pltpu.roll(tile, 64, 1))
    split = pick(coef[...].reshape(fine.t * fine.y, 128), split_lanes(False)).reshape(fine.t, fine.y, 128)
    for t in range(fine.t):
        sides["k"]["st"][t] = swap(split[t], t)
    pack_sides(levels["k"], sides["k"])
    send("k", (1, 2))
    r["incoming"][me] = r["outgoing"][me]

    half_t, half_y = fine.t // 2, fine.y // 2
    for i in range(half_t):
        pair = sides["k"]["st"][2 * i] + sides["k"]["st"][2 * i + 1]
        r["pairs"][i] = pair + pltpu.roll(pair, 64, 1)
    coarse = 0.125 * fold_rows(r["pairs"], half_y)
    pair_planes([coarse[i] for i in range(half_t)], sides["c"]["st"])
    pack_sides(mid, sides["c"])
    pl.semaphore_wait(r["hello"], greeted)
    send("k", (3,))
    send("c")
    for i in range(half_t // 2):
        r["pairsm"][i] = coarse[2 * i] + coarse[2 * i + 1]
    here = (at["gx"], at["gy"], at["gz"])
    r["gk"][here] = coarse_low(r["pairsm"], r["tmp"])
    loads[3].wait()
    if groups > 1:
        part = r["incoming"].at[pl.ds(0, groups - 1)]
        for n in range(2):
            pltpu.make_async_copy(part, part, sems["move"].at[n]).wait()
    source = place_boxes(r["incoming"], r["held"], owner, r["rows"], boxes, groups)
    source = source.reshape(fine.t, fine.y, 128)
    for t in range(fine.t):
        sides["f"]["st"][t] = swap(source[t], t).astype(BF16)
    pack_sides(fine, sides["f"])
    send("f")

    pair_of = lambda name: (r[name + "r"], r[name + "b"])
    v0, g0, k0 = pair_of("v0"), pair_of("g0"), pair_of("k0")
    fx, fy, zo, dd0, iv0 = (pair_of(name) for name in ("fx0", "fy0", "zo0", "dd0", "iv0"))
    faces0 = (fx, fy, r["zs0"], zo)
    faces1 = (r["fx1"], r["fy1"], r["fz1"])
    dd1, iv1, v1, K1, G1, E1 = (r[name] for name in ("dd1", "iv1", "v1", "K1", "G1", "E1"))

    def store_pair(refs):
        def emit(t, first, second):
            refs[0][t] = first
            refs[1][t] = second
        return emit

    def store_planes(ref):
        def emit(t, first, second):
            ref[2 * t] = first
            ref[2 * t + 1] = second
        return emit

    take("k", store_pair(k0))
    prepare_fine(fine, k0, sides["k"]["lk"], fx, fy, r["zs0"], zo, dd0, iv0)

    def open_fine(t, red, black):
        g0[0][t] = red
        g0[1][t] = black
        v0[0][t] = red * iv0[0][t]

    take("f", open_fine)
    for reach, colour in ((3, 1), (2, 0), (1, 1)):
        half_sweep_fine(fine, v0, g0, faces0, iv0, colour, reach)
    residual_fine(fine, v0, g0, faces0, dd0, r["pairs"])

    coarse = 0.5 * fold_rows(r["pairs"], half_y)
    pair_planes([coarse[i] for i in range(half_t)], sides["g"]["st"])
    pack_sides(mid, sides["g"])
    send("g")
    take("c", store_planes(K1))
    prepare(K1, *faces1, dd1, iv1)
    for name in ("k2", "f2", "s2", "v2"):
        r[name][...] = jnp.zeros(r[name].shape, F32)
    pair_planes([v0[1][fine.wt + x, 0 : fine.y, :] for x in range(fine.t)], sides["q"]["st"])
    pack_sides(levels["q"], sides["q"])
    send("q")
    gather_start(r["gk"], sems["low_k"], counts)
    wm = 2 * mid.wt
    parity = iota((mid.ye, 128), 0) + iota((mid.ye, 128), 1)

    def open_mid(t, *planes):
        for k, plane in enumerate(planes):
            x = 2 * t + k
            G1[x] = plane
            v1[x] = jnp.where(((parity + x) & 1) == 0, plane * iv1[x], 0.0)

    take("g", open_mid)
    for reach, colour in ((3, 1), (2, 0), (1, 1)):
        half_sweep(v1, G1, faces1, iv1, colour, wm - reach, wm + half_t + reach)
    residual_pairs(v1, G1, faces1, dd1, r["pairsm"], wm)
    r["gf"][here] = coarse_low(r["pairsm"], r["tmp"])
    gather_start(r["gf"], sems["low_f"], counts)
    pair_planes([v1[wm + x, 0 : mid.y, :] for x in range(half_t)], sides["e"]["st"])
    pack_sides(mid, sides["e"])
    send("e")

    planes, rows, lanes = dims = (4 * counts["gx"], 4 * counts["gy"], 32 * counts["gz"])
    pad = wm // 2
    low = tuple(r[name] for name in ("cx", "cy0", "cy1", "cz0", "cz1", "cd"))
    take("q", store_planes(r["q0"]))
    gather_wait(sems["low_k"], counts, units)
    spread_low(r["gk"], r["k2"], counts, pad)
    low_faces(r["k2"], low, dims, pad)
    take("e", store_planes(E1))
    gather_wait(sems["low_f"], counts, units)
    spread_low(r["gf"], r["f2"], counts, pad)
    alpha, omega = bottom(r["f2"], r["s2"], r["v2"], r["w2"], low, dims, pad)
    around_low = mid.te
    for q in range(around_low):
        turned = alpha * r["f2"][4 * at["gx"] + q] + omega * r["s2"][4 * at["gx"] + q]
        plane = turned
        for c in range(1, counts["gy"]):
            turned = jnp.where(at["gy"] == c, pltpu.roll(plane, rows - 4 * c, 0), turned)
        r["local"][q, 0:8, :] = turned[0:8, :]
        r["local"][q, 8:16, :] = pltpu.roll(turned[rows - 8 : rows, :], 4, 0)
    goal = iota((lanes, 128), 1)
    cell = jnp.where(goal < 64 + wm, goal, goal - 128)
    cell = (cell + 128) // 2 - 64
    wanted = (goal < 64 + wm) | (goal >= 128 - wm)
    matrix = jnp.where((iota((lanes, 128), 0) == 32 * at["gz"] + cell) & wanted, 1.0, 0.0).astype(F32)
    spread = pick(r["local"][...].reshape(16 * around_low, lanes), matrix).reshape(around_low, 16, 128)
    for q in range(around_low):
        wide = r["wide"].at[q]
        for k in range(2):
            wide[pl.ds(k, 12, stride=2), :] = spread[q, 0:12]
        for k in range(2):
            x = 2 * q + k
            E1[x] = jnp.where(K1[x] > 0.0, E1[x] + wide[...], 0.0)
    for reach, colour in ((5, 0), (4, 1), (3, 0), (2, 1)):
        half_sweep(E1, G1, faces1, iv1, colour, wm - reach, wm + half_t + reach)

    low_w = fine.wt // 2
    row = iota((8, 128), 0)
    for i in range(half_t + 2 * low_w):
        x = wm - low_w + i
        wide = r["wide"].at[i]
        ends = jnp.where(row < low_w, E1[x, 8:16, :], pltpu.roll(E1[x, mid.ye - 8 : mid.ye, :], 4, 0))
        turned = jnp.concatenate([E1[x, 0:8, :], ends[0:4]], axis=0)
        for k in range(2):
            wide[pl.ds(k, 12, stride=2), :] = turned
        for k in range(2):
            v0[1][2 * i + k] = r["q0"][2 * i + k] + wide[...]
    for reach, colour in ((3, 0), (2, 1), (1, 0), (0, 1)):
        half_sweep_fine(fine, v0, g0, faces0, iv0, colour, reach)
    lane = iota((fine.y, 128), 1)
    for t in range(fine.t):
        red, black = (v0[c][fine.wt + t, 0 : fine.y, :] for c in range(2))
        r["joined"][t] = swap(jnp.where(lane < 64, red, pltpu.roll(black, 64, 1)), t)
    joined = pick(r["joined"][...].reshape(fine.t * fine.y, 128), split_lanes(True))
    out[...] = joined.reshape(out.shape)


def per_device(counts, old_slots, old_ids, old_owner, coefficient):
    x, y, z = coefficient.shape
    planes, rows, lanes = 4 * counts["gx"], 4 * counts["gy"], 32 * counts["gz"]
    groups, boxes = counts["gz"], z // BOX
    cells = old_slots.shape[3]
    mid = Level(x // 4, y // 2, 3, 8, 6)
    levels = {
        "k": Level(x, y, 5, 4, 3, deep=True), "f": Level(x, y, 4, 4, 2, dtype=BF16), "q": Level(x // 2, y, 2, 4, 2),
        "c": mid, "g": mid, "e": mid}
    fine, edge = levels["f"], levels["k"]
    pad = mid.wt
    devices = counts["gx"] * counts["gy"] * groups
    vmem = lambda *shape: pltpu.VMEM(shape, F32)
    dma = lambda *shape: pltpu.SemaphoreType.DMA(shape)
    scratch = {}
    for tag, level in levels.items():
        scratch.update(level.scratch(tag))
    for name in ("v0", "g0", "fx0", "fy0", "zo0", "dd0", "iv0", "k0"):
        for colour in "rb":
            scratch[name + colour] = vmem(edge.te if name == "k0" else fine.te, fine.ye, 128)
    for name in ("zs0", "q0"):
        scratch[name] = vmem(fine.te, fine.ye, 128)
    for name in ("fx1", "fy1", "fz1", "dd1", "iv1", "v1", "K1", "G1", "E1"):
        scratch[name] = vmem(2 * mid.te, mid.ye, 128)
    scratch.update(
        slots=pltpu.VMEM(old_slots.shape, old_slots.dtype), ids=pltpu.VMEM(old_ids.shape, old_ids.dtype),
        owner=pltpu.VMEM(old_owner.shape, old_owner.dtype), coef=vmem(*coefficient.shape), loads=dma(4),
        outgoing=pltpu.VMEM((groups, SEND, cells), BF16), incoming=pltpu.VMEM((groups, SEND, cells), BF16),
        held=vmem(groups * SEND, cells), sems=dma(9, 2), hello=pltpu.SemaphoreType.REGULAR, units=vmem(max(160, devices), 4, 128),
        half_units=pltpu.VMEM((160, 4, 128), BF16),
        rows=vmem(BOX * BOX, 128), pairs=vmem(x // 2, y, 128), pairsm=vmem(x // 4, y // 2, 128),
        joined=vmem(x, y, 128), tmp=vmem(x * y // 16, 128), local=vmem(mid.te, 16, lanes),
        wide=vmem(max(mid.te, fine.te // 2), 24, 128),
        gk=vmem(counts["gx"], counts["gy"], groups, 4, 128), gf=vmem(counts["gx"], counts["gy"], groups, 4, 128),
        cx=vmem(planes + 1, rows, lanes), w2=vmem(planes, rows, lanes))
    for name in ("cy0", "cy1", "cz0", "cz1", "cd"):
        scratch[name] = vmem(planes, rows, lanes)
    for name in ("f2", "k2", "s2", "v2"):
        scratch[name] = vmem(planes + 2 * pad, rows, lanes)
    return pl.pallas_call(
        functools.partial(kernel, levels, counts, tuple(scratch)),
        out_shape=jax.ShapeDtypeStruct(coefficient.shape, F32),
        in_specs=[pl.BlockSpec(memory_space=pltpu.MemorySpace.HBM)] * 4,
        out_specs=pl.BlockSpec(memory_space=pltpu.VMEM),
        scratch_shapes=list(scratch.values()),
        compiler_params=pltpu.CompilerParams(
            collective_id=0, has_side_effects=True, vmem_limit_bytes=44 * 1024 * 1024),
    )(*[pltpu.with_memory_space_constraint(v, pltpu.HBM) for v in (old_slots, old_ids, old_owner, coefficient)])


def solution(mesh):
    counts = {axis: mesh.shape[axis] for axis in ("gx", "gy", "gz")}
    return jax.shard_map(
        functools.partial(per_device, counts), mesh=mesh,
        in_specs=(P("gx", "gy", "gz", None), P("gx", "gy", "gz"), P("gx", "gy", None), P("gx", "gy", "gz")),
        out_specs=P("gx", "gy", "gz"), check_vma=False)
```

```python
import functools
import itertools

import jax
import jax.numpy as jnp
from jax import lax
from jax.experimental import pallas as pl
from jax.experimental.pallas import tpu as pltpu
from jax.sharding import PartitionSpec as P

BOX = 16
SEND = 2
F32 = jnp.float32
BF16 = jnp.bfloat16
MESH = pl.DeviceIdType.MESH
HIGH = lax.Precision.HIGHEST


def iota(shape, dim):
    return lax.broadcasted_iota(jnp.int32, shape, dim)


def up(v, axis):
    return pltpu.roll(v, 1, axis)


def down(v, axis):
    return pltpu.roll(v, v.shape[axis] - 1, axis)


class Level:
    def __init__(self, t, y, wt, wy, h, deep=False, dtype=F32):
        self.dtype = dtype
        self.t, self.y, self.wt, self.wy, self.h, self.deep = t, y, wt, wy, h, deep
        self.te, self.ye = t + 2 * wt, y + 2 * wy
        self.blocks = y // wy

    def units(self, a, b, c):
        if c:
            return (self.wy if b else self.y) // 4
        extra = self.t // 4 if self.deep and b and not a else 0
        return (self.wt if a else self.t) * (self.wy if b else self.y) // 4 + extra

    def scratch(self, tag):
        vmem = lambda *shape: pltpu.VMEM(shape + (128,), self.dtype)
        made = {
            "st": vmem(self.t, self.y), "py": vmem(2, self.t, self.wy), "lt": vmem(self.te, self.y),
            "ly": vmem(2, self.te, self.wy), "pf": vmem(self.blocks, self.wy), "pl": vmem(self.blocks, self.wy),
            "lz": vmem(2, 3, self.blocks, self.wy), "lzb": vmem(2, 3, 2, self.wy)}
        if self.deep:
            made.update(ky=vmem(2, self.t), lk=vmem(2, self.t))
        return {name + tag: value for name, value in made.items()}


NEAR = [(a, b, c) for c in (-1, 0, 1) for b in (-1, 0, 1) for a in (-1, 0, 1) if (a, b, c) != (0, 0, 0)]


def near(offset, counts):
    target, exists = {}, None
    for axis, step in zip(("gx", "gy", "gz"), offset):
        me, n = lax.axis_index(axis), counts[axis]
        if step:
            target[axis] = lax.rem(me + step + n, n)
            inside = me > 0 if step < 0 else me < n - 1
            exists = inside if exists is None else jnp.logical_and(exists, inside)
    return target, exists


def wait_units(units, count, sem):
    part = units.at[pl.ds(0, count)]
    pltpu.make_async_copy(part, part, sem).wait()


def wait_near(lv, counts, units, sems):
    choices = []
    for axis in ("gx", "gy", "gz"):
        me, n = lax.axis_index(axis), counts[axis]
        if n == 1:
            choices.append([(0, None)])
        elif n == 2:
            choices.append([(1, None)])
        else:
            edge = jnp.logical_or(me == 0, me == n - 1)
            choices.append([(1, edge), (2, jnp.logical_not(edge))])
    for chosen in itertools.product(*choices):
        total = 0
        for kind in itertools.product((0, 1), repeat=3):
            if any(kind):
                copies = 1
                for used, (number, _) in zip(kind, chosen):
                    copies *= number if used else 1
                total += copies * lv.units(*kind)
        conditions = [condition for _, condition in chosen if condition is not None]

        def wait():
            for sem in sems:
                wait_units(units, total, sem)

        if conditions:
            pl.when(functools.reduce(jnp.logical_and, conditions))(wait)
        else:
            wait()


def clear_sides(lv, b):
    b["lt"][0 : lv.wt] = jnp.zeros((lv.wt, lv.y, 128), lv.dtype)
    b["lt"][lv.t + lv.wt : lv.te] = jnp.zeros((lv.wt, lv.y, 128), lv.dtype)
    for name in ("ly", "lz", "lzb") + (("lk",) if lv.deep else ()):
        b[name][...] = jnp.zeros(b[name].shape, lv.dtype)


def pack_sides(lv, b):
    h, st, lane = lv.h, b["st"], iota((lv.y, 128), 1)
    first = last = jnp.zeros((lv.y, 128), F32)
    for t in range(lv.t):
        tile = st[t].astype(F32)
        if lv.blocks > 1:
            b["py"][0, t] = tile[0 : lv.wy].astype(lv.dtype)
            b["py"][1, t] = tile[lv.y - lv.wy : lv.y].astype(lv.dtype)
        for half in range(2):
            at = 2 * h * t + h * half
            turned = pltpu.roll(tile, (at - 64 * half) % 128, 1)
            first = jnp.where(((lane - at) & 127) < h, turned, first)
            last = jnp.where(((lane - at - 64 + h) & 127) < h, turned, last)
        if lv.deep:
            b["ky"][0, t : t + 1, :] = tile[lv.wy : lv.wy + 1, :]
            b["ky"][1, t : t + 1, :] = tile[lv.y - lv.wy - 1 : lv.y - lv.wy, :]
    for block in range(lv.blocks):
        rows = slice(block * lv.wy, block * lv.wy + lv.wy)
        b["pf"][block], b["pl"][block] = first[rows].astype(lv.dtype), last[rows].astype(lv.dtype)


def send_sides(lv, b, sems, counts, axes):
    taken = {-1: (0, lv.wt), 0: (0, lv.t), 1: (lv.t - lv.wt, lv.wt)}
    landed = {-1: lv.t + lv.wt, 0: lv.wt, 1: 0}
    pair = counts["gy"] == 2
    me = lax.axis_index("gy")

    def start(x, y, z):
        target = near((x, y, z), counts)[0]
        first, count = taken[x]
        source, goal = pl.ds(first, count), pl.ds(landed[x], count)
        side = 1 - me if pair else (y + 1) // 2
        if z:
            ends = b["pf"] if z < 0 else b["pl"]
            if y:
                pairs = [(ends.at[side * (lv.blocks - 1)], b["lzb"].at[(1 - z) // 2, 1 - x, 1 - side])]
            else:
                pairs = [(ends, b["lz"].at[(1 - z) // 2, 1 - x])]
        elif y:
            pairs = [(b["py"].at[side, source] if lv.blocks > 1 else b["st"].at[source], b["ly"].at[side, goal])]
            if lv.deep and not x:
                pairs.append((b["ky"].at[side], b["lk"].at[side]))
        else:
            pairs = [(b["st"].at[source], b["lt"].at[goal])]
        for src, dst in pairs:
            pltpu.make_async_remote_copy(
                src, dst, sems.at[0], sems.at[1], device_id=target, device_id_type=MESH).start()

    steps = (1, 0) if pair else (1, -1, 0)
    for x, z in sorted(itertools.product((-1, 0, 1), repeat=2), key=lambda n: -abs(n[0]) - abs(n[1])):
        chosen = [y for y in steps if abs(x) + abs(y) + abs(z) in axes]

        def send():
            for y in chosen:
                if pair or not y:
                    start(x, y, z)
                else:
                    pl.when(near((0, y, 0), counts)[1])(functools.partial(start, x, y, z))

        exists = near((x, 0, z), counts)[1]
        if chosen:
            send() if exists is None else pl.when(exists)(send)


def take_sides(lv, b, sems, counts, units, emit):
    h, wt = lv.h, lv.wt
    wait_near(lv, counts, units, (sems.at[0], sems.at[1]))
    lane = iota((lv.ye, 128), 1)
    own, edge = lane < 64, (lane < 64 + h) | (lane >= 128 - h)
    for a in range(3):
        low, high = [
            jnp.concatenate(
                [b["lz"][c, a, block].astype(F32) for block in range(lv.blocks)]
                + [b["lzb"][c, a, side].astype(F32) for side in (1, 0)], axis=0)
            for c in range(2)]
        mixed = [jnp.where(((lane - 16 * h * q + h) & 127) < 64, high, low) for q in range(-(-lv.t // 8))]
        place = (0, wt, lv.t + wt)[a]
        start, count = ((lv.t - wt, wt), (0, lv.t), (0, wt))[a]
        for k in range(count):
            n, t = start + k, place + k
            rows = b["st"][n] if a == 1 else b["lt"][t]
            full = jnp.concatenate([part.astype(F32) for part in (rows, b["ly"][0, t], b["ly"][1, t])], axis=0)
            slices = []
            for half in range(2):
                ends = pltpu.roll(mixed[n // 8], (64 - 2 * h * n - h * half) % 128, 1)
                values = pltpu.roll(full, 64, 1) if half else full
                slices.append(jnp.where(own, values, jnp.where(edge, ends, 0.0)))
            emit(t, *slices)


def gather_start(buf, sems, counts):
    me = {axis: lax.axis_index(axis) for axis in counts}
    mine = buf.at[me["gx"], me["gy"], me["gz"]]
    ranges = [[n - k if k else 0 for k in range(n)] for n in counts.values()]
    for offset in sorted(itertools.product(*ranges), key=lambda o: -sum(1 for k in o if k)):
        if any(offset):
            target = {
                axis: lax.rem(me[axis] + jnp.where(me[axis] < counts[axis] // 2, k, counts[axis] - k), counts[axis])
                for axis, k in zip(counts, offset) if k}
            pltpu.make_async_remote_copy(
                mine, mine, sems.at[0], sems.at[1], device_id=target, device_id_type=MESH).start()


def gather_wait(sems, counts, units):
    others = counts["gx"] * counts["gy"] * counts["gz"] - 1
    if others:
        wait_units(units, others, sems.at[0])
        wait_units(units, others, sems.at[1])


def batches(low, high, size, body):
    whole = (high - low) // size
    if whole == 1:
        body(low, size)
    elif whole:
        def run(step, carry):
            body(low + step * size, size)
            return carry

        lax.fori_loop(0, whole, run, 0)
    if low + whole * size < high:
        body(low + whole * size, high - low - whole * size)


def even_rows(x, rows):
    return ((iota((rows, 128), 0) + x) & 1) == 0


def prepare_fine(lv, k, rows, fx, fy, zs, zo, dd, iv):
    row = iota((lv.ye, 128), 0)

    def body(first, count, inside=False):
        made = []
        for x in [first + i for i in range(count)]:
            first_red = even_rows(x, lv.ye)
            mids = [k[c][x + 1] for c in range(2)]
            for c in range(2):
                kx, other = mids[c], mids[1 - c]
                below = 0.5 * (k[1 - c][x] + kx)
                above = 0.5 * (kx + k[1 - c][x + 2])
                lower, upper = up(other, 0), down(other, 0)
                if inside:
                    ends = [jnp.broadcast_to(rows[side, pl.ds(x - lv.wt, 1), :], (lv.ye, 128)) for side in range(2)]
                    if c == 0:
                        ends = [pltpu.roll(end, 64, 1) for end in ends]
                    upper = jnp.where(row == lv.y + lv.wy - 1, ends[0], upper)
                    lower = jnp.where(row == lv.y + lv.wy, ends[1], lower)
                second = 0.5 * (lower + kx)
                same = 0.5 * (kx + other)
                moved = [up(other, 1), down(other, 1)]
                third = 0.5 * (kx + jnp.where(first_red, moved[c], moved[1 - c]))
                total = below + above + second + 0.5 * (kx + upper) + same + third
                made.append((x, c, below, second, third, total, jnp.where(kx > 0.0, 1.0 / total, 0.0), same))
        for x, c, *values, same in made:
            for ref, value in zip((fx, fy, zo, dd, iv), values):
                ref[c][x] = value
            if c == 0:
                zs[x] = same

    batches(0, lv.wt, 4, body)
    batches(lv.wt, lv.wt + lv.t, 8, functools.partial(body, inside=True))
    batches(lv.wt + lv.t, lv.te, 4, body)


def around_fine(lv, v, c, x, faces):
    fx, fy, zs, zo = faces
    o = 1 - c
    mid, first_red = v[o][x], even_rows(x, lv.ye)
    moved = [up(mid, 1), down(mid, 1)]
    summed = fx[c][x] * v[o][x - 1] + fx[o][x + 1] * v[o][x + 1]
    summed = summed + fy[c][x] * up(mid, 0) + down(fy[o][x] * mid, 0)
    return summed + zs[x] * mid + zo[c][x] * jnp.where(first_red, moved[c], moved[o])


def half_sweep_fine(lv, v, g, faces, iv, c, reach):
    low, high = lv.wt - reach, lv.wt + lv.t + reach

    def body(first, count):
        fresh = [(x, (g[c][x] + around_fine(lv, v, c, x, faces)) * iv[c][x]) for x in [first + i for i in range(count)]]
        for x, value in fresh:
            v[c][x] = value

    batches(low, high, high - low, body)


def residual_fine(lv, v, g, faces, dd, pairs):
    def body(first, count):
        made = []
        for i in [first + j for j in range(count)]:
            total = jnp.zeros((lv.ye, 128), F32)
            for x in (lv.wt + 2 * i, lv.wt + 2 * i + 1):
                for c in range(2):
                    total = total + (g[c][x] - dd[c][x] * v[c][x] + around_fine(lv, v, c, x, faces))
            made.append((i, total))
        for i, total in made:
            pairs[i] = total[0 : lv.y, :]

    batches(0, lv.t // 2, lv.t // 2, body)


def even_cells(shape):
    return ((iota(shape, 0) + iota(shape, 1)) & 1) == 0


def merge_planes(first, second):
    even = even_cells(first.shape)
    return jnp.where(even, first, second), jnp.where(even, second, first)


def beside(v, c, t):
    low, high = v[1 - c][max(t - 1, 0)], v[1 - c][min(t + 1, v[1 - c].shape[0] - 1)]
    even = even_cells(low.shape)
    return jnp.where(even, low, high) if c == 0 else jnp.where(even, high, low)


def prepare_mid(k, xs, xo, fy, fz, dd, iv):
    for t in range(xs.shape[0]):
        same = 0.5 * (k[0][t] + k[1][t])
        xs[t] = same
        second, third = [], []
        for c in range(2):
            second.append(0.5 * (up(k[1 - c][t], 0) + k[c][t]))
            third.append(0.5 * (up(k[1 - c][t], 1) + k[c][t]))
        for c in range(2):
            o, kx = 1 - c, k[c][t]
            other = 0.5 * (beside(k, c, t) + kx)
            total = same + other + second[c] + down(second[o], 0) + third[c] + down(third[o], 1)
            xo[c][t], fy[c][t], fz[c][t], dd[c][t] = other, second[c], third[c], total
            iv[c][t] = jnp.where(kx > 0.0, 1.0 / total, 0.0)


def around_mid(v, c, t, faces):
    xs, xo, fy, fz = faces
    o = 1 - c
    mid = v[o][t]
    summed = xs[t] * mid + xo[c][t] * beside(v, c, t)
    summed = summed + fy[c][t] * up(mid, 0) + down(fy[o][t] * mid, 0)
    return summed + fz[c][t] * up(mid, 1) + down(fz[o][t] * mid, 1)


def half_sweep_mid(lv, v, g, faces, iv, c, reach):
    low, high = 2 * lv.wt - reach, 2 * (lv.wt + lv.t) + reach
    fresh = [
        (t, (g[c][t] + around_mid(v, c, t, faces)) * iv[c][t]) for t in range(low // 2, (high + 1) // 2)]
    for t, value in fresh:
        v[c][t] = value


def residual_mid(lv, v, g, faces, dd, pairs):
    for i in range(lv.t):
        t = lv.wt + i
        total = 0.0
        for c in range(2):
            total = total + (g[c][t] - dd[c][t] * v[c][t] + around_mid(v, c, t, faces))
        pairs[i] = 0.25 * total[0 : lv.y]


def pair_planes(planes, target):
    lane = iota(planes[0].shape, 1)
    for t in range(len(planes) // 2):
        target[t] = jnp.where(lane < 64, planes[2 * t], pltpu.roll(planes[2 * t + 1], 64, 1))


def fold_rows(pairs, rows):
    return pairs[:, pl.ds(0, rows, stride=2), :] + pairs[:, pl.ds(1, rows, stride=2), :]


def dot(a, b):
    return jnp.dot(a, b, precision=HIGH, preferred_element_type=F32)


def pick(values, matrix):
    parts, rest = [], values
    for _ in range(3):
        parts.append(rest.astype(BF16))
        rest = rest - parts[-1].astype(F32)
    return jnp.dot(
        jnp.concatenate(parts, axis=1), jnp.concatenate([matrix.astype(BF16)] * 3, axis=0), preferred_element_type=F32)


def split_lanes(transposed):
    cell, lane = iota((128, 128), int(transposed)), iota((128, 128), 1 - int(transposed))
    return jnp.where(lane == cell // 2 + 64 * (cell % 2), 1.0, 0.0).astype(F32)


def coarse_low(pairs, tmp):
    count, rows, _ = pairs.shape
    half = rows // 2
    for x in range(count):
        tmp[half * x : half * x + half, :] = pairs[x, pl.ds(0, half, stride=2), :] + pairs[x, pl.ds(1, half, stride=2), :]
    source, goal = iota((128, 128), 0), iota((128, 128), 1)
    means = 0.125 * pick(tmp[...], jnp.where((source // 2 == goal) & (source < 64), 1.0, 0.0))
    total = means[0:half]
    for x in range(1, count):
        total = total + pltpu.roll(means[half * x : half * x + half], 32 * x, 1)
    return total


def repeat(count, body, carry):
    if count <= 16:
        for p in range(count):
            carry = body(p, carry)
        return carry
    return lax.fori_loop(0, count, body, carry)


def spread_low(buf, whole, counts, pad):
    lane = iota((8, 128), 1)

    def body(a, carry):
        for ct in range(counts["gy"] // 2):
            for gt in range(counts["gz"] // 4):
                pieces = [
                    jnp.concatenate([buf[a, 2 * ct, 4 * gt + g], buf[a, 2 * ct + 1, 4 * gt + g]], axis=0)
                    for g in range(4)]
                for i in range(4):
                    total = pieces[0] if i == 0 else pltpu.roll(pieces[0], (-32 * i) % 128, 1)
                    for g in range(1, 4):
                        piece = pieces[g] if g == i else pltpu.roll(pieces[g], (32 * (g - i)) % 128, 1)
                        total = jnp.where(lane // 32 == g, piece, total)
                    whole[pad + 4 * a + i, 8 * ct : 8 * ct + 8, 128 * gt : 128 * gt + 128] = total
        return carry

    repeat(counts["gx"], body, 0)


def low_faces(k, faces, dims, pad):
    planes, rows, lanes = dims
    cx, cy0, cy1, cz0, cz1, cd = faces
    row, lane = iota((rows, lanes), 0), iota((rows, lanes), 1)
    scale = 0.5 * 0.0625

    def body(p, carry):
        kx = k[p + pad]
        below, above = scale * (k[p + pad - 1] + kx), scale * (kx + k[p + pad + 1])
        total = below + above
        cx[p] = below
        cx[p + 1] = above
        for target, inside, moved in (
            (cy0, row > 0, up(kx, 0)), (cy1, row < rows - 1, down(kx, 0)),
            (cz0, lane > 0, up(kx, 1)), (cz1, lane < lanes - 1, down(kx, 1))):
            face = scale * (kx + moved)
            target[p] = jnp.where(inside, face, 0.0)
            total = total + jnp.where(inside, face, scale * kx)
        cd[p] = total
        return carry

    repeat(planes, body, 0)


def bottom(f, s, vv, ww, faces, dims, pad):
    planes, rows, lanes = dims
    cx, cy0, cy1, cz0, cz1, cd = faces

    def operate(v, p):
        mid = v[p + pad]
        summed = cx[p] * v[p + pad - 1] + cx[p + 1] * v[p + pad + 1]
        summed = summed + (cy0[p] * up(mid, 0) + cy1[p] * down(mid, 0))
        summed = summed + (cz0[p] * up(mid, 1) + cz1[p] * down(mid, 1))
        return mid, cd[p] * mid - summed

    zero = jnp.zeros((rows, lanes), F32)

    def first(p, carry):
        mid, image = operate(f, p)
        vv[p + pad] = image
        return carry[0] + mid * mid, carry[1] + mid * image

    def total(v):
        return jnp.sum(jnp.sum(v, axis=0, keepdims=True), axis=1, keepdims=True)

    norm, along = repeat(planes, first, (zero, zero))
    alpha = total(norm) / total(along)

    def second(p, carry):
        ww[p] = operate(vv, p)[1]
        return carry

    repeat(planes, second, 0)

    def last(p, carry):
        rest = f[p + pad] - alpha * vv[p + pad]
        image = vv[p + pad] - alpha * ww[p]
        s[p + pad] = rest
        return carry[0] + image * rest, carry[1] + image * image

    turned, norm = repeat(planes, last, (zero, zero))
    return alpha, total(turned) / total(norm)


def pack_boxes(slots, ids, outgoing, boxes, groups):
    held = ids[0].astype(F32)
    cap = held.shape[1]
    eye = iota((cap, cap), 0) == iota((cap, cap), 1)
    rows = jnp.broadcast_to(held, (cap, cap))
    cols = jnp.broadcast_to(jnp.sum(jnp.where(eye, rows, 0.0), axis=1, keepdims=True), (cap, cap))

    def target(v):
        return jnp.floor((v + 0.5) * (1.0 / boxes))

    earlier = (target(rows) == target(cols)) & (cols < rows) & (cols >= 0.0)
    ranking = jnp.sum(jnp.where(earlier, 1.0, 0.0), axis=0, keepdims=True)
    send_row = jnp.where(held >= 0.0, target(held) * SEND + ranking, -1.0)
    count = groups * SEND
    picker = jnp.where(iota((count, cap), 0).astype(F32) == jnp.broadcast_to(send_row, (count, cap)), 1.0, 0.0)
    data = slots[0, 0].astype(F32)
    total = jnp.zeros((count, data.shape[1]), F32)
    for q in range(cap):
        total = total + picker[:, q : q + 1] * data[q : q + 1, :]
    for t in range(groups):
        outgoing[t] = total[SEND * t : SEND * t + SEND, :].astype(BF16)


def choose_boxes(owner, boxes):
    me = lax.axis_index("gz")
    owners = jnp.broadcast_to(owner[0].astype(F32), (boxes, owner.shape[2]))
    here = iota(owners.shape, 1) == iota(owners.shape, 0) + me * boxes
    col = jnp.sum(jnp.where(here, owners, 0.0), axis=1, keepdims=True)
    cols = jnp.broadcast_to(col, (boxes, boxes))
    first, second = iota((boxes, boxes), 0), iota((boxes, boxes), 1)
    row = jnp.sum(jnp.where(first == second, cols, 0.0), axis=0, keepdims=True)
    before = (jnp.broadcast_to(row, (boxes, boxes)) == cols) & (second < first)
    pick = col * SEND + jnp.sum(jnp.where(before, 1.0, 0.0), axis=1, keepdims=True)
    return pick


def place_boxes(incoming, held, pick, rows, boxes, groups):
    for t in range(groups):
        held[SEND * t : SEND * t + SEND, :] = incoming[t].astype(F32)
    per = 128 // BOX
    lane_box, row = iota((boxes, 128), 1) // BOX, iota((boxes, 128), 0)
    for part in range(BOX * BOX // per):
        lanes = slice(128 * part, 128 * part + 128)
        chosen = jnp.zeros((boxes, 128), F32)
        for r in range(groups * SEND):
            chosen = jnp.where(pick == float(r), held[r : r + 1, lanes], chosen)
        total = chosen
        for d in range(1, boxes):
            moved = pltpu.roll(pltpu.roll(chosen, BOX * d, 1), boxes - d, 0)
            total = jnp.where(((lane_box - row) & (boxes - 1)) == d, moved, total)
        rows[per * part : per * part + per, :] = total
    return jnp.dot(rows[...].astype(BF16), split_lanes(False).astype(BF16), preferred_element_type=F32)


def kernel(levels, counts, names, slots_in, ids_in, owner_in, coef_in, out, *scratch):
    r = dict(zip(names, scratch))
    groups = counts["gz"]
    at = {axis: lax.axis_index(axis) for axis in counts}
    slots, ids, owner, coef, units = r["slots"], r["ids"], r["owner"], r["coef"], r["units"]
    loads = [
        pltpu.make_async_copy(source, target, r["loads"].at[n])
        for n, (source, target) in enumerate(((slots_in, slots), (ids_in, ids), (coef_in, coef), (owner_in, owner)))]
    for load in loads:
        load.start()
    fine, mid = levels["f"], levels["g"]
    sides = {tag: {name[: -len(tag)]: r[name] for name in lv.scratch(tag)} for tag, lv in levels.items()}
    for tag, lv in levels.items():
        clear_sides(lv, sides[tag])

    barrier = pltpu.get_barrier_semaphore()
    def signal_near(sem, offsets):
        count = 0
        for offset in offsets:
            target, exists = near(offset, counts)

            @pl.when(exists)
            def _():
                pl.semaphore_signal(sem, inc=1, device_id=target, device_id_type=MESH)

            count = count + jnp.where(exists, 1, 0)
        return count

    expected = signal_near(barrier, sorted([n for n in NEAR if 0 in n], key=lambda n: -sum(map(abs, n))))
    others = [{"gz": lax.rem(at["gz"] + k, groups)} for k in range(1, groups)]
    if counts["gx"] > 4 or counts["gy"] > 4:
        for offset in itertools.product(*[range(n) for n in counts.values()]):
            if any(offset):
                others.append({axis: lax.rem(at[axis] + k, counts[axis]) for axis, k in zip(counts, offset) if k})
    for target in others:
        pl.semaphore_signal(barrier, inc=1, device_id=target, device_id_type=MESH)

    sems = {tag: r["sems"].at[n] for n, tag in enumerate(("k", "c", "f", "g", "q", "e", "move", "low_k", "low_f"))}

    def send(tag, axes=(1, 2, 3)):
        send_sides(levels[tag], sides[tag], sems[tag], counts, axes)

    def take(tag, emit):
        counted = units if levels[tag].dtype == F32 else r["half_units"]
        take_sides(levels[tag], sides[tag], sems[tag], counts, counted, emit)

    loads[0].wait()
    loads[1].wait()
    boxes = out.shape[2] // BOX
    pack_boxes(slots, ids, r["outgoing"], boxes, groups)
    pl.semaphore_wait(barrier, expected + len(others))

    me = at["gz"]
    for k in range(1, groups):
        to = lax.rem(me + k, groups)
        pltpu.make_async_remote_copy(
            r["outgoing"].at[to], r["incoming"].at[me], sems["move"].at[0], sems["move"].at[1],
            device_id={"gz": to}, device_id_type=MESH).start()
    greeted = signal_near(r["hello"], list(itertools.product((-1, 1), (0,), (-1, 0, 1))))
    loads[2].wait()
    swap = lambda tile, t: jnp.where(even_rows(t, fine.y), tile, pltpu.roll(tile, 64, 1))
    split = pick(coef[...].reshape(fine.t * fine.y, 128), split_lanes(False)).reshape(fine.t, fine.y, 128)
    for t in range(fine.t):
        sides["k"]["st"][t] = swap(split[t], t)
    pack_sides(levels["k"], sides["k"])
    send("k", (1, 2))
    r["incoming"][me] = r["outgoing"][me]

    half_t, half_y = fine.t // 2, fine.y // 2
    for i in range(half_t):
        pair = sides["k"]["st"][2 * i] + sides["k"]["st"][2 * i + 1]
        r["pairs"][i] = pair + pltpu.roll(pair, 64, 1)
    coarse = 0.125 * fold_rows(r["pairs"], half_y)
    merged = [merge_planes(coarse[i], coarse[i + 1]) for i in range(0, half_t, 2)]
    pair_planes([plane for pair in merged for plane in pair], sides["c"]["st"])
    pack_sides(mid, sides["c"])
    pl.semaphore_wait(r["hello"], greeted)
    send("k", (3,))
    send("c")
    for i in range(half_t // 2):
        r["pairsm"][i] = coarse[2 * i] + coarse[2 * i + 1]
    here = (at["gx"], at["gy"], at["gz"])
    r["gk"][here] = coarse_low(r["pairsm"], r["tmp"])
    loads[3].wait()
    r["pick"][...] = jnp.broadcast_to(choose_boxes(owner, boxes), r["pick"].shape)
    if groups > 1:
        part = r["incoming"].at[pl.ds(0, groups - 1)]
        for n in range(2):
            pltpu.make_async_copy(part, part, sems["move"].at[n]).wait()
    source = place_boxes(r["incoming"], r["held"], r["pick"][...], r["rows"], boxes, groups)
    source = source.reshape(fine.t, fine.y, 128)
    for t in range(fine.t):
        sides["f"]["st"][t] = swap(source[t], t).astype(BF16)
    pack_sides(fine, sides["f"])
    send("f")

    pair_of = lambda name: (r[name + "r"], r[name + "b"])
    v0, g0, k0 = pair_of("v0"), pair_of("g0"), pair_of("k0")
    fx, fy, zo, dd0, iv0 = (pair_of(name) for name in ("fx0", "fy0", "zo0", "dd0", "iv0"))
    faces0 = (fx, fy, r["zs0"], zo)
    fx1, fy1, fz1, dd1, iv1, v1, g1, k1 = (pair_of(n) for n in ("fx1", "fy1", "fz1", "dd1", "iv1", "v1", "g1", "k1"))
    faces1 = (r["xs1"], fx1, fy1, fz1)

    def store_pair(refs):
        def emit(t, first, second):
            refs[0][t] = first
            refs[1][t] = second
        return emit

    def store_planes(ref):
        def emit(t, first, second):
            ref[2 * t] = first
            ref[2 * t + 1] = second
        return emit

    take("k", store_pair(k0))
    prepare_fine(fine, k0, sides["k"]["lk"], fx, fy, r["zs0"], zo, dd0, iv0)

    def open_fine(t, red, black):
        g0[0][t] = red
        g0[1][t] = black
        v0[0][t] = red * iv0[0][t]

    take("f", open_fine)
    for reach, colour in ((3, 1), (2, 0), (1, 1)):
        half_sweep_fine(fine, v0, g0, faces0, iv0, colour, reach)
    residual_fine(fine, v0, g0, faces0, dd0, r["pairs"])

    coarse = 0.5 * fold_rows(r["pairs"], half_y)
    merged = [merge_planes(coarse[i], coarse[i + 1]) for i in range(0, half_t, 2)]
    pair_planes([plane for pair in merged for plane in pair], sides["g"]["st"])
    pack_sides(mid, sides["g"])
    send("g")
    take("c", store_pair(k1))
    prepare_mid(k1, *faces1, dd1, iv1)
    for name in ("k2", "f2", "s2", "v2"):
        r[name][...] = jnp.zeros(r[name].shape, F32)
    pair_planes([v0[1][fine.wt + x, 0 : fine.y, :] for x in range(fine.t)], sides["q"]["st"])
    pack_sides(levels["q"], sides["q"])
    send("q")
    gather_start(r["gk"], sems["low_k"], counts)
    wm = 2 * mid.wt

    def open_mid(t, red, black):
        g1[0][t] = red
        g1[1][t] = black
        v1[0][t] = red * iv1[0][t]

    take("g", open_mid)
    for reach, colour in ((3, 1), (2, 0), (1, 1)):
        half_sweep_mid(mid, v1, g1, faces1, iv1, colour, reach)
    residual_mid(mid, v1, g1, faces1, dd1, r["pairsm"])
    r["gf"][here] = coarse_low(r["pairsm"], r["tmp"])
    gather_start(r["gf"], sems["low_f"], counts)
    pair_planes([v1[c][mid.wt + t, 0 : mid.y, :] for t in range(mid.t) for c in range(2)], sides["e"]["st"])
    pack_sides(mid, sides["e"])
    send("e")

    planes, rows, lanes = dims = (4 * counts["gx"], 4 * counts["gy"], 32 * counts["gz"])
    pad = wm // 2
    low = tuple(r[name] for name in ("cx", "cy0", "cy1", "cz0", "cz1", "cd"))
    take("q", store_planes(r["q0"]))
    gather_wait(sems["low_k"], counts, units)
    spread_low(r["gk"], r["k2"], counts, pad)
    low_faces(r["k2"], low, dims, pad)
    take("e", store_pair(v1))
    gather_wait(sems["low_f"], counts, units)
    spread_low(r["gf"], r["f2"], counts, pad)
    alpha, omega = bottom(r["f2"], r["s2"], r["v2"], r["w2"], low, dims, pad)
    around_low = mid.te
    for q in range(around_low):
        turned = alpha * r["f2"][4 * at["gx"] + q] + omega * r["s2"][4 * at["gx"] + q]
        plane = turned
        for c in range(1, counts["gy"]):
            turned = jnp.where(at["gy"] == c, pltpu.roll(plane, rows - 4 * c, 0), turned)
        r["local"][q, 0:8, :] = turned[0:8, :]
        r["local"][q, 8:16, :] = pltpu.roll(turned[rows - 8 : rows, :], 4, 0)
    goal = iota((lanes, 128), 1)
    cell = jnp.where(goal < 64 + wm, goal, goal - 128)
    cell = (cell + 128) // 2 - 64
    wanted = (goal < 64 + wm) | (goal >= 128 - wm)
    matrix = jnp.where((iota((lanes, 128), 0) == 32 * at["gz"] + cell) & wanted, 1.0, 0.0).astype(F32)
    spread = pick(r["local"][...].reshape(16 * around_low, lanes), matrix).reshape(around_low, 16, 128)
    for q in range(around_low):
        wide = r["wide"].at[q]
        for k in range(2):
            wide[pl.ds(k, 12, stride=2), :] = spread[q, 0:12]
        v1[1][q] = jnp.where(k1[1][q] > 0.0, v1[1][q] + wide[...], 0.0)
    for reach, colour in ((5, 0), (4, 1), (3, 0), (2, 1)):
        half_sweep_mid(mid, v1, g1, faces1, iv1, colour, reach)

    low_w = fine.wt // 2
    row = iota((8, 128), 0)
    for i in range(half_t + 2 * low_w):
        x = wm - low_w + i
        wide = r["wide"].at[i]
        plane = merge_planes(v1[0][x // 2], v1[1][x // 2])[x % 2]
        ends = jnp.where(row < low_w, plane[8:16], pltpu.roll(plane[mid.ye - 8 : mid.ye], 4, 0))
        turned = jnp.concatenate([plane[0:8], ends[0:4]], axis=0)
        for k in range(2):
            wide[pl.ds(k, 12, stride=2), :] = turned
        for k in range(2):
            v0[1][2 * i + k] = r["q0"][2 * i + k] + wide[...]
    for reach, colour in ((3, 0), (2, 1), (1, 0), (0, 1)):
        half_sweep_fine(fine, v0, g0, faces0, iv0, colour, reach)
    lane = iota((fine.y, 128), 1)
    for t in range(fine.t):
        red, black = (v0[c][fine.wt + t, 0 : fine.y, :] for c in range(2))
        r["joined"][t] = swap(jnp.where(lane < 64, red, pltpu.roll(black, 64, 1)), t)
    joined = pick(r["joined"][...].reshape(fine.t * fine.y, 128), split_lanes(True))
    out[...] = joined.reshape(out.shape)


def per_device(counts, old_slots, old_ids, old_owner, coefficient):
    x, y, z = coefficient.shape
    planes, rows, lanes = 4 * counts["gx"], 4 * counts["gy"], 32 * counts["gz"]
    groups, boxes = counts["gz"], z // BOX
    cells = old_slots.shape[3]
    mid = Level(x // 4, y // 2, 3, 8, 6)
    levels = {
        "k": Level(x, y, 5, 4, 3, deep=True), "f": Level(x, y, 4, 4, 2, dtype=BF16), "q": Level(x // 2, y, 2, 4, 2),
        "c": mid, "g": mid, "e": mid}
    fine, edge = levels["f"], levels["k"]
    pad = mid.wt
    devices = counts["gx"] * counts["gy"] * groups
    vmem = lambda *shape: pltpu.VMEM(shape, F32)
    dma = lambda *shape: pltpu.SemaphoreType.DMA(shape)
    scratch = {}
    for tag, level in levels.items():
        scratch.update(level.scratch(tag))
    for name in ("v0", "g0", "fx0", "fy0", "zo0", "dd0", "iv0", "k0"):
        for colour in "rb":
            scratch[name + colour] = vmem(edge.te if name == "k0" else fine.te, fine.ye, 128)
    for name in ("zs0", "q0"):
        scratch[name] = vmem(fine.te, fine.ye, 128)
    for name in ("fx1", "fy1", "fz1", "dd1", "iv1", "v1", "g1", "k1"):
        for colour in "rb":
            scratch[name + colour] = vmem(mid.te, mid.ye, 128)
    scratch["xs1"] = vmem(mid.te, mid.ye, 128)
    scratch.update(
        slots=pltpu.VMEM(old_slots.shape, old_slots.dtype), ids=pltpu.VMEM(old_ids.shape, old_ids.dtype),
        owner=pltpu.VMEM(old_owner.shape, old_owner.dtype), coef=vmem(*coefficient.shape), loads=dma(4),
        outgoing=pltpu.VMEM((groups, SEND, cells), BF16), incoming=pltpu.VMEM((groups, SEND, cells), BF16),
        held=vmem(groups * SEND, cells), sems=dma(9, 2), hello=pltpu.SemaphoreType.REGULAR, units=vmem(max(160, devices), 4, 128),
        half_units=pltpu.VMEM((160, 4, 128), BF16),
        rows=vmem(BOX * BOX, 128), pick=vmem(boxes, 128), pairs=vmem(x // 2, y, 128), pairsm=vmem(x // 4, y // 2, 128),
        joined=vmem(x, y, 128), tmp=vmem(x * y // 16, 128), local=vmem(mid.te, 16, lanes),
        wide=vmem(max(mid.te, fine.te // 2), 24, 128),
        gk=vmem(counts["gx"], counts["gy"], groups, 4, 128), gf=vmem(counts["gx"], counts["gy"], groups, 4, 128),
        cx=vmem(planes + 1, rows, lanes), w2=vmem(planes, rows, lanes))
    for name in ("cy0", "cy1", "cz0", "cz1", "cd"):
        scratch[name] = vmem(planes, rows, lanes)
    for name in ("f2", "k2", "s2", "v2"):
        scratch[name] = vmem(planes + 2 * pad, rows, lanes)
    return pl.pallas_call(
        functools.partial(kernel, levels, counts, tuple(scratch)),
        out_shape=jax.ShapeDtypeStruct(coefficient.shape, F32),
        in_specs=[pl.BlockSpec(memory_space=pltpu.MemorySpace.HBM)] * 4,
        out_specs=pl.BlockSpec(memory_space=pltpu.VMEM),
        scratch_shapes=list(scratch.values()),
        compiler_params=pltpu.CompilerParams(
            collective_id=0, has_side_effects=True, vmem_limit_bytes=44 * 1024 * 1024),
    )(*[pltpu.with_memory_space_constraint(v, pltpu.HBM) for v in (old_slots, old_ids, old_owner, coefficient)])


def solution(mesh):
    counts = {axis: mesh.shape[axis] for axis in ("gx", "gy", "gz")}
    return jax.shard_map(
        functools.partial(per_device, counts), mesh=mesh,
        in_specs=(P("gx", "gy", "gz", None), P("gx", "gy", "gz"), P("gx", "gy", None), P("gx", "gy", "gz")),
        out_specs=P("gx", "gy", "gz"), check_vma=False)
```

```python
import functools
import itertools

import jax
import jax.numpy as jnp
from jax import lax
from jax.experimental import pallas as pl
from jax.experimental.pallas import tpu as pltpu
from jax.sharding import PartitionSpec as P

BOX = 16
SEND = 2
F32 = jnp.float32
BF16 = jnp.bfloat16
MESH = pl.DeviceIdType.MESH
HIGH = lax.Precision.HIGHEST


def iota(shape, dim):
    return lax.broadcasted_iota(jnp.int32, shape, dim)


def up(v, axis):
    return pltpu.roll(v, 1, axis)


def down(v, axis):
    return pltpu.roll(v, v.shape[axis] - 1, axis)


class Level:
    def __init__(self, t, y, wt, wy, h, deep=False, dtype=F32):
        self.dtype = dtype
        self.t, self.y, self.wt, self.wy, self.h, self.deep = t, y, wt, wy, h, deep
        self.te, self.ye = t + 2 * wt, y + 2 * wy
        self.blocks = y // wy

    def units(self, a, b, c):
        if c:
            return (self.wy if b else self.y) // 4
        extra = self.t // 4 if self.deep and b and not a else 0
        return (self.wt if a else self.t) * (self.wy if b else self.y) // 4 + extra

    def scratch(self, tag):
        vmem = lambda *shape: pltpu.VMEM(shape + (128,), self.dtype)
        made = {
            "st": vmem(self.t, self.y), "py": vmem(2, self.t, self.wy), "lt": vmem(self.te, self.y),
            "ly": vmem(2, self.te, self.wy), "pf": vmem(self.blocks, self.wy), "pl": vmem(self.blocks, self.wy),
            "lz": vmem(2, 3, self.blocks, self.wy), "lzb": vmem(2, 3, 2, self.wy)}
        if self.deep:
            made.update(ky=vmem(2, self.t), lk=vmem(2, self.t))
        return {name + tag: value for name, value in made.items()}


NEAR = [(a, b, c) for c in (-1, 0, 1) for b in (-1, 0, 1) for a in (-1, 0, 1) if (a, b, c) != (0, 0, 0)]


def near(offset, counts):
    target, exists = {}, None
    for axis, step in zip(("gx", "gy", "gz"), offset):
        me, n = lax.axis_index(axis), counts[axis]
        if step:
            target[axis] = lax.rem(me + step + n, n)
            inside = me > 0 if step < 0 else me < n - 1
            exists = inside if exists is None else jnp.logical_and(exists, inside)
    return target, exists


def wait_units(units, count, sem):
    part = units.at[pl.ds(0, count)]
    pltpu.make_async_copy(part, part, sem).wait()


def wait_near(lv, counts, units, sems):
    choices = []
    for axis in ("gx", "gy", "gz"):
        me, n = lax.axis_index(axis), counts[axis]
        if n == 1:
            choices.append([(0, None)])
        elif n == 2:
            choices.append([(1, None)])
        else:
            edge = jnp.logical_or(me == 0, me == n - 1)
            choices.append([(1, edge), (2, jnp.logical_not(edge))])
    for chosen in itertools.product(*choices):
        total = 0
        for kind in itertools.product((0, 1), repeat=3):
            if any(kind):
                copies = 1
                for used, (number, _) in zip(kind, chosen):
                    copies *= number if used else 1
                total += copies * lv.units(*kind)
        conditions = [condition for _, condition in chosen if condition is not None]

        def wait():
            for sem in sems:
                wait_units(units, total, sem)

        if conditions:
            pl.when(functools.reduce(jnp.logical_and, conditions))(wait)
        else:
            wait()


def clear_sides(lv, b):
    b["lt"][0 : lv.wt] = jnp.zeros((lv.wt, lv.y, 128), lv.dtype)
    b["lt"][lv.t + lv.wt : lv.te] = jnp.zeros((lv.wt, lv.y, 128), lv.dtype)
    for name in ("ly", "lz", "lzb") + (("lk",) if lv.deep else ()):
        b[name][...] = jnp.zeros(b[name].shape, lv.dtype)


def pack_sides(lv, b):
    h, st, lane = lv.h, b["st"], iota((lv.y, 128), 1)
    first = last = jnp.zeros((lv.y, 128), F32)
    for t in range(lv.t):
        tile = st[t].astype(F32)
        if lv.blocks > 1:
            b["py"][0, t] = tile[0 : lv.wy].astype(lv.dtype)
            b["py"][1, t] = tile[lv.y - lv.wy : lv.y].astype(lv.dtype)
        for half in range(2):
            at = 2 * h * t + h * half
            turned = pltpu.roll(tile, (at - 64 * half) % 128, 1)
            first = jnp.where(((lane - at) & 127) < h, turned, first)
            last = jnp.where(((lane - at - 64 + h) & 127) < h, turned, last)
        if lv.deep:
            b["ky"][0, t : t + 1, :] = tile[lv.wy : lv.wy + 1, :]
            b["ky"][1, t : t + 1, :] = tile[lv.y - lv.wy - 1 : lv.y - lv.wy, :]
    for block in range(lv.blocks):
        rows = slice(block * lv.wy, block * lv.wy + lv.wy)
        b["pf"][block], b["pl"][block] = first[rows].astype(lv.dtype), last[rows].astype(lv.dtype)


def send_sides(lv, b, sems, counts, axes):
    taken = {-1: (0, lv.wt), 0: (0, lv.t), 1: (lv.t - lv.wt, lv.wt)}
    landed = {-1: lv.t + lv.wt, 0: lv.wt, 1: 0}
    pair = counts["gy"] == 2
    me = lax.axis_index("gy")

    def start(x, y, z):
        target = near((x, y, z), counts)[0]
        first, count = taken[x]
        source, goal = pl.ds(first, count), pl.ds(landed[x], count)
        side = 1 - me if pair else (y + 1) // 2
        if z:
            ends = b["pf"] if z < 0 else b["pl"]
            if y:
                pairs = [(ends.at[side * (lv.blocks - 1)], b["lzb"].at[(1 - z) // 2, 1 - x, 1 - side])]
            else:
                pairs = [(ends, b["lz"].at[(1 - z) // 2, 1 - x])]
        elif y:
            pairs = [(b["py"].at[side, source] if lv.blocks > 1 else b["st"].at[source], b["ly"].at[side, goal])]
            if lv.deep and not x:
                pairs.append((b["ky"].at[side], b["lk"].at[side]))
        else:
            pairs = [(b["st"].at[source], b["lt"].at[goal])]
        for src, dst in pairs:
            pltpu.make_async_remote_copy(
                src, dst, sems[0], sems[1], device_id=target, device_id_type=MESH).start()

    steps = (1, 0) if pair else (1, -1, 0)
    for x, z in sorted(itertools.product((-1, 0, 1), repeat=2), key=lambda n: -abs(n[0]) - abs(n[1])):
        chosen = [y for y in steps if abs(x) + abs(y) + abs(z) in axes]

        def send():
            for y in chosen:
                if pair or not y:
                    start(x, y, z)
                else:
                    pl.when(near((0, y, 0), counts)[1])(functools.partial(start, x, y, z))

        exists = near((x, 0, z), counts)[1]
        if chosen:
            send() if exists is None else pl.when(exists)(send)


def take_sides(lv, b, sems, counts, units, emit):
    h, wt = lv.h, lv.wt
    wait_near(lv, counts, units, sems)
    lane = iota((lv.ye, 128), 1)
    own, edge = lane < 64, (lane < 64 + h) | (lane >= 128 - h)
    for a in range(3):
        low, high = [
            jnp.concatenate(
                [b["lz"][c, a, block].astype(F32) for block in range(lv.blocks)]
                + [b["lzb"][c, a, side].astype(F32) for side in (1, 0)], axis=0)
            for c in range(2)]
        mixed = [jnp.where(((lane - 16 * h * q + h) & 127) < 64, high, low) for q in range(-(-lv.t // 8))]
        place = (0, wt, lv.t + wt)[a]
        start, count = ((lv.t - wt, wt), (0, lv.t), (0, wt))[a]
        for k in range(count):
            n, t = start + k, place + k
            rows = b["st"][n] if a == 1 else b["lt"][t]
            full = jnp.concatenate([part.astype(F32) for part in (rows, b["ly"][0, t], b["ly"][1, t])], axis=0)
            slices = []
            for half in range(2):
                ends = pltpu.roll(mixed[n // 8], (64 - 2 * h * n - h * half) % 128, 1)
                values = pltpu.roll(full, 64, 1) if half else full
                slices.append(jnp.where(own, values, jnp.where(edge, ends, 0.0)))
            emit(t, *slices)


def gather_start(buf, sems, counts):
    me = {axis: lax.axis_index(axis) for axis in counts}
    mine = buf.at[me["gx"], me["gy"], me["gz"]]
    ranges = [[n - k if k else 0 for k in range(n)] for n in counts.values()]
    for offset in sorted(itertools.product(*ranges), key=lambda o: -sum(1 for k in o if k)):
        if any(offset):
            target = {
                axis: lax.rem(me[axis] + jnp.where(me[axis] < counts[axis] // 2, k, counts[axis] - k), counts[axis])
                for axis, k in zip(counts, offset) if k}
            pltpu.make_async_remote_copy(
                mine, mine, sems[0], sems[1], device_id=target, device_id_type=MESH).start()


def gather_wait(sems, counts, units):
    others = counts["gx"] * counts["gy"] * counts["gz"] - 1
    if others:
        wait_units(units, others, sems[0])
        wait_units(units, others, sems[1])


def batches(low, high, size, body):
    whole = (high - low) // size
    if whole == 1:
        body(low, size)
    elif whole:
        def run(step, carry):
            body(low + step * size, size)
            return carry

        lax.fori_loop(0, whole, run, 0)
    if low + whole * size < high:
        body(low + whole * size, high - low - whole * size)


def even_rows(x, rows):
    return ((iota((rows, 128), 0) + x) & 1) == 0


def prepare_fine(lv, k, rows, fx, fy, zs, zo, dd, iv):
    row = iota((lv.ye, 128), 0)

    def body(first, count, inside=False):
        made = []
        for x in [first + i for i in range(count)]:
            first_red = even_rows(x, lv.ye)
            mids = [k[c][x + 1] for c in range(2)]
            for c in range(2):
                kx, other = mids[c], mids[1 - c]
                below = 0.5 * (k[1 - c][x] + kx)
                above = 0.5 * (kx + k[1 - c][x + 2])
                lower, upper = up(other, 0), down(other, 0)
                if inside:
                    ends = [jnp.broadcast_to(rows[side, pl.ds(x - lv.wt, 1), :], (lv.ye, 128)) for side in range(2)]
                    if c == 0:
                        ends = [pltpu.roll(end, 64, 1) for end in ends]
                    upper = jnp.where(row == lv.y + lv.wy - 1, ends[0], upper)
                    lower = jnp.where(row == lv.y + lv.wy, ends[1], lower)
                second = 0.5 * (lower + kx)
                same = 0.5 * (kx + other)
                moved = [up(other, 1), down(other, 1)]
                third = 0.5 * (kx + jnp.where(first_red, moved[c], moved[1 - c]))
                total = below + above + second + 0.5 * (kx + upper) + same + third
                made.append((x, c, below, second, third, total, jnp.where(kx > 0.0, 1.0 / total, 0.0), same))
        for x, c, *values, same in made:
            for ref, value in zip((fx, fy, zo, dd, iv), values):
                ref[c][x] = value
            if c == 0:
                zs[x] = same

    batches(0, lv.wt, 4, body)
    batches(lv.wt, lv.wt + lv.t, 8, functools.partial(body, inside=True))
    batches(lv.wt + lv.t, lv.te, 4, body)


def around_fine(lv, v, c, x, faces):
    fx, fy, zs, zo = faces
    o = 1 - c
    mid, first_red = v[o][x], even_rows(x, lv.ye)
    moved = [up(mid, 1), down(mid, 1)]
    summed = fx[c][x] * v[o][x - 1] + fx[o][x + 1] * v[o][x + 1]
    summed = summed + fy[c][x] * up(mid, 0) + down(fy[o][x] * mid, 0)
    return summed + zs[x] * mid + zo[c][x] * jnp.where(first_red, moved[c], moved[o])


def half_sweep_fine(lv, v, g, faces, iv, c, reach):
    low, high = lv.wt - reach, lv.wt + lv.t + reach

    def body(first, count):
        fresh = [(x, (g[c][x] + around_fine(lv, v, c, x, faces)) * iv[c][x]) for x in [first + i for i in range(count)]]
        for x, value in fresh:
            v[c][x] = value

    batches(low, high, high - low, body)


def residual_fine(lv, v, g, faces, dd, pairs):
    def body(first, count):
        made = []
        for i in [first + j for j in range(count)]:
            total = jnp.zeros((lv.ye, 128), F32)
            for x in (lv.wt + 2 * i, lv.wt + 2 * i + 1):
                for c in range(2):
                    total = total + (g[c][x] - dd[c][x] * v[c][x] + around_fine(lv, v, c, x, faces))
            made.append((i, total))
        for i, total in made:
            pairs[i] = total[0 : lv.y, :]

    batches(0, lv.t // 2, lv.t // 2, body)


def even_cells(shape):
    return ((iota(shape, 0) + iota(shape, 1)) & 1) == 0


def merge_planes(first, second):
    even = even_cells(first.shape)
    return jnp.where(even, first, second), jnp.where(even, second, first)


def beside(v, c, t):
    low, high = v[1 - c][max(t - 1, 0)], v[1 - c][min(t + 1, v[1 - c].shape[0] - 1)]
    even = even_cells(low.shape)
    return jnp.where(even, low, high) if c == 0 else jnp.where(even, high, low)


def prepare_mid(k, xs, xo, fy, fz, dd, iv):
    for t in range(xs.shape[0]):
        same = 0.5 * (k[0][t] + k[1][t])
        xs[t] = same
        second, third = [], []
        for c in range(2):
            second.append(0.5 * (up(k[1 - c][t], 0) + k[c][t]))
            third.append(0.5 * (up(k[1 - c][t], 1) + k[c][t]))
        for c in range(2):
            o, kx = 1 - c, k[c][t]
            other = 0.5 * (beside(k, c, t) + kx)
            total = same + other + second[c] + down(second[o], 0) + third[c] + down(third[o], 1)
            xo[c][t], fy[c][t], fz[c][t], dd[c][t] = other, second[c], third[c], total
            iv[c][t] = jnp.where(kx > 0.0, 1.0 / total, 0.0)


def around_mid(v, c, t, faces):
    xs, xo, fy, fz = faces
    o = 1 - c
    mid = v[o][t]
    summed = xs[t] * mid + xo[c][t] * beside(v, c, t)
    summed = summed + fy[c][t] * up(mid, 0) + down(fy[o][t] * mid, 0)
    return summed + fz[c][t] * up(mid, 1) + down(fz[o][t] * mid, 1)


def half_sweep_mid(lv, v, g, faces, iv, c, reach):
    low, high = 2 * lv.wt - reach, 2 * (lv.wt + lv.t) + reach
    fresh = [
        (t, (g[c][t] + around_mid(v, c, t, faces)) * iv[c][t]) for t in range(low // 2, (high + 1) // 2)]
    for t, value in fresh:
        v[c][t] = value


def residual_mid(lv, v, g, faces, dd, pairs):
    for i in range(lv.t):
        t = lv.wt + i
        total = 0.0
        for c in range(2):
            total = total + (g[c][t] - dd[c][t] * v[c][t] + around_mid(v, c, t, faces))
        pairs[i] = 0.25 * total[0 : lv.y]


def pair_planes(planes, target):
    lane = iota(planes[0].shape, 1)
    for t in range(len(planes) // 2):
        target[t] = jnp.where(lane < 64, planes[2 * t], pltpu.roll(planes[2 * t + 1], 64, 1))


def fold_rows(pairs, rows):
    return pairs[:, pl.ds(0, rows, stride=2), :] + pairs[:, pl.ds(1, rows, stride=2), :]


def dot(a, b):
    return jnp.dot(a, b, precision=HIGH, preferred_element_type=F32)


def pick(values, matrix):
    parts, rest = [], values
    for _ in range(3):
        parts.append(rest.astype(BF16))
        rest = rest - parts[-1].astype(F32)
    return jnp.dot(
        jnp.concatenate(parts, axis=1), jnp.concatenate([matrix.astype(BF16)] * 3, axis=0), preferred_element_type=F32)


def split_lanes(transposed):
    cell, lane = iota((128, 128), int(transposed)), iota((128, 128), 1 - int(transposed))
    return jnp.where(lane == cell // 2 + 64 * (cell % 2), 1.0, 0.0).astype(F32)


def split_both(transposed):
    matrix = split_lanes(transposed)
    return jnp.concatenate([matrix, pltpu.roll(matrix, 64, 1 - int(transposed))], axis=1)


def coarse_low(pairs, tmp):
    count, rows, _ = pairs.shape
    half = rows // 2
    for x in range(count):
        tmp[half * x : half * x + half, :] = pairs[x, pl.ds(0, half, stride=2), :] + pairs[x, pl.ds(1, half, stride=2), :]
    source, goal = iota((128, 128), 0), iota((128, 128), 1)
    means = 0.125 * pick(tmp[...], jnp.where((source // 2 == goal) & (source < 64), 1.0, 0.0))
    total = means[0:half]
    for x in range(1, count):
        total = total + pltpu.roll(means[half * x : half * x + half], 32 * x, 1)
    return total


def repeat(count, body, carry):
    if count <= 16:
        for p in range(count):
            carry = body(p, carry)
        return carry
    return lax.fori_loop(0, count, body, carry)


def spread_low(buf, whole, counts, pad):
    lane = iota((8, 128), 1)

    def body(a, carry):
        for ct in range(counts["gy"] // 2):
            for gt in range(counts["gz"] // 4):
                pieces = [
                    jnp.concatenate([buf[a, 2 * ct, 4 * gt + g], buf[a, 2 * ct + 1, 4 * gt + g]], axis=0)
                    for g in range(4)]
                for i in range(4):
                    total = pieces[0] if i == 0 else pltpu.roll(pieces[0], (-32 * i) % 128, 1)
                    for g in range(1, 4):
                        piece = pieces[g] if g == i else pltpu.roll(pieces[g], (32 * (g - i)) % 128, 1)
                        total = jnp.where(lane // 32 == g, piece, total)
                    whole[pad + 4 * a + i, 8 * ct : 8 * ct + 8, 128 * gt : 128 * gt + 128] = total
        return carry

    repeat(counts["gx"], body, 0)


def low_faces(k, faces, dims, pad):
    planes, rows, lanes = dims
    cx, cy0, cy1, cz0, cz1, cd = faces
    row, lane = iota((rows, lanes), 0), iota((rows, lanes), 1)
    scale = 0.5 * 0.0625

    def body(p, carry):
        kx = k[p + pad]
        below, above = scale * (k[p + pad - 1] + kx), scale * (kx + k[p + pad + 1])
        total = below + above
        cx[p] = below
        cx[p + 1] = above
        for target, inside, moved in (
            (cy0, row > 0, up(kx, 0)), (cy1, row < rows - 1, down(kx, 0)),
            (cz0, lane > 0, up(kx, 1)), (cz1, lane < lanes - 1, down(kx, 1))):
            face = scale * (kx + moved)
            target[p] = jnp.where(inside, face, 0.0)
            total = total + jnp.where(inside, face, scale * kx)
        cd[p] = total
        return carry

    repeat(planes, body, 0)


def bottom(f, s, vv, ww, faces, dims, pad):
    planes, rows, lanes = dims
    cx, cy0, cy1, cz0, cz1, cd = faces

    def operate(v, p):
        mid = v[p + pad]
        summed = cx[p] * v[p + pad - 1] + cx[p + 1] * v[p + pad + 1]
        summed = summed + (cy0[p] * up(mid, 0) + cy1[p] * down(mid, 0))
        summed = summed + (cz0[p] * up(mid, 1) + cz1[p] * down(mid, 1))
        return mid, cd[p] * mid - summed

    zero = jnp.zeros((rows, lanes), F32)

    def first(p, carry):
        mid, image = operate(f, p)
        vv[p + pad] = image
        return carry[0] + mid * mid, carry[1] + mid * image

    def total(v):
        return jnp.sum(jnp.sum(v, axis=0, keepdims=True), axis=1, keepdims=True)

    norm, along = repeat(planes, first, (zero, zero))
    alpha = total(norm) / total(along)

    def second(p, carry):
        ww[p] = operate(vv, p)[1]
        return carry

    repeat(planes, second, 0)

    def last(p, carry):
        rest = f[p + pad] - alpha * vv[p + pad]
        image = vv[p + pad] - alpha * ww[p]
        s[p + pad] = rest
        return carry[0] + image * rest, carry[1] + image * image

    turned, norm = repeat(planes, last, (zero, zero))
    return alpha, total(turned) / total(norm)


def choose_slots(ids, boxes, groups):
    held = ids[0].astype(F32)
    cap = held.shape[1]
    eye = iota((cap, cap), 0) == iota((cap, cap), 1)
    rows = jnp.broadcast_to(held, (cap, cap))
    cols = jnp.broadcast_to(jnp.sum(jnp.where(eye, rows, 0.0), axis=1, keepdims=True), (cap, cap))

    def target(v):
        return jnp.floor((v + 0.5) * (1.0 / boxes))

    earlier = (target(rows) == target(cols)) & (cols < rows) & (cols >= 0.0)
    ranking = jnp.sum(jnp.where(earlier, 1.0, 0.0), axis=0, keepdims=True)
    send_row = jnp.where(held >= 0.0, target(held) * SEND + ranking, -1.0)
    count = groups * SEND
    picker = jnp.where(iota((count, cap), 0).astype(F32) == jnp.broadcast_to(send_row, (count, cap)), 1.0, 0.0)
    return picker


def pack_boxes(slots, picker, outgoing):
    count, cap = picker.shape
    data = slots[0, 0].astype(F32)
    total = jnp.zeros((count, data.shape[1]), F32)
    for q in range(cap):
        total = total + picker[:, q : q + 1] * data[q : q + 1, :]
    for t in range(outgoing.shape[0]):
        outgoing[t] = total[SEND * t : SEND * t + SEND, :].astype(BF16)


def choose_boxes(owner, boxes):
    me = lax.axis_index("gz")
    owners = jnp.broadcast_to(owner[0].astype(F32), (boxes, owner.shape[2]))
    here = iota(owners.shape, 1) == iota(owners.shape, 0) + me * boxes
    col = jnp.sum(jnp.where(here, owners, 0.0), axis=1, keepdims=True)
    cols = jnp.broadcast_to(col, (boxes, boxes))
    first, second = iota((boxes, boxes), 0), iota((boxes, boxes), 1)
    row = jnp.sum(jnp.where(first == second, cols, 0.0), axis=0, keepdims=True)
    before = (jnp.broadcast_to(row, (boxes, boxes)) == cols) & (second < first)
    pick = col * SEND + jnp.sum(jnp.where(before, 1.0, 0.0), axis=1, keepdims=True)
    return pick


def place_boxes(incoming, held, pick, rows, boxes, groups):
    for t in range(groups):
        held[SEND * t : SEND * t + SEND, :] = incoming[t].astype(F32)
    per = 128 // BOX
    lane_box, row = iota((boxes, 128), 1) // BOX, iota((boxes, 128), 0)
    for part in range(BOX * BOX // per):
        lanes = slice(128 * part, 128 * part + 128)
        chosen = jnp.zeros((boxes, 128), F32)
        for r in range(groups * SEND):
            chosen = jnp.where(pick == float(r), held[r : r + 1, lanes], chosen)
        total = chosen
        for d in range(1, boxes):
            moved = pltpu.roll(pltpu.roll(chosen, BOX * d, 1), boxes - d, 0)
            total = jnp.where(((lane_box - row) & (boxes - 1)) == d, moved, total)
        rows[per * part : per * part + per, :] = total
    return jnp.dot(rows[...].astype(BF16), split_both(False).astype(BF16), preferred_element_type=F32)


def kernel(levels, counts, names, slots_in, ids_in, owner_in, coef_in, out, *scratch):
    r = dict(zip(names, scratch))
    groups = counts["gz"]
    at = {axis: lax.axis_index(axis) for axis in counts}
    slots, ids, owner, coef, units = r["slots"], r["ids"], r["owner"], r["coef"], r["units"]
    turns = (("move", "g", "low_f"), ("k", "q"), ("f", "low_k"), ("c", "e"))
    sends = {tag: n for n, tags in enumerate(turns) for tag in tags}
    sems = {tag: (r["sems"].at[n], r["sems"].at[len(turns) + k]) for k, (tag, n) in enumerate(sends.items())}
    loads = [
        pltpu.make_async_copy(source, target, r["sems"].at[n])
        for n, (source, target) in enumerate(((ids_in, ids), (slots_in, slots), (coef_in, coef), (owner_in, owner)))]
    for load in loads:
        load.start()
    fine, mid = levels["f"], levels["g"]
    sides = {tag: {name[: -len(tag)]: r[name] for name in lv.scratch(tag)} for tag, lv in levels.items()}
    for tag, lv in levels.items():
        clear_sides(lv, sides[tag])

    barrier = pltpu.get_barrier_semaphore()
    def signal_near(sem, offsets):
        count = 0
        for offset in offsets:
            target, exists = near(offset, counts)

            @pl.when(exists)
            def _():
                pl.semaphore_signal(sem, inc=1, device_id=target, device_id_type=MESH)

            count = count + jnp.where(exists, 1, 0)
        return count

    expected = signal_near(barrier, sorted([n for n in NEAR if 0 in n], key=lambda n: -sum(map(abs, n))))
    others = [{"gz": lax.rem(at["gz"] + k, groups)} for k in range(1, groups)]
    if counts["gx"] > 4 or counts["gy"] > 4:
        for offset in itertools.product(*[range(n) for n in counts.values()]):
            if any(offset):
                others.append({axis: lax.rem(at[axis] + k, counts[axis]) for axis, k in zip(counts, offset) if k})
    for target in others:
        pl.semaphore_signal(barrier, inc=1, device_id=target, device_id_type=MESH)

    def send(tag, axes=(1, 2, 3)):
        send_sides(levels[tag], sides[tag], sems[tag], counts, axes)

    def take(tag, emit):
        counted = units if levels[tag].dtype == F32 else r["half_units"]
        take_sides(levels[tag], sides[tag], sems[tag], counts, counted, emit)

    loads[0].wait()
    boxes = out.shape[2] // BOX
    picker = choose_slots(ids, boxes, groups)
    loads[1].wait()
    pack_boxes(slots, picker, r["outgoing"])
    pl.semaphore_wait(barrier, expected + len(others))

    me = at["gz"]
    for k in range(1, groups):
        to = lax.rem(me + k, groups)
        pltpu.make_async_remote_copy(
            r["outgoing"].at[to], r["incoming"].at[me], sems["move"][0], sems["move"][1],
            device_id={"gz": to}, device_id_type=MESH).start()
    greeted = signal_near(r["hello"], list(itertools.product((-1, 1), (0,), (-1, 0, 1))))
    loads[2].wait()
    loads[3].wait()
    choose = lambda both, t: jnp.where(even_rows(t, fine.y), both[t, :, 0:128], both[t, :, 128:256])
    split = pick(coef[...].reshape(fine.t * fine.y, 128), split_both(False)).reshape(fine.t, fine.y, 256)
    for t in range(fine.t):
        sides["k"]["st"][t] = choose(split, t)
    pack_sides(levels["k"], sides["k"])
    send("k", (1, 2))
    r["incoming"][me] = r["outgoing"][me]

    half_t, half_y = fine.t // 2, fine.y // 2
    for i in range(half_t):
        pair = sides["k"]["st"][2 * i] + sides["k"]["st"][2 * i + 1]
        r["pairs"][i] = pair + pltpu.roll(pair, 64, 1)
    coarse = 0.125 * fold_rows(r["pairs"], half_y)
    merged = [merge_planes(coarse[i], coarse[i + 1]) for i in range(0, half_t, 2)]
    pair_planes([plane for pair in merged for plane in pair], sides["c"]["st"])
    pack_sides(mid, sides["c"])
    pl.semaphore_wait(r["hello"], greeted)
    send("k", (3,))
    send("c")
    for i in range(half_t // 2):
        r["pairsm"][i] = coarse[2 * i] + coarse[2 * i + 1]
    here = (at["gx"], at["gy"], at["gz"])
    r["gk"][here] = coarse_low(r["pairsm"], r["tmp"])
    r["pick"][...] = jnp.broadcast_to(choose_boxes(owner, boxes), r["pick"].shape)
    if groups > 1:
        part = r["incoming"].at[pl.ds(0, groups - 1)]
        for n in range(2):
            pltpu.make_async_copy(part, part, sems["move"][n]).wait()
    source = place_boxes(r["incoming"], r["held"], r["pick"][...], r["rows"], boxes, groups)
    source = source.reshape(fine.t, fine.y, 256)
    for t in range(fine.t):
        sides["f"]["st"][t] = choose(source, t).astype(BF16)
    pack_sides(fine, sides["f"])
    send("f")

    pair_of = lambda name: (r[name + "r"], r[name + "b"])
    v0, g0, k0 = pair_of("v0"), pair_of("g0"), pair_of("k0")
    fx, fy, zo, dd0, iv0 = (pair_of(name) for name in ("fx0", "fy0", "zo0", "dd0", "iv0"))
    faces0 = (fx, fy, r["zs0"], zo)
    fx1, fy1, fz1, dd1, iv1, v1, g1, k1 = (pair_of(n) for n in ("fx1", "fy1", "fz1", "dd1", "iv1", "v1", "g1", "k1"))
    faces1 = (r["xs1"], fx1, fy1, fz1)

    def store_pair(refs):
        def emit(t, first, second):
            refs[0][t] = first
            refs[1][t] = second
        return emit

    def store_planes(ref):
        def emit(t, first, second):
            ref[2 * t] = first
            ref[2 * t + 1] = second
        return emit

    take("k", store_pair(k0))
    prepare_fine(fine, k0, sides["k"]["lk"], fx, fy, r["zs0"], zo, dd0, iv0)

    def open_fine(t, red, black):
        g0[0][t] = red
        g0[1][t] = black
        v0[0][t] = red * iv0[0][t]

    take("f", open_fine)
    for reach, colour in ((3, 1), (2, 0), (1, 1)):
        half_sweep_fine(fine, v0, g0, faces0, iv0, colour, reach)
    residual_fine(fine, v0, g0, faces0, dd0, r["pairs"])

    coarse = 0.5 * fold_rows(r["pairs"], half_y)
    merged = [merge_planes(coarse[i], coarse[i + 1]) for i in range(0, half_t, 2)]
    pair_planes([plane for pair in merged for plane in pair], sides["g"]["st"])
    pack_sides(mid, sides["g"])
    send("g")
    take("c", store_pair(k1))
    prepare_mid(k1, *faces1, dd1, iv1)
    for name in ("k2", "f2", "s2", "v2"):
        r[name][...] = jnp.zeros(r[name].shape, F32)
    pair_planes([v0[1][fine.wt + x, 0 : fine.y, :] for x in range(fine.t)], sides["q"]["st"])
    pack_sides(levels["q"], sides["q"])
    send("q")
    gather_start(r["gk"], sems["low_k"], counts)
    wm = 2 * mid.wt

    def open_mid(t, red, black):
        g1[0][t] = red
        g1[1][t] = black
        v1[0][t] = red * iv1[0][t]

    take("g", open_mid)
    for reach, colour in ((3, 1), (2, 0), (1, 1)):
        half_sweep_mid(mid, v1, g1, faces1, iv1, colour, reach)
    residual_mid(mid, v1, g1, faces1, dd1, r["pairsm"])
    r["gf"][here] = coarse_low(r["pairsm"], r["tmp"])
    gather_start(r["gf"], sems["low_f"], counts)
    pair_planes([v1[1][mid.wt + t, 0 : mid.y, :] for t in range(mid.t)], sides["e"]["st"])
    pack_sides(levels["e"], sides["e"])
    send("e")

    planes, rows, lanes = dims = (4 * counts["gx"], 4 * counts["gy"], 32 * counts["gz"])
    pad = wm // 2
    low = tuple(r[name] for name in ("cx", "cy0", "cy1", "cz0", "cz1", "cd"))
    take("q", store_planes(r["q0"]))
    gather_wait(sems["low_k"], counts, units)
    spread_low(r["gk"], r["k2"], counts, pad)
    low_faces(r["k2"], low, dims, pad)

    def store_black(t, *planes):
        for k, plane in enumerate(planes):
            n = 2 * t + k - (2 * levels["e"].wt - mid.wt)
            if 0 <= n < mid.te:
                v1[1][n] = plane

    take("e", store_black)
    gather_wait(sems["low_f"], counts, units)
    spread_low(r["gf"], r["f2"], counts, pad)
    alpha, omega = bottom(r["f2"], r["s2"], r["v2"], r["w2"], low, dims, pad)
    around_low = mid.te
    for q in range(around_low):
        turned = alpha * r["f2"][4 * at["gx"] + q] + omega * r["s2"][4 * at["gx"] + q]
        plane = turned
        for c in range(1, counts["gy"]):
            turned = jnp.where(at["gy"] == c, pltpu.roll(plane, rows - 4 * c, 0), turned)
        r["local"][q, 0:8, :] = turned[0:8, :]
        r["local"][q, 8:16, :] = pltpu.roll(turned[rows - 8 : rows, :], 4, 0)
    goal = iota((lanes, 128), 1)
    cell = jnp.where(goal < 64 + wm, goal, goal - 128)
    cell = (cell + 128) // 2 - 64
    wanted = (goal < 64 + wm) | (goal >= 128 - wm)
    matrix = jnp.where((iota((lanes, 128), 0) == 32 * at["gz"] + cell) & wanted, 1.0, 0.0).astype(F32)
    spread = pick(r["local"][...].reshape(16 * around_low, lanes), matrix).reshape(around_low, 16, 128)
    for q in range(around_low):
        wide = r["wide"].at[q]
        for k in range(2):
            wide[pl.ds(k, 12, stride=2), :] = spread[q, 0:12]
        v1[1][q] = jnp.where(k1[1][q] > 0.0, v1[1][q] + wide[...], 0.0)
    for reach, colour in ((5, 0), (4, 1), (3, 0), (2, 1)):
        half_sweep_mid(mid, v1, g1, faces1, iv1, colour, reach)

    low_w = fine.wt // 2
    row = iota((8, 128), 0)
    for i in range(half_t + 2 * low_w):
        x = wm - low_w + i
        wide = r["wide"].at[i]
        plane = merge_planes(v1[0][x // 2], v1[1][x // 2])[x % 2]
        ends = jnp.where(row < low_w, plane[8:16], pltpu.roll(plane[mid.ye - 8 : mid.ye], 4, 0))
        turned = jnp.concatenate([plane[0:8], ends[0:4]], axis=0)
        for k in range(2):
            wide[pl.ds(k, 12, stride=2), :] = turned
        for k in range(2):
            v0[1][2 * i + k] = r["q0"][2 * i + k] + wide[...]
    for reach, colour in ((3, 0), (2, 1), (1, 0), (0, 1)):
        half_sweep_fine(fine, v0, g0, faces0, iv0, colour, reach)
    lane = iota((fine.y, 128), 1)
    for t in range(fine.t):
        red, black = (v0[c][fine.wt + t, 0 : fine.y, :] for c in range(2))
        r["joined"][t] = jnp.where(lane < 64, red, pltpu.roll(black, 64, 1))
    joined = pick(r["joined"][...].reshape(fine.t * fine.y, 128), split_both(True)).reshape(fine.t, fine.y, 256)
    for t in range(fine.t):
        out[t] = choose(joined, t)


def per_device(counts, old_slots, old_ids, old_owner, coefficient):
    x, y, z = coefficient.shape
    planes, rows, lanes = 4 * counts["gx"], 4 * counts["gy"], 32 * counts["gz"]
    groups, boxes = counts["gz"], z // BOX
    cells = old_slots.shape[3]
    mid = Level(x // 4, y // 2, 3, 8, 6)
    levels = {
        "k": Level(x, y, 5, 4, 3, deep=True), "f": Level(x, y, 4, 4, 2, dtype=BF16), "q": Level(x // 2, y, 2, 4, 2),
        "c": mid, "g": mid, "e": Level(x // 8, y // 2, 2, 8, 6)}
    fine, edge = levels["f"], levels["k"]
    pad = mid.wt
    devices = counts["gx"] * counts["gy"] * groups
    vmem = lambda *shape: pltpu.VMEM(shape, F32)
    dma = lambda *shape: pltpu.SemaphoreType.DMA(shape)
    scratch = {}
    for tag, level in levels.items():
        scratch.update(level.scratch(tag))
    for name in ("v0", "g0", "fx0", "fy0", "zo0", "dd0", "iv0", "k0"):
        for colour in "rb":
            scratch[name + colour] = vmem(edge.te if name == "k0" else fine.te, fine.ye, 128)
    for name in ("zs0", "q0"):
        scratch[name] = vmem(fine.te, fine.ye, 128)
    for name in ("fx1", "fy1", "fz1", "dd1", "iv1", "v1", "g1", "k1"):
        for colour in "rb":
            scratch[name + colour] = vmem(mid.te, mid.ye, 128)
    scratch["xs1"] = vmem(mid.te, mid.ye, 128)
    scratch.update(
        slots=pltpu.VMEM(old_slots.shape, old_slots.dtype), ids=pltpu.VMEM(old_ids.shape, old_ids.dtype),
        owner=pltpu.VMEM(old_owner.shape, old_owner.dtype), coef=vmem(*coefficient.shape),
        outgoing=pltpu.VMEM((groups, SEND, cells), BF16), incoming=pltpu.VMEM((groups, SEND, cells), BF16),
        held=vmem(groups * SEND, cells), sems=dma(13), hello=pltpu.SemaphoreType.REGULAR, units=vmem(max(160, devices), 4, 128),
        half_units=pltpu.VMEM((160, 4, 128), BF16),
        rows=vmem(BOX * BOX, 128), pick=vmem(boxes, 128), pairs=vmem(x // 2, y, 128), pairsm=vmem(x // 4, y // 2, 128),
        joined=vmem(x, y, 128), tmp=vmem(x * y // 16, 128), local=vmem(mid.te, 16, lanes),
        wide=vmem(max(mid.te, fine.te // 2), 24, 128),
        gk=vmem(counts["gx"], counts["gy"], groups, 4, 128), gf=vmem(counts["gx"], counts["gy"], groups, 4, 128),
        cx=vmem(planes + 1, rows, lanes), w2=vmem(planes, rows, lanes))
    for name in ("cy0", "cy1", "cz0", "cz1", "cd"):
        scratch[name] = vmem(planes, rows, lanes)
    for name in ("f2", "k2", "s2", "v2"):
        scratch[name] = vmem(planes + 2 * pad, rows, lanes)
    return pl.pallas_call(
        functools.partial(kernel, levels, counts, tuple(scratch)),
        out_shape=jax.ShapeDtypeStruct(coefficient.shape, F32),
        in_specs=[pl.BlockSpec(memory_space=pltpu.MemorySpace.HBM)] * 4,
        out_specs=pl.BlockSpec(memory_space=pltpu.VMEM),
        scratch_shapes=list(scratch.values()),
        compiler_params=pltpu.CompilerParams(
            collective_id=0, has_side_effects=True, vmem_limit_bytes=44 * 1024 * 1024),
    )(*[pltpu.with_memory_space_constraint(v, pltpu.HBM) for v in (old_slots, old_ids, old_owner, coefficient)])


def solution(mesh):
    counts = {axis: mesh.shape[axis] for axis in ("gx", "gy", "gz")}
    return jax.shard_map(
        functools.partial(per_device, counts), mesh=mesh,
        in_specs=(P("gx", "gy", "gz", None), P("gx", "gy", "gz"), P("gx", "gy", None), P("gx", "gy", "gz")),
        out_specs=P("gx", "gy", "gz"), check_vma=False)
```

```python
import functools
import itertools

import jax
import jax.numpy as jnp
from jax import lax
from jax.experimental import pallas as pl
from jax.experimental.pallas import tpu as pltpu
from jax.sharding import PartitionSpec as P

BOX = 16
SEND = 2
F32 = jnp.float32
BF16 = jnp.bfloat16
MESH = pl.DeviceIdType.MESH
HIGH = lax.Precision.HIGHEST


def iota(shape, dim):
    return lax.broadcasted_iota(jnp.int32, shape, dim)


def up(v, axis):
    return pltpu.roll(v, 1, axis)


def down(v, axis):
    return pltpu.roll(v, v.shape[axis] - 1, axis)


class Level:
    def __init__(self, t, y, wt, wy, h, deep=False, dtype=F32):
        self.dtype = dtype
        self.t, self.y, self.wt, self.wy, self.h, self.deep = t, y, wt, wy, h, deep
        self.te, self.ye = t + 2 * wt, y + 2 * wy
        self.blocks = y // wy

    def units(self, a, b, c):
        if c:
            return (self.wy if b else self.y) // 4
        extra = self.t // 4 if self.deep and b and not a else 0
        return (self.wt if a else self.t) * (self.wy if b else self.y) // 4 + extra

    def scratch(self, tag):
        vmem = lambda *shape: pltpu.VMEM(shape + (128,), self.dtype)
        made = {
            "st": vmem(self.t, self.y), "py": vmem(2, self.t, self.wy), "lt": vmem(self.te, self.y),
            "ly": vmem(2, self.te, self.wy), "pf": vmem(self.blocks, self.wy), "pl": vmem(self.blocks, self.wy),
            "lz": vmem(2, 3, self.blocks, self.wy), "lzb": vmem(2, 3, 2, self.wy)}
        if self.deep:
            made.update(ky=vmem(2, self.t), lk=vmem(2, self.t))
        return {name + tag: value for name, value in made.items()}


NEAR = [(a, b, c) for c in (-1, 0, 1) for b in (-1, 0, 1) for a in (-1, 0, 1) if (a, b, c) != (0, 0, 0)]


def near(offset, counts):
    target, exists = {}, None
    for axis, step in zip(("gx", "gy", "gz"), offset):
        me, n = lax.axis_index(axis), counts[axis]
        if step:
            target[axis] = lax.rem(me + step + n, n)
            inside = me > 0 if step < 0 else me < n - 1
            exists = inside if exists is None else jnp.logical_and(exists, inside)
    return target, exists


def wait_units(units, count, sem):
    part = units.at[pl.ds(0, count)]
    pltpu.make_async_copy(part, part, sem).wait()


def wait_near(lv, counts, units, sems):
    choices = []
    for axis in ("gx", "gy", "gz"):
        me, n = lax.axis_index(axis), counts[axis]
        if n == 1:
            choices.append([(0, None)])
        elif n == 2:
            choices.append([(1, None)])
        else:
            edge = jnp.logical_or(me == 0, me == n - 1)
            choices.append([(1, edge), (2, jnp.logical_not(edge))])
    for chosen in itertools.product(*choices):
        total = 0
        for kind in itertools.product((0, 1), repeat=3):
            if any(kind):
                copies = 1
                for used, (number, _) in zip(kind, chosen):
                    copies *= number if used else 1
                total += copies * lv.units(*kind)
        conditions = [condition for _, condition in chosen if condition is not None]

        def wait():
            for sem in sems:
                wait_units(units, total, sem)

        if conditions:
            pl.when(functools.reduce(jnp.logical_and, conditions))(wait)
        else:
            wait()


def clear_sides(lv, b):
    b["lt"][0 : lv.wt] = jnp.zeros((lv.wt, lv.y, 128), lv.dtype)
    b["lt"][lv.t + lv.wt : lv.te] = jnp.zeros((lv.wt, lv.y, 128), lv.dtype)
    for name in ("ly", "lz", "lzb") + (("lk",) if lv.deep else ()):
        b[name][...] = jnp.zeros(b[name].shape, lv.dtype)


def pack_sides(lv, b):
    h, st, lane = lv.h, b["st"], iota((lv.y, 128), 1)
    first = last = jnp.zeros((lv.y, 128), F32)
    for t in range(lv.t):
        tile = st[t].astype(F32)
        if lv.blocks > 1:
            b["py"][0, t] = tile[0 : lv.wy].astype(lv.dtype)
            b["py"][1, t] = tile[lv.y - lv.wy : lv.y].astype(lv.dtype)
        for half in range(2):
            at = 2 * h * t + h * half
            turned = pltpu.roll(tile, (at - 64 * half) % 128, 1)
            first = jnp.where(((lane - at) & 127) < h, turned, first)
            last = jnp.where(((lane - at - 64 + h) & 127) < h, turned, last)
        if lv.deep:
            b["ky"][0, t : t + 1, :] = tile[lv.wy : lv.wy + 1, :]
            b["ky"][1, t : t + 1, :] = tile[lv.y - lv.wy - 1 : lv.y - lv.wy, :]
    for block in range(lv.blocks):
        rows = slice(block * lv.wy, block * lv.wy + lv.wy)
        b["pf"][block], b["pl"][block] = first[rows].astype(lv.dtype), last[rows].astype(lv.dtype)


def send_sides(lv, b, sems, counts, axes):
    taken = {-1: (0, lv.wt), 0: (0, lv.t), 1: (lv.t - lv.wt, lv.wt)}
    landed = {-1: lv.t + lv.wt, 0: lv.wt, 1: 0}
    pair = counts["gy"] == 2
    me = lax.axis_index("gy")

    def start(x, y, z):
        target = near((x, y, z), counts)[0]
        first, count = taken[x]
        source, goal = pl.ds(first, count), pl.ds(landed[x], count)
        side = 1 - me if pair else (y + 1) // 2
        if z:
            ends = b["pf"] if z < 0 else b["pl"]
            if y:
                pairs = [(ends.at[side * (lv.blocks - 1)], b["lzb"].at[(1 - z) // 2, 1 - x, 1 - side])]
            else:
                pairs = [(ends, b["lz"].at[(1 - z) // 2, 1 - x])]
        elif y:
            pairs = [(b["py"].at[side, source] if lv.blocks > 1 else b["st"].at[source], b["ly"].at[side, goal])]
            if lv.deep and not x:
                pairs.append((b["ky"].at[side], b["lk"].at[side]))
        else:
            pairs = [(b["st"].at[source], b["lt"].at[goal])]
        for src, dst in pairs:
            pltpu.make_async_remote_copy(
                src, dst, sems[0], sems[1], device_id=target, device_id_type=MESH).start()

    steps = (1, 0) if pair else (1, -1, 0)
    for x, z in sorted(itertools.product((-1, 0, 1), repeat=2), key=lambda n: -abs(n[0]) - abs(n[1])):
        chosen = [y for y in steps if abs(x) + abs(y) + abs(z) in axes]

        def send():
            for y in chosen:
                if pair or not y:
                    start(x, y, z)
                else:
                    pl.when(near((0, y, 0), counts)[1])(functools.partial(start, x, y, z))

        exists = near((x, 0, z), counts)[1]
        if chosen:
            send() if exists is None else pl.when(exists)(send)


def take_sides(lv, b, sems, counts, units, emit):
    h, wt = lv.h, lv.wt
    wait_near(lv, counts, units, sems)
    lane = iota((lv.ye, 128), 1)
    own, edge = lane < 64, (lane < 64 + h) | (lane >= 128 - h)
    for a in range(3):
        low, high = [
            jnp.concatenate(
                [b["lz"][c, a, block].astype(F32) for block in range(lv.blocks)]
                + [b["lzb"][c, a, side].astype(F32) for side in (1, 0)], axis=0)
            for c in range(2)]
        mixed = [jnp.where(((lane - 16 * h * q + h) & 127) < 64, high, low) for q in range(-(-lv.t // 8))]
        place = (0, wt, lv.t + wt)[a]
        start, count = ((lv.t - wt, wt), (0, lv.t), (0, wt))[a]
        for k in range(count):
            n, t = start + k, place + k
            rows = b["st"][n] if a == 1 else b["lt"][t]
            full = jnp.concatenate([part.astype(F32) for part in (rows, b["ly"][0, t], b["ly"][1, t])], axis=0)
            slices = []
            for half in range(2):
                ends = pltpu.roll(mixed[n // 8], (64 - 2 * h * n - h * half) % 128, 1)
                values = pltpu.roll(full, 64, 1) if half else full
                slices.append(jnp.where(own, values, jnp.where(edge, ends, 0.0)))
            emit(t, *slices)


def gather_start(buf, sems, counts):
    me = {axis: lax.axis_index(axis) for axis in counts}
    mine = buf.at[me["gx"], me["gy"], me["gz"]]
    ranges = [[n - k if k else 0 for k in range(n)] for n in counts.values()]
    for offset in sorted(itertools.product(*ranges), key=lambda o: -sum(1 for k in o if k)):
        if any(offset):
            target = {
                axis: lax.rem(me[axis] + jnp.where(me[axis] < counts[axis] // 2, k, counts[axis] - k), counts[axis])
                for axis, k in zip(counts, offset) if k}
            pltpu.make_async_remote_copy(
                mine, mine, sems[0], sems[1], device_id=target, device_id_type=MESH).start()


def gather_wait(sems, counts, units):
    others = counts["gx"] * counts["gy"] * counts["gz"] - 1
    if others:
        wait_units(units, others, sems[0])
        wait_units(units, others, sems[1])


def batches(low, high, size, body):
    whole = (high - low) // size
    if whole == 1:
        body(low, size)
    elif whole:
        def run(step, carry):
            body(low + step * size, size)
            return carry

        lax.fori_loop(0, whole, run, 0)
    if low + whole * size < high:
        body(low + whole * size, high - low - whole * size)


def even_rows(x, rows):
    return ((iota((rows, 128), 0) + x) & 1) == 0


def prepare_fine(lv, k, rows, fx, fy, zs, zo, dd, iv):
    row = iota((lv.ye, 128), 0)

    def body(first, count, inside=False):
        made = []
        for x in [first + i for i in range(count)]:
            first_red = even_rows(x, lv.ye)
            mids = [k[c][x + 1] for c in range(2)]
            for c in range(2):
                kx, other = mids[c], mids[1 - c]
                below = 0.5 * (k[1 - c][x] + kx)
                above = 0.5 * (kx + k[1 - c][x + 2])
                lower, upper = up(other, 0), down(other, 0)
                if inside:
                    ends = [jnp.broadcast_to(rows[side, pl.ds(x - lv.wt, 1), :], (lv.ye, 128)) for side in range(2)]
                    if c == 0:
                        ends = [pltpu.roll(end, 64, 1) for end in ends]
                    upper = jnp.where(row == lv.y + lv.wy - 1, ends[0], upper)
                    lower = jnp.where(row == lv.y + lv.wy, ends[1], lower)
                second = 0.5 * (lower + kx)
                same = 0.5 * (kx + other)
                moved = [up(other, 1), down(other, 1)]
                third = 0.5 * (kx + jnp.where(first_red, moved[c], moved[1 - c]))
                total = below + above + second + 0.5 * (kx + upper) + same + third
                made.append((x, c, below, second, third, total, jnp.where(kx > 0.0, 1.0 / total, 0.0), same))
        for x, c, *values, same in made:
            for ref, value in zip((fx, fy, zo, dd, iv), values):
                ref[c][x] = value
            if c == 0:
                zs[x] = same

    batches(0, lv.wt, 4, body)
    batches(lv.wt, lv.wt + lv.t, 8, functools.partial(body, inside=True))
    batches(lv.wt + lv.t, lv.te, 4, body)


def around_fine(lv, v, c, x, faces):
    fx, fy, zs, zo = faces
    o = 1 - c
    mid, first_red = v[o][x], even_rows(x, lv.ye)
    moved = [up(mid, 1), down(mid, 1)]
    summed = fx[c][x] * v[o][x - 1] + fx[o][x + 1] * v[o][x + 1]
    summed = summed + fy[c][x] * up(mid, 0) + down(fy[o][x] * mid, 0)
    return summed + zs[x] * mid + zo[c][x] * jnp.where(first_red, moved[c], moved[o])


def half_sweep_fine(lv, v, g, faces, iv, c, reach):
    low, high = lv.wt - reach, lv.wt + lv.t + reach

    def body(first, count):
        fresh = [(x, (g[c][x] + around_fine(lv, v, c, x, faces)) * iv[c][x]) for x in [first + i for i in range(count)]]
        for x, value in fresh:
            v[c][x] = value

    batches(low, high, high - low, body)


def residual_fine(lv, v, g, faces, dd, pairs):
    def body(first, count):
        made = []
        for i in [first + j for j in range(count)]:
            total = jnp.zeros((lv.ye, 128), F32)
            for x in (lv.wt + 2 * i, lv.wt + 2 * i + 1):
                for c in range(2):
                    total = total + (g[c][x] - dd[c][x] * v[c][x] + around_fine(lv, v, c, x, faces))
            made.append((i, total))
        for i, total in made:
            pairs[i] = total[0 : lv.y, :]

    batches(0, lv.t // 2, lv.t // 2, body)


def even_cells(shape):
    return ((iota(shape, 0) + iota(shape, 1)) & 1) == 0


def merge_planes(first, second):
    even = even_cells(first.shape)
    return jnp.where(even, first, second), jnp.where(even, second, first)


def beside(v, c, t):
    low, high = v[1 - c][max(t - 1, 0)], v[1 - c][min(t + 1, v[1 - c].shape[0] - 1)]
    even = even_cells(low.shape)
    return jnp.where(even, low, high) if c == 0 else jnp.where(even, high, low)


def prepare_mid(k, xs, xo, fy, fz, dd, iv):
    for t in range(xs.shape[0]):
        same = 0.5 * (k[0][t] + k[1][t])
        xs[t] = same
        second, third = [], []
        for c in range(2):
            second.append(0.5 * (up(k[1 - c][t], 0) + k[c][t]))
            third.append(0.5 * (up(k[1 - c][t], 1) + k[c][t]))
        for c in range(2):
            o, kx = 1 - c, k[c][t]
            other = 0.5 * (beside(k, c, t) + kx)
            total = same + other + second[c] + down(second[o], 0) + third[c] + down(third[o], 1)
            xo[c][t], fy[c][t], fz[c][t], dd[c][t] = other, second[c], third[c], total
            iv[c][t] = jnp.where(kx > 0.0, 1.0 / total, 0.0)


def around_mid(v, c, t, faces):
    xs, xo, fy, fz = faces
    o = 1 - c
    mid = v[o][t]
    summed = xs[t] * mid + xo[c][t] * beside(v, c, t)
    summed = summed + fy[c][t] * up(mid, 0) + down(fy[o][t] * mid, 0)
    return summed + fz[c][t] * up(mid, 1) + down(fz[o][t] * mid, 1)


def half_sweep_mid(lv, v, g, faces, iv, c, reach):
    low, high = 2 * lv.wt - reach, 2 * (lv.wt + lv.t) + reach
    fresh = [
        (t, (g[c][t] + around_mid(v, c, t, faces)) * iv[c][t]) for t in range(low // 2, (high + 1) // 2)]
    for t, value in fresh:
        v[c][t] = value


def residual_mid(lv, v, g, faces, dd, pairs):
    for i in range(lv.t):
        t = lv.wt + i
        total = 0.0
        for c in range(2):
            total = total + (g[c][t] - dd[c][t] * v[c][t] + around_mid(v, c, t, faces))
        pairs[i] = 0.25 * total[0 : lv.y]


def pair_planes(planes, target):
    lane = iota(planes[0].shape, 1)
    for t in range(len(planes) // 2):
        target[t] = jnp.where(lane < 64, planes[2 * t], pltpu.roll(planes[2 * t + 1], 64, 1))


def fold_rows(pairs, rows):
    return pairs[:, pl.ds(0, rows, stride=2), :] + pairs[:, pl.ds(1, rows, stride=2), :]


def dot(a, b):
    return jnp.dot(a, b, precision=HIGH, preferred_element_type=F32)


def pick(values, matrix):
    parts, rest = [], values
    for _ in range(3):
        parts.append(rest.astype(BF16))
        rest = rest - parts[-1].astype(F32)
    return jnp.dot(
        jnp.concatenate(parts, axis=1), jnp.concatenate([matrix.astype(BF16)] * 3, axis=0), preferred_element_type=F32)


def split_lanes(transposed):
    cell, lane = iota((128, 128), int(transposed)), iota((128, 128), 1 - int(transposed))
    return jnp.where(lane == cell // 2 + 64 * (cell % 2), 1.0, 0.0).astype(F32)


def split_both(transposed):
    matrix = split_lanes(transposed)
    return jnp.concatenate([matrix, pltpu.roll(matrix, 64, 1 - int(transposed))], axis=1)


def coarse_low(pairs, tmp):
    count, rows, _ = pairs.shape
    half = rows // 2
    for x in range(count):
        tmp[half * x : half * x + half, :] = pairs[x, pl.ds(0, half, stride=2), :] + pairs[x, pl.ds(1, half, stride=2), :]
    shape = (128, 128 * count)
    source, goal, x = iota(shape, 0), iota(shape, 1) % 128, iota(shape, 1) // 128
    means = pick(tmp[...], jnp.where((source // 2 + 32 * x == goal) & (source < 64), 1.0, 0.0))
    total = means[0:half, 0:128]
    for x in range(1, count):
        total = total + means[half * x : half * x + half, 128 * x : 128 * x + 128]
    return 0.125 * total


def repeat(count, body, carry):
    if count <= 16:
        for p in range(count):
            carry = body(p, carry)
        return carry
    return lax.fori_loop(0, count, body, carry)


def spread_low(buf, whole, counts, pad):
    lane = iota((8, 128), 1)

    def body(a, carry):
        for ct in range(counts["gy"] // 2):
            for gt in range(counts["gz"] // 4):
                pieces = [
                    jnp.concatenate([buf[a, 2 * ct, 4 * gt + g], buf[a, 2 * ct + 1, 4 * gt + g]], axis=0)
                    for g in range(4)]
                for i in range(4):
                    total = pieces[0] if i == 0 else pltpu.roll(pieces[0], (-32 * i) % 128, 1)
                    for g in range(1, 4):
                        piece = pieces[g] if g == i else pltpu.roll(pieces[g], (32 * (g - i)) % 128, 1)
                        total = jnp.where(lane // 32 == g, piece, total)
                    whole[pad + 4 * a + i, 8 * ct : 8 * ct + 8, 128 * gt : 128 * gt + 128] = total
        return carry

    repeat(counts["gx"], body, 0)


def low_faces(k, faces, dims, pad):
    planes, rows, lanes = dims
    cx, cy0, cy1, cz0, cz1, cd = faces
    row, lane = iota((rows, lanes), 0), iota((rows, lanes), 1)
    scale = 0.5 * 0.0625

    def body(p, carry):
        kx = k[p + pad]
        below, above = scale * (k[p + pad - 1] + kx), scale * (kx + k[p + pad + 1])
        total = below + above
        cx[p] = below
        cx[p + 1] = above
        for target, inside, moved in (
            (cy0, row > 0, up(kx, 0)), (cy1, row < rows - 1, down(kx, 0)),
            (cz0, lane > 0, up(kx, 1)), (cz1, lane < lanes - 1, down(kx, 1))):
            face = scale * (kx + moved)
            target[p] = jnp.where(inside, face, 0.0)
            total = total + jnp.where(inside, face, scale * kx)
        cd[p] = total
        return carry

    repeat(planes, body, 0)


def bottom(f, s, vv, ww, faces, dims, pad):
    planes, rows, lanes = dims
    cx, cy0, cy1, cz0, cz1, cd = faces

    def operate(v, p):
        mid = v[p + pad]
        summed = cx[p] * v[p + pad - 1] + cx[p + 1] * v[p + pad + 1]
        summed = summed + (cy0[p] * up(mid, 0) + cy1[p] * down(mid, 0))
        summed = summed + (cz0[p] * up(mid, 1) + cz1[p] * down(mid, 1))
        return mid, cd[p] * mid - summed

    zero = jnp.zeros((rows, lanes), F32)

    def first(p, carry):
        mid, image = operate(f, p)
        vv[p + pad] = image
        return carry[0] + mid * mid, carry[1] + mid * image

    def total(v):
        return jnp.sum(jnp.sum(v, axis=0, keepdims=True), axis=1, keepdims=True)

    norm, along = repeat(planes, first, (zero, zero))
    alpha = total(norm) / total(along)

    def second(p, carry):
        ww[p] = operate(vv, p)[1]
        return carry

    repeat(planes, second, 0)

    def last(p, carry):
        rest = f[p + pad] - alpha * vv[p + pad]
        image = vv[p + pad] - alpha * ww[p]
        s[p + pad] = rest
        return carry[0] + image * rest, carry[1] + image * image

    turned, norm = repeat(planes, last, (zero, zero))
    return alpha, total(turned) / total(norm)


def choose_slots(ids, boxes, groups):
    held = ids[0].astype(F32)
    cap = held.shape[1]
    eye = iota((cap, cap), 0) == iota((cap, cap), 1)
    rows = jnp.broadcast_to(held, (cap, cap))
    cols = jnp.broadcast_to(jnp.sum(jnp.where(eye, rows, 0.0), axis=1, keepdims=True), (cap, cap))

    def target(v):
        return jnp.floor((v + 0.5) * (1.0 / boxes))

    earlier = (target(rows) == target(cols)) & (cols < rows) & (cols >= 0.0)
    ranking = jnp.sum(jnp.where(earlier, 1.0, 0.0), axis=0, keepdims=True)
    send_row = jnp.where(held >= 0.0, target(held) * SEND + ranking, -1.0)
    count = groups * SEND
    picker = jnp.where(iota((count, cap), 0).astype(F32) == jnp.broadcast_to(send_row, (count, cap)), 1.0, 0.0)
    return picker


def pack_boxes(slots, picker, outgoing):
    count, cap = picker.shape
    data = slots[0, 0].astype(F32)
    total = jnp.zeros((count, data.shape[1]), F32)
    for q in range(cap):
        total = total + picker[:, q : q + 1] * data[q : q + 1, :]
    for t in range(outgoing.shape[0]):
        outgoing[t] = total[SEND * t : SEND * t + SEND, :].astype(BF16)


def choose_boxes(owner, boxes):
    me = lax.axis_index("gz")
    owners = jnp.broadcast_to(owner[0].astype(F32), (boxes, owner.shape[2]))
    here = iota(owners.shape, 1) == iota(owners.shape, 0) + me * boxes
    col = jnp.sum(jnp.where(here, owners, 0.0), axis=1, keepdims=True)
    cols = jnp.broadcast_to(col, (boxes, boxes))
    first, second = iota((boxes, boxes), 0), iota((boxes, boxes), 1)
    row = jnp.sum(jnp.where(first == second, cols, 0.0), axis=0, keepdims=True)
    before = (jnp.broadcast_to(row, (boxes, boxes)) == cols) & (second < first)
    pick = col * SEND + jnp.sum(jnp.where(before, 1.0, 0.0), axis=1, keepdims=True)
    return pick


def place_boxes(incoming, held, pick, rows, boxes, groups):
    for t in range(groups):
        held[SEND * t : SEND * t + SEND, :] = incoming[t].astype(F32)
    per = 128 // BOX
    lane_box, row = iota((boxes, 128), 1) // BOX, iota((boxes, 128), 0)
    for part in range(BOX * BOX // per):
        lanes = slice(128 * part, 128 * part + 128)
        chosen = jnp.zeros((boxes, 128), F32)
        for r in range(groups * SEND):
            chosen = jnp.where(pick == float(r), held[r : r + 1, lanes], chosen)
        total = chosen
        for d in range(1, boxes):
            moved = pltpu.roll(pltpu.roll(chosen, BOX * d, 1), boxes - d, 0)
            total = jnp.where(((lane_box - row) & (boxes - 1)) == d, moved, total)
        rows[per * part : per * part + per, :] = total
    return jnp.dot(rows[...].astype(BF16), split_both(False).astype(BF16), preferred_element_type=F32)


def kernel(levels, counts, names, slots_in, ids_in, owner_in, coef_in, out, *scratch):
    r = dict(zip(names, scratch))
    groups = counts["gz"]
    at = {axis: lax.axis_index(axis) for axis in counts}
    slots, ids, owner, coef, units = r["slots"], r["ids"], r["owner"], r["coef"], r["units"]
    turns = (("move", "g", "low_f"), ("k", "q"), ("f", "low_k"), ("c", "e"))
    sends = {tag: n for n, tags in enumerate(turns) for tag in tags}
    sems = {tag: (r["sems"].at[n], r["sems"].at[len(turns) + k]) for k, (tag, n) in enumerate(sends.items())}
    loads = [
        pltpu.make_async_copy(source, target, r["sems"].at[n])
        for n, (source, target) in enumerate(((ids_in, ids), (slots_in, slots), (coef_in, coef), (owner_in, owner)))]
    for load in loads:
        load.start()
    fine, mid = levels["f"], levels["g"]
    sides = {tag: {name[: -len(tag)]: r[name] for name in lv.scratch(tag)} for tag, lv in levels.items()}
    for tag, lv in levels.items():
        clear_sides(lv, sides[tag])

    barrier = pltpu.get_barrier_semaphore()
    def signal_near(sem, offsets):
        count = 0
        for offset in offsets:
            target, exists = near(offset, counts)

            @pl.when(exists)
            def _():
                pl.semaphore_signal(sem, inc=1, device_id=target, device_id_type=MESH)

            count = count + jnp.where(exists, 1, 0)
        return count

    expected = signal_near(barrier, sorted([n for n in NEAR if 0 in n], key=lambda n: -sum(map(abs, n))))
    others = [{"gz": lax.rem(at["gz"] + k, groups)} for k in range(1, groups)]
    if counts["gx"] > 4 or counts["gy"] > 4:
        for offset in itertools.product(*[range(n) for n in counts.values()]):
            if any(offset):
                others.append({axis: lax.rem(at[axis] + k, counts[axis]) for axis, k in zip(counts, offset) if k})
    for target in others:
        pl.semaphore_signal(barrier, inc=1, device_id=target, device_id_type=MESH)

    def send(tag, axes=(1, 2, 3)):
        send_sides(levels[tag], sides[tag], sems[tag], counts, axes)

    def take(tag, emit):
        counted = units if levels[tag].dtype == F32 else r["half_units"]
        take_sides(levels[tag], sides[tag], sems[tag], counts, counted, emit)

    loads[0].wait()
    boxes = out.shape[2] // BOX
    picker = choose_slots(ids, boxes, groups)
    loads[1].wait()
    pack_boxes(slots, picker, r["outgoing"])
    pl.semaphore_wait(barrier, expected + len(others))

    me = at["gz"]
    for k in range(1, groups):
        to = lax.rem(me + k, groups)
        pltpu.make_async_remote_copy(
            r["outgoing"].at[to], r["incoming"].at[me], sems["move"][0], sems["move"][1],
            device_id={"gz": to}, device_id_type=MESH).start()
    greeted = signal_near(r["hello"], list(itertools.product((-1, 1), (0,), (-1, 0, 1))))
    loads[2].wait()
    loads[3].wait()
    choose = lambda both, t: jnp.where(even_rows(t, fine.y), both[t, :, 0:128], both[t, :, 128:256])
    split = pick(coef[...].reshape(fine.t * fine.y, 128), split_both(False)).reshape(fine.t, fine.y, 256)
    for t in range(fine.t):
        sides["k"]["st"][t] = choose(split, t)
    pack_sides(levels["k"], sides["k"])
    send("k", (1, 2))
    r["incoming"][me] = r["outgoing"][me]

    half_t, half_y = fine.t // 2, fine.y // 2
    for i in range(half_t):
        pair = sides["k"]["st"][2 * i] + sides["k"]["st"][2 * i + 1]
        r["pairs"][i] = pair + pltpu.roll(pair, 64, 1)
    coarse = 0.125 * fold_rows(r["pairs"], half_y)
    merged = [merge_planes(coarse[i], coarse[i + 1]) for i in range(0, half_t, 2)]
    pair_planes([plane for pair in merged for plane in pair], sides["c"]["st"])
    pack_sides(mid, sides["c"])
    pl.semaphore_wait(r["hello"], greeted)
    send("k", (3,))
    send("c")
    for i in range(half_t // 2):
        r["pairsm"][i] = coarse[2 * i] + coarse[2 * i + 1]
    here = (at["gx"], at["gy"], at["gz"])
    r["gk"][here] = coarse_low(r["pairsm"], r["tmp"])
    r["pick"][...] = jnp.broadcast_to(choose_boxes(owner, boxes), r["pick"].shape)
    if groups > 1:
        part = r["incoming"].at[pl.ds(0, groups - 1)]
        for n in range(2):
            pltpu.make_async_copy(part, part, sems["move"][n]).wait()
    source = place_boxes(r["incoming"], r["held"], r["pick"][...], r["rows"], boxes, groups)
    source = source.reshape(fine.t, fine.y, 256)
    for t in range(fine.t):
        sides["f"]["st"][t] = choose(source, t).astype(BF16)
    pack_sides(fine, sides["f"])
    send("f")

    pair_of = lambda name: (r[name + "r"], r[name + "b"])
    v0, g0, k0 = pair_of("v0"), pair_of("g0"), pair_of("k0")
    fx, fy, zo, dd0, iv0 = (pair_of(name) for name in ("fx0", "fy0", "zo0", "dd0", "iv0"))
    faces0 = (fx, fy, r["zs0"], zo)
    fx1, fy1, fz1, dd1, iv1, v1, g1, k1 = (pair_of(n) for n in ("fx1", "fy1", "fz1", "dd1", "iv1", "v1", "g1", "k1"))
    faces1 = (r["xs1"], fx1, fy1, fz1)

    def store_pair(refs):
        def emit(t, first, second):
            refs[0][t] = first
            refs[1][t] = second
        return emit

    def store_planes(ref):
        def emit(t, first, second):
            ref[2 * t] = first
            ref[2 * t + 1] = second
        return emit

    take("k", store_pair(k0))
    prepare_fine(fine, k0, sides["k"]["lk"], fx, fy, r["zs0"], zo, dd0, iv0)

    def open_fine(t, red, black):
        g0[0][t] = red
        g0[1][t] = black
        v0[0][t] = red * iv0[0][t]

    take("f", open_fine)
    for reach, colour in ((3, 1), (2, 0), (1, 1)):
        half_sweep_fine(fine, v0, g0, faces0, iv0, colour, reach)
    residual_fine(fine, v0, g0, faces0, dd0, r["pairs"])

    coarse = 0.5 * fold_rows(r["pairs"], half_y)
    merged = [merge_planes(coarse[i], coarse[i + 1]) for i in range(0, half_t, 2)]
    pair_planes([plane for pair in merged for plane in pair], sides["g"]["st"])
    pack_sides(mid, sides["g"])
    send("g")
    take("c", store_pair(k1))
    prepare_mid(k1, *faces1, dd1, iv1)
    for name in ("k2", "f2", "s2", "v2"):
        r[name][...] = jnp.zeros(r[name].shape, F32)
    pair_planes([v0[1][fine.wt + x, 0 : fine.y, :] for x in range(fine.t)], sides["q"]["st"])
    pack_sides(levels["q"], sides["q"])
    send("q")
    gather_start(r["gk"], sems["low_k"], counts)
    wm = 2 * mid.wt

    def open_mid(t, red, black):
        g1[0][t] = red
        g1[1][t] = black
        v1[0][t] = red * iv1[0][t]

    take("g", open_mid)
    for reach, colour in ((3, 1), (2, 0), (1, 1)):
        half_sweep_mid(mid, v1, g1, faces1, iv1, colour, reach)
    residual_mid(mid, v1, g1, faces1, dd1, r["pairsm"])
    r["gf"][here] = coarse_low(r["pairsm"], r["tmp"])
    gather_start(r["gf"], sems["low_f"], counts)
    pair_planes([v1[1][mid.wt + t, 0 : mid.y, :] for t in range(mid.t)], sides["e"]["st"])
    pack_sides(levels["e"], sides["e"])
    send("e")

    planes, rows, lanes = dims = (4 * counts["gx"], 4 * counts["gy"], 32 * counts["gz"])
    pad = wm // 2
    low = tuple(r[name] for name in ("cx", "cy0", "cy1", "cz0", "cz1", "cd"))
    take("q", store_planes(r["q0"]))
    gather_wait(sems["low_k"], counts, units)
    spread_low(r["gk"], r["k2"], counts, pad)
    low_faces(r["k2"], low, dims, pad)

    def store_black(t, *planes):
        for k, plane in enumerate(planes):
            n = 2 * t + k - (2 * levels["e"].wt - mid.wt)
            if 0 <= n < mid.te:
                v1[1][n] = plane

    take("e", store_black)
    gather_wait(sems["low_f"], counts, units)
    spread_low(r["gf"], r["f2"], counts, pad)
    alpha, omega = bottom(r["f2"], r["s2"], r["v2"], r["w2"], low, dims, pad)
    around_low = mid.te
    for q in range(around_low):
        turned = alpha * r["f2"][4 * at["gx"] + q] + omega * r["s2"][4 * at["gx"] + q]
        plane = turned
        for c in range(1, counts["gy"]):
            turned = jnp.where(at["gy"] == c, pltpu.roll(plane, rows - 4 * c, 0), turned)
        r["local"][q, 0:8, :] = turned[0:8, :]
        r["local"][q, 8:16, :] = pltpu.roll(turned[rows - 8 : rows, :], 4, 0)
    goal = iota((lanes, 128), 1)
    cell = jnp.where(goal < 64 + wm, goal, goal - 128)
    cell = (cell + 128) // 2 - 64
    wanted = (goal < 64 + wm) | (goal >= 128 - wm)
    matrix = jnp.where((iota((lanes, 128), 0) == 32 * at["gz"] + cell) & wanted, 1.0, 0.0).astype(F32)
    spread = pick(r["local"][...].reshape(16 * around_low, lanes), matrix).reshape(around_low, 16, 128)
    for q in range(around_low):
        wide = r["wide"].at[q]
        for k in range(2):
            wide[pl.ds(k, 12, stride=2), :] = spread[q, 0:12]
        v1[1][q] = jnp.where(k1[1][q] > 0.0, v1[1][q] + wide[...], 0.0)
    for reach, colour in ((5, 0), (4, 1), (3, 0), (2, 1)):
        half_sweep_mid(mid, v1, g1, faces1, iv1, colour, reach)

    low_w = fine.wt // 2
    row = iota((8, 128), 0)
    for i in range(half_t + 2 * low_w):
        x = wm - low_w + i
        wide = r["wide"].at[i]
        plane = merge_planes(v1[0][x // 2], v1[1][x // 2])[x % 2]
        ends = jnp.where(row < low_w, plane[8:16], pltpu.roll(plane[mid.ye - 8 : mid.ye], 4, 0))
        turned = jnp.concatenate([plane[0:8], ends[0:4]], axis=0)
        for k in range(2):
            wide[pl.ds(k, 12, stride=2), :] = turned
        for k in range(2):
            v0[1][2 * i + k] = r["q0"][2 * i + k] + wide[...]
    for reach, colour in ((3, 0), (2, 1), (1, 0), (0, 1)):
        half_sweep_fine(fine, v0, g0, faces0, iv0, colour, reach)
    lane = iota((fine.y, 128), 1)
    for t in range(fine.t):
        red, black = (v0[c][fine.wt + t, 0 : fine.y, :] for c in range(2))
        r["joined"][t] = jnp.where(lane < 64, red, pltpu.roll(black, 64, 1))
    joined = pick(r["joined"][...].reshape(fine.t * fine.y, 128), split_both(True)).reshape(fine.t, fine.y, 256)
    for t in range(fine.t):
        out[t] = choose(joined, t)


def per_device(counts, old_slots, old_ids, old_owner, coefficient):
    x, y, z = coefficient.shape
    planes, rows, lanes = 4 * counts["gx"], 4 * counts["gy"], 32 * counts["gz"]
    groups, boxes = counts["gz"], z // BOX
    cells = old_slots.shape[3]
    mid = Level(x // 4, y // 2, 3, 8, 6)
    levels = {
        "k": Level(x, y, 5, 4, 3, deep=True), "f": Level(x, y, 4, 4, 2, dtype=BF16), "q": Level(x // 2, y, 2, 4, 2),
        "c": mid, "g": mid, "e": Level(x // 8, y // 2, 2, 8, 6)}
    fine, edge = levels["f"], levels["k"]
    pad = mid.wt
    devices = counts["gx"] * counts["gy"] * groups
    vmem = lambda *shape: pltpu.VMEM(shape, F32)
    dma = lambda *shape: pltpu.SemaphoreType.DMA(shape)
    scratch = {}
    for tag, level in levels.items():
        scratch.update(level.scratch(tag))
    for name in ("v0", "g0", "fx0", "fy0", "zo0", "dd0", "iv0", "k0"):
        for colour in "rb":
            scratch[name + colour] = vmem(edge.te if name == "k0" else fine.te, fine.ye, 128)
    for name in ("zs0", "q0"):
        scratch[name] = vmem(fine.te, fine.ye, 128)
    for name in ("fx1", "fy1", "fz1", "dd1", "iv1", "v1", "g1", "k1"):
        for colour in "rb":
            scratch[name + colour] = vmem(mid.te, mid.ye, 128)
    scratch["xs1"] = vmem(mid.te, mid.ye, 128)
    scratch.update(
        slots=pltpu.VMEM(old_slots.shape, old_slots.dtype), ids=pltpu.VMEM(old_ids.shape, old_ids.dtype),
        owner=pltpu.VMEM(old_owner.shape, old_owner.dtype), coef=vmem(*coefficient.shape),
        outgoing=pltpu.VMEM((groups, SEND, cells), BF16), incoming=pltpu.VMEM((groups, SEND, cells), BF16),
        held=vmem(groups * SEND, cells), sems=dma(13), hello=pltpu.SemaphoreType.REGULAR, units=vmem(max(160, devices), 4, 128),
        half_units=pltpu.VMEM((160, 4, 128), BF16),
        rows=vmem(BOX * BOX, 128), pick=vmem(boxes, 128), pairs=vmem(x // 2, y, 128), pairsm=vmem(x // 4, y // 2, 128),
        joined=vmem(x, y, 128), tmp=vmem(x * y // 16, 128), local=vmem(mid.te, 16, lanes),
        wide=vmem(max(mid.te, fine.te // 2), 24, 128),
        gk=vmem(counts["gx"], counts["gy"], groups, 4, 128), gf=vmem(counts["gx"], counts["gy"], groups, 4, 128),
        cx=vmem(planes + 1, rows, lanes), w2=vmem(planes, rows, lanes))
    for name in ("cy0", "cy1", "cz0", "cz1", "cd"):
        scratch[name] = vmem(planes, rows, lanes)
    for name in ("f2", "k2", "s2", "v2"):
        scratch[name] = vmem(planes + 2 * pad, rows, lanes)
    return pl.pallas_call(
        functools.partial(kernel, levels, counts, tuple(scratch)),
        out_shape=jax.ShapeDtypeStruct(coefficient.shape, F32),
        in_specs=[pl.BlockSpec(memory_space=pltpu.MemorySpace.HBM)] * 4,
        out_specs=pl.BlockSpec(memory_space=pltpu.VMEM),
        scratch_shapes=list(scratch.values()),
        compiler_params=pltpu.CompilerParams(
            collective_id=0, has_side_effects=True, vmem_limit_bytes=44 * 1024 * 1024),
    )(*[pltpu.with_memory_space_constraint(v, pltpu.HBM) for v in (old_slots, old_ids, old_owner, coefficient)])


def solution(mesh):
    counts = {axis: mesh.shape[axis] for axis in ("gx", "gy", "gz")}
    return jax.shard_map(
        functools.partial(per_device, counts), mesh=mesh,
        in_specs=(P("gx", "gy", "gz", None), P("gx", "gy", "gz"), P("gx", "gy", None), P("gx", "gy", "gz")),
        out_specs=P("gx", "gy", "gz"), check_vma=False)
```
